32 devices in a mesh: gz: 32 (over z, y, x, core).
Axes of the slice: x: 2, y: 2, z: 4, core: 2. Of those that a mesh axis runs over, the one named last changes fastest.
Arguments:
- coefficient: float32 [64, 512, 512], P('gz'), may hold values from 0.2 to 1.3
- initial_field: float32 [64, 512, 512], P('gz'), may hold values from -6 to 6
- observed: float32 [64, 512, 512], P('gz'), may hold values from -6 to 6
- misfit_weight: float32 [64, 512, 512], P('gz'), may hold values from 0.5 to 6, as said below
Outputs:
- coeff_gradient: float32 [64, 512, 512], P('gz')
- adjoint_field: float32 [64, 512, 512], P('gz')
- misfit: float32 [], replicated
The draws below stay inside these ranges and needn't reach their ends.
Inputs may be any that keep to these rules, and one draw needn't show every extreme that they name: `misfit_weight`: positive cell weights.
All inputs are finite; a program needn't handle non-finite values.
Results may differ from the reference program's by a relative error of at most 0.00002.
Values sent between devices are 32-bit elements; how exact they have to be, the bound alone decides.
No kernel may reach another device: no remote copies, remote signals or barrier semaphores. Data moves between devices by JAX's collectives and lax.ppermute only.
A program may use at most 128 MiB of HBM per device.

```python
import math
import jax
import jax.numpy as jnp

NY = 512
NX = 512
ITERS = 4
NZ = 64


def draw_misfit_weight(key, part):
    depth = jnp.arange(NZ, dtype=jnp.float32)[:, None, None]
    ramp = 1.0 + 2.0 * depth / (NZ - 1)
    base = jnp.exp(jax.random.uniform(key, (NZ, NY, NX), jnp.float32, jnp.log(0.5), jnp.log(2.0)))
    return (ramp * base).astype(jnp.float32)


def block_scale(stream_key, shape, split, smallest, high):
    def one(axis_at, parts):
        steps = jax.random.uniform(jax.random.fold_in(jax.random.fold_in(stream_key, 6), axis_at), (parts,), jnp.float32, smallest / len(split), high / len(split))
        return jnp.repeat(jnp.exp(steps), shape[axis_at] // parts).reshape((-1,) + (1,) * (len(shape) - axis_at - 1))

    gain = one(*split[0])
    for cut in split[1:]:
        gain = gain * one(*cut)
    return gain


def centred(key, extent, width, bound, split=(), kind=jnp.bfloat16):
    array = width * jax.random.normal(key, extent, jnp.float32)
    if split:
        array = array * block_scale(key, extent, split, -0.22, 0.18)
    return jnp.clip(array, -bound, bound).astype(kind)


def setup_inputs(seed: int = 0) -> dict:
    splits = jax.random.split(jax.random.key(seed), 5)
    coefficient = jnp.clip(jnp.exp(math.log(1.3) - 1.8718021 * jax.random.uniform(splits[0], (NZ, NY, NX), jnp.float32) ** block_scale(splits[0], (NZ, NY, NX), ((0, 32),), -0.2, 0.2)), 0.2, 1.3)
    initial_field = centred(splits[1], (NZ, NY, NX), 1.0, 6.0, ((0, 32),), jnp.float32)
    observed = centred(splits[2], (NZ, NY, NX), 1.0, 6.0, ((0, 32),), jnp.float32)
    misfit_weight = draw_misfit_weight(jax.random.fold_in(splits[4], 71), 0)
    return {"coefficient": coefficient, "initial_field": initial_field, "observed": observed, "misfit_weight": misfit_weight}


time_step = 0.125

def laplace(field):
    padded = jnp.pad(field, 1)
    beside = padded[2:, 1:-1, 1:-1] + padded[:-2, 1:-1, 1:-1]
    beside = beside + padded[1:-1, 2:, 1:-1] + padded[1:-1, :-2, 1:-1]
    beside = beside + padded[1:-1, 1:-1, 2:] + padded[1:-1, 1:-1, :-2]
    return beside - 6.0 * field

def reference(coefficient, initial_field, observed, misfit_weight):
    state = initial_field
    slopes = []
    for step in range(ITERS):
        slope = laplace(state)
        slopes.append(slope)
        state = state + time_step * coefficient * slope
    resid = state - observed
    total = jnp.sum(misfit_weight * resid * resid)
    misfit = jnp.sqrt(total / (NZ * NY * NX) + 1e-06)
    adjoint = misfit_weight * resid / misfit
    gradient = jnp.zeros_like(coefficient)
    for step in reversed(range(ITERS)):
        gradient = gradient + time_step * adjoint * slopes[step]
        adjoint = adjoint + time_step * laplace(coefficient * adjoint)
    return (gradient, adjoint, misfit)
```

```python
import jax
import jax.numpy as jnp
from jax import lax
from jax.experimental import pallas as pl
from jax.experimental.pallas import tpu as pltpu
from jax.sharding import PartitionSpec as P

ITERS = 4
time_step = 0.125

GROUP = 8
PARTS = 4
HALO = 8
ROUNDS = ((0, 0), (0, 1), (1, 0), (1, 1))


VM = pl.BlockSpec(memory_space=pltpu.VMEM)
SM = pl.BlockSpec(memory_space=pltpu.SMEM)
PARAMS = pltpu.CompilerParams(vmem_limit_bytes=60 * 1024 * 1024)
F32 = jnp.float32


def call(kernel, name, outs, n_in, scratch=(), out_specs=None):
    return pl.pallas_call(
        kernel,
        name=name,
        out_shape=outs,
        in_specs=[SM] + [VM] * n_in,
        out_specs=out_specs if out_specs is not None else [VM] * len(outs),
        scratch_shapes=scratch,
        compiler_params=PARAMS,
    )


def bits(me):
    return (me >> 2) & 1, (me >> 1) & 1, me & 1


def part(y, x):
    return 2 * y + x


def send_pairs(count, r1, r0):
    pairs = []
    for i in range(count):
        y, x, c = bits(i)
        pairs.append((i, (i & ~7) + 4 * (c ^ r1) + 2 * (x ^ r0) + y))
    return pairs


def row_loop(rows, body, step=16):
    def one(t, carry):
        body(pl.ds(pl.multiple_of(t * step, 8), step))
        return carry

    lax.fori_loop(0, rows // step, one, 0)


def pack_kernel(me_ref, a_ref, b_ref, *out_refs):
    y, x, c = bits(me_ref[0])
    height = a_ref.shape[1]
    rows = height // PARTS
    planes = a_ref.shape[0]
    for (r1, r0), out in zip(ROUNDS, out_refs):
        q = part(c ^ r1, x ^ r0)
        start = pl.multiple_of(q * rows, 8)
        above = pl.multiple_of(jnp.maximum(start - HALO, 0), 8)
        below = pl.multiple_of(jnp.minimum(start + rows, height - HALO), 8)
        for k, src in enumerate((a_ref, b_ref)):
            for i in range(planes):
                top = src[i, pl.ds(above, HALO), :]
                out[k, i, :HALO, :] = jnp.where(q > 0, top, 0.0)
                low = src[i, pl.ds(below, HALO), :]
                out[k, i, HALO + rows :, :] = jnp.where(q < PARTS - 1, low, 0.0)

                def one(t, carry, src=src, out=out, k=k, i=i, start=start):
                    at = pl.multiple_of(t * 16, 8)
                    out[k, i, pl.ds(at + HALO, 16), :] = src[i, pl.ds(pl.multiple_of(start + at, 8), 16), :]
                    return carry

                lax.fori_loop(0, rows // 16, one, 0, unroll=True)


def slot(me, r, planes, i):
    y, x, c = bits(me)
    r1, r0 = r
    from_c = y ^ r1
    block = x ^ r0 ^ c
    ahead = planes * from_c + i
    return block, jnp.where(c == 0, ahead, 2 * planes - 1 - ahead)


def place_kernel(me_ref, m0, m1, m2, m3, a_ref, b_ref):
    me = me_ref[0]
    planes, rows = m0.shape[1], m0.shape[2]
    for r, m in zip(ROUNDS, (m0, m1, m2, m3)):
        for i in range(planes):
            block, at = slot(me, r, planes, i)
            for flag, dst in ((1, a_ref), (0, b_ref)):

                @pl.when(block == flag)
                def _(dst=dst, m=m, i=i, at=at):
                    for k in range(2):
                        row_loop(rows, lambda s, k=k: dst.__setitem__((k, at, s), m[k, i, s]))


def edges(shape):
    col = lax.broadcasted_iota(jnp.int32, shape, 1)
    return col == 0, col == shape[1] - 1


def lap_rows(ref, s, r0, n, first, last):
    lo = HALO + r0
    mid = ref[s, lo : lo + n, :]
    width = mid.shape[1]
    beside = ref[s + 1, lo : lo + n, :] + ref[s - 1, lo : lo + n, :]
    beside = beside + (ref[s, lo + 1 : lo + n + 1, :] + ref[s, lo - 1 : lo + n - 1, :])
    right = jnp.where(last, 0.0, pltpu.roll(mid, width - 1, 1))
    left = jnp.where(first, 0.0, pltpu.roll(mid, 1, 1))
    return beside + (right + left) - 6.0 * mid, mid


def clear_rims(ref, rows):
    width = ref.shape[2]

    def one(s, carry):
        ref[s, :HALO, :] = jnp.zeros((HALO, width), F32)
        ref[s, HALO + rows :, :] = jnp.zeros((HALO, width), F32)
        return carry

    lax.fori_loop(0, ref.shape[0], one, 0)


def sequence(a_ref, b_ref, ra_ref, rb_ref, half):
    out = []
    for s in range(half):
        out.append((rb_ref, half - 1 - s, s))
        out.append((b_ref, s, half + s))
        out.append((a_ref, s, 2 * half + s))
        out.append((ra_ref, half - 1 - s, 3 * half + s))
    return out


CHUNK = 16


def forward_kernel(me_ref, a_ref, b_ref, ra_ref, rb_ref, u_out, c_out, slopes, u0, u1):
    half, rows = a_ref.shape[1], a_ref.shape[2]
    clear_rims(u0, rows)
    clear_rims(u1, rows)
    for src, at, s in sequence(a_ref, b_ref, ra_ref, rb_ref, half):

        def fill(t, carry, src=src, at=at, s=s):
            r = pl.multiple_of(t * 16, 8)
            u0[s, pl.ds(r + HALO, 16), :] = src[0, at, pl.ds(r, 16), :]
            c_out[s, pl.ds(r, 16), :] = time_step * src[1, at, pl.ds(r, 16), :]
            return carry

        lax.fori_loop(0, rows // 16, fill, 0)
    first, last = edges((CHUNK, a_ref.shape[3]))
    own = range(half, 3 * half)
    for k in range(ITERS):
        old, new = (u0, u1) if k % 2 == 0 else (u1, u0)
        wide = ITERS - 1 - k

        def plane(s, carry, k=k, old=old, new=new):
            keep = jnp.clip(s - half, 0, 2 * half - 1)
            for r0 in range(0, rows, CHUNK):
                slope, mid = lap_rows(old, s, r0, CHUNK, first, last)
                moved = mid + c_out[s, r0 : r0 + CHUNK, :] * slope
                if k == ITERS - 1:
                    u_out[s - half, r0 : r0 + CHUNK, :] = moved
                    slopes[k, s - half, r0 : r0 + CHUNK, :] = slope
                else:
                    new[s, HALO + r0 : HALO + r0 + CHUNK, :] = moved
                    slopes[k, keep, r0 : r0 + CHUNK, :] = slope
            return carry

        for lo, hi in ((own[0] - wide, own[0]), (own[-1] + 1, own[-1] + 1 + wide), (own[0], own[-1] + 1)):
            if hi > lo:
                lax.fori_loop(lo, hi, plane, 0)


def resid_kernel(me_ref, m0, m1, m2, m3, u_ref, a_ref, b_ref, total_ref):
    me = me_ref[0]
    planes, rows, width = m0.shape[1], m0.shape[2], m0.shape[3]
    acc = jnp.zeros((8, width), F32)
    for r, m in zip(ROUNDS, (m0, m1, m2, m3)):
        for i in range(planes):
            block, at = slot(me, r, planes, i)
            pos = 2 * planes * block + at

            def one(t, carry, m=m, i=i, pos=pos, block=block, at=at):
                s = pl.ds(pl.multiple_of(t * 8, 8), 8)
                resid = u_ref[pos, s, :] - m[0, i, s, :]
                weighted = m[1, i, s, :] * resid

                @pl.when(block == 1)
                def _():
                    a_ref[at, s, :] = weighted

                @pl.when(block == 0)
                def _():
                    b_ref[at, s, :] = weighted

                inside = jnp.logical_and(t > 0, t < rows // 8 - 1)
                return carry + jnp.where(inside, weighted * resid, 0.0)

            acc = lax.fori_loop(0, rows // 8, one, acc)
    total_ref[0, 0] = jnp.sum(acc)


def backward_kernel(me_ref, a_ref, b_ref, ra_ref, rb_ref, c_ref, slopes, o0, o1, o2, o3, lam, mv0, mv1, grad):
    me = me_ref[0]
    half, rows = a_ref.shape[0], a_ref.shape[1]
    inner = rows - 2 * HALO
    clear_rims(mv0, rows)
    clear_rims(mv1, rows)
    for src, at, s in sequence(a_ref, b_ref, ra_ref, rb_ref, half):

        def fill(t, carry, src=src, at=at, s=s):
            r = pl.multiple_of(t * 16, 8)
            v = src[at, pl.ds(r, 16), :]
            lam[s, pl.ds(r, 16), :] = v
            mv0[s, pl.ds(r + HALO, 16), :] = c_ref[s, pl.ds(r, 16), :] * v
            return carry

        lax.fori_loop(0, rows // 16, fill, 0)
    first, last = edges((CHUNK, a_ref.shape[2]))
    first8, last8 = edges((HALO, a_ref.shape[2]))
    own = range(half, 3 * half)
    for k in reversed(range(ITERS)):
        old, new = (mv0, mv1) if (ITERS - 1 - k) % 2 == 0 else (mv1, mv0)
        wide = k

        def halo_plane(s, carry, old=old, new=new):
            for r0 in range(0, rows, CHUNK):
                change, _ = lap_rows(old, s, r0, CHUNK, first, last)
                after = lam[s, r0 : r0 + CHUNK, :] + change
                lam[s, r0 : r0 + CHUNK, :] = after
                new[s, HALO + r0 : HALO + r0 + CHUNK, :] = c_ref[s, r0 : r0 + CHUNK, :] * after
            return carry

        def own_plane(s, carry, k=k, old=old, new=new):
            for r0 in range(HALO, rows - HALO, CHUNK):
                change, _ = lap_rows(old, s, r0, CHUNK, first, last)
                before = lam[s, r0 : r0 + CHUNK, :]
                g = before * slopes[k, s - half, r0 : r0 + CHUNK, :]
                at = slice(r0 - HALO, r0 - HALO + CHUNK)
                grad[s - half, at, :] = g if k == ITERS - 1 else grad[s - half, at, :] + g
                after = before + change
                lam[s, r0 : r0 + CHUNK, :] = after
                if k:
                    new[s, HALO + r0 : HALO + r0 + CHUNK, :] = c_ref[s, r0 : r0 + CHUNK, :] * after
            if k:
                for r0 in (0, rows - HALO):
                    change, _ = lap_rows(old, s, r0, HALO, first8, last8)
                    after = lam[s, r0 : r0 + HALO, :] + change
                    lam[s, r0 : r0 + HALO, :] = after
                    new[s, HALO + r0 : 2 * HALO + r0, :] = c_ref[s, r0 : r0 + HALO, :] * after
            return carry

        if wide:
            lax.fori_loop(own[0] - wide, own[0], halo_plane, 0)
            lax.fori_loop(own[-1] + 1, own[-1] + 1 + wide, halo_plane, 0)
        lax.fori_loop(own[0], own[-1] + 1, own_plane, 0)
    planes = half // 2
    for r, out in zip(ROUNDS, (o0, o1, o2, o3)):
        for i in range(planes):
            block, at = slot(me, r, planes, i)
            pos = half * block + at

            def one(t, carry, out=out, i=i, pos=pos):
                s = pl.multiple_of(t * 16, 8)
                out[0, i, pl.ds(s, 16), :] = grad[pos, pl.ds(s, 16), :]
                out[1, i, pl.ds(s, 16), :] = lam[half + pos, pl.ds(s + HALO, 16), :]
                return carry

            lax.fori_loop(0, inner // 16, one, 0)


def home_kernel(me_ref, scale_ref, m0, m1, m2, m3, g_ref, a_ref):
    y, x, c = bits(me_ref[0])
    planes, rows = m0.shape[1], m0.shape[2]
    for (r1, r0), m in zip(ROUNDS, (m0, m1, m2, m3)):
        start = part(c ^ r1, x ^ r0) * rows
        for k, out in enumerate((g_ref, a_ref)):
            scale = scale_ref[k]
            for i in range(planes):

                def one(t, carry, m=m, k=k, i=i, out=out, start=start, scale=scale):
                    s = pl.multiple_of(t * 16, 8)
                    out[i, pl.ds(pl.multiple_of(start + s, 8), 16), :] = m[k, i, pl.ds(s, 16), :] * scale
                    return carry

                lax.fori_loop(0, rows // 16, one, 0)


def shape(*dims):
    return jax.ShapeDtypeStruct(dims, F32)


def group_sum(value, axis, count):
    if count & (count - 1):
        return lax.psum(value, axis)
    step = 1
    while step < count:
        value = value + lax.ppermute(value, axis, [(i, i ^ step) for i in range(count)])
        step *= 2
    return value


def on_device(coefficient, initial_field, observed, misfit_weight):
    axis = "gz"
    count = lax.axis_size(axis)
    planes, height, width = coefficient.shape
    if count % GROUP or height % (16 * PARTS) or 2 * planes < ITERS or ITERS * 2 > HALO:
        raise ValueError("unsupported sizes")
    rows = height // PARTS
    tall = rows + 2 * HALO
    half = 2 * planes
    me = lax.axis_index(axis).astype(jnp.int32).reshape(1)

    partner = [(i, i ^ 1) for i in range(count)]
    beyond = []
    for i in range(count - GROUP + 1):
        if i % 2:
            if i + GROUP - 1 < count:
                beyond += [(i, i + GROUP - 1), (i + GROUP - 1, i)]

    def regroup(a, b, name):
        msgs = call(pack_kernel, name, [shape(2, planes, tall, width)] * 4, 2)(me, a, b)
        return [lax.ppermute(m, axis, send_pairs(count, *r)) for m, r in zip(msgs, ROUNDS)]

    first = regroup(initial_field, coefficient, "pack_state")
    second = regroup(observed, misfit_weight, "pack_data")

    pair = [shape(2, half, tall, width)] * 2
    blk_a, blk_b = call(place_kernel, "place", pair, 4)(me, *first)
    far_a = lax.ppermute(blk_a, axis, partner)
    far_b = lax.ppermute(blk_b, axis, beyond)
    final, coef, slopes = call(
        forward_kernel,
        "forward",
        [shape(2 * half, tall, width), shape(4 * half, tall, width), shape(ITERS, 2 * half, tall, width)],
        4,
        [pltpu.VMEM((4 * half, tall + 2 * HALO, width), F32)] * 2,
    )(me, blk_a, blk_b, far_a, far_b)

    lam_a, lam_b, part_total = call(
        resid_kernel,
        "resid",
        [shape(half, tall, width)] * 2 + [shape(1, 1)],
        5,
        out_specs=[VM, VM, SM],
    )(me, *second, final)
    far_la = lax.ppermute(lam_a, axis, partner)
    far_lb = lax.ppermute(lam_b, axis, beyond)
    outs = call(
        backward_kernel,
        "backward",
        [shape(2, planes, rows, width)] * 4,
        6,
        [pltpu.VMEM((4 * half, tall, width), F32)]
        + [pltpu.VMEM((4 * half, tall + 2 * HALO, width), F32)] * 2
        + [pltpu.VMEM((2 * half, rows, width), F32)],
    )(me, lam_a, lam_b, far_la, far_lb, coef, slopes)
    back = [
        lax.ppermute(m, axis, [(j, i) for i, j in send_pairs(count, *r)]) for m, r in zip(outs, ROUNDS)
    ]

    total = group_sum(part_total, axis, count)
    cells = count * planes * height * width
    misfit = jnp.sqrt(total[0, 0] / cells + 1e-06)
    inverse = 1.0 / misfit
    scale = jnp.stack([time_step * inverse, inverse])
    gradient, adjoint = pl.pallas_call(
        home_kernel,
        name="home",
        out_shape=[shape(planes, height, width)] * 2,
        in_specs=[SM, SM] + [VM] * 4,
        out_specs=[VM] * 2,
        compiler_params=PARAMS,
    )(me, scale, *back)
    return gradient, adjoint, misfit


def solution(mesh):
    placed = P("gz", None, None)
    return jax.shard_map(
        on_device,
        mesh=mesh,
        in_specs=(placed,) * 4,
        out_specs=(placed, placed, P()),
        check_vma=False,
    )
```

```python
import jax
import jax.numpy as jnp
from jax import lax
from jax.experimental import pallas as pl
from jax.experimental.pallas import tpu as pltpu
from jax.sharding import PartitionSpec as P


ITERS = 4
time_step = 0.125

GROUP = 8
PARTS = 4
HALO = 8
ROUNDS = ((0, 0), (0, 1), (1, 0), (1, 1))


VM = pl.BlockSpec(memory_space=pltpu.VMEM)
SM = pl.BlockSpec(memory_space=pltpu.SMEM)
PARAMS = pltpu.CompilerParams(vmem_limit_bytes=60 * 1024 * 1024)
F32 = jnp.float32


def call(kernel, outs, n_in, scratch=(), out_specs=None):
    return pl.pallas_call(
        kernel,
        out_shape=outs,
        in_specs=[SM] + [VM] * n_in,
        out_specs=out_specs if out_specs is not None else [VM] * len(outs),
        scratch_shapes=scratch,
        compiler_params=PARAMS,
    )


def bits(me):
    return (me >> 2) & 1, (me >> 1) & 1, me & 1


def part(y, x):
    return 2 * y + x


def send_pairs(count, r1, r0):
    pairs = []
    for i in range(count):
        y, x, c = bits(i)
        pairs.append((i, (i & ~7) + 4 * (c ^ r1) + 2 * (x ^ r0) + y))
    return pairs


def row_loop(rows, body, step=16):
    def one(t, carry):
        body(pl.ds(pl.multiple_of(t * step, 8), step))
        return carry

    lax.fori_loop(0, rows // step, one, 0)


def pack_kernel(me_ref, a_ref, b_ref, *out_refs):
    _, x, c = bits(me_ref[0])
    height = a_ref.shape[1]
    rows = height // PARTS
    planes = a_ref.shape[0]
    for (r1, r0), out in zip(ROUNDS, out_refs):
        q = part(c ^ r1, x ^ r0)
        start = pl.multiple_of(q * rows, 8)
        above = pl.multiple_of(jnp.maximum(start - HALO, 0), 8)
        below = pl.multiple_of(jnp.minimum(start + rows, height - HALO), 8)
        for k, src in enumerate((a_ref, b_ref)):
            for i in range(planes):
                top = src[i, pl.ds(above, HALO), :]
                out[k, i, :HALO, :] = jnp.where(q > 0, top, 0.0)
                low = src[i, pl.ds(below, HALO), :]
                out[k, i, HALO + rows :, :] = jnp.where(q < PARTS - 1, low, 0.0)

                def one(t, carry, src=src, out=out, k=k, i=i, start=start):
                    at = pl.multiple_of(t * 16, 8)
                    out[k, i, pl.ds(at + HALO, 16), :] = src[i, pl.ds(pl.multiple_of(start + at, 8), 16), :]
                    return carry

                lax.fori_loop(0, rows // 16, one, 0, unroll=True)


def slot(me, r, planes, i):
    y, x, c = bits(me)
    r1, r0 = r
    from_c = y ^ r1
    block = x ^ r0 ^ c
    ahead = planes * from_c + i
    return block, jnp.where(c == 0, ahead, 2 * planes - 1 - ahead)


def place_kernel(me_ref, m0, m1, m2, m3, a_ref, b_ref):
    me = me_ref[0]
    planes, rows = m0.shape[1], m0.shape[2]
    for r, m in zip(ROUNDS, (m0, m1, m2, m3)):
        for i in range(planes):
            block, at = slot(me, r, planes, i)
            for flag, dst in ((1, a_ref), (0, b_ref)):

                @pl.when(block == flag)
                def _(dst=dst, m=m, i=i, at=at):
                    for k in range(2):
                        row_loop(rows, lambda s, k=k: dst.__setitem__((k, at, s), m[k, i, s]))


def edges(shape):
    col = lax.broadcasted_iota(jnp.int32, shape, 1)
    return col == 0, col == shape[1] - 1


def lap_rows(ref, s, r0, n, first, last):
    lo = HALO + r0
    mid = ref[s, lo : lo + n, :]
    width = mid.shape[1]
    beside = ref[s + 1, lo : lo + n, :] + ref[s - 1, lo : lo + n, :]
    beside = beside + (ref[s, lo + 1 : lo + n + 1, :] + ref[s, lo - 1 : lo + n - 1, :])
    right = jnp.where(last, 0.0, pltpu.roll(mid, width - 1, 1))
    left = jnp.where(first, 0.0, pltpu.roll(mid, 1, 1))
    return beside + (right + left) - 6.0 * mid, mid


def clear_rims(ref, rows):
    width = ref.shape[2]

    def one(s, carry):
        ref[s, :HALO, :] = jnp.zeros((HALO, width), F32)
        ref[s, HALO + rows :, :] = jnp.zeros((HALO, width), F32)
        return carry

    lax.fori_loop(0, ref.shape[0], one, 0)


def sequence(a_ref, b_ref, ra_ref, rb_ref, half):
    out = []
    for s in range(half):
        out.append((rb_ref, half - 1 - s, s))
        out.append((b_ref, s, half + s))
        out.append((a_ref, s, 2 * half + s))
        out.append((ra_ref, half - 1 - s, 3 * half + s))
    return out


CHUNK = 16


def forward_kernel(me_ref, a_ref, b_ref, ra_ref, rb_ref, u_out, c_out, slopes, u0, u1):
    half, rows = a_ref.shape[1], a_ref.shape[2]
    clear_rims(u0, rows)
    clear_rims(u1, rows)
    for src, at, s in sequence(a_ref, b_ref, ra_ref, rb_ref, half):

        def fill(t, carry, src=src, at=at, s=s):
            r = pl.multiple_of(t * 16, 8)
            u0[s, pl.ds(r + HALO, 16), :] = src[0, at, pl.ds(r, 16), :]
            c_out[s, pl.ds(r, 16), :] = time_step * src[1, at, pl.ds(r, 16), :]
            return carry

        lax.fori_loop(0, rows // 16, fill, 0)
    first, last = edges((CHUNK, a_ref.shape[3]))
    own = range(half, 3 * half)
    for k in range(ITERS):
        old, new = (u0, u1) if k % 2 == 0 else (u1, u0)
        wide = ITERS - 1 - k

        def plane(s, carry, k=k, old=old, new=new):
            keep = jnp.clip(s - half, 0, 2 * half - 1)
            for r0 in range(0, rows, CHUNK):
                slope, mid = lap_rows(old, s, r0, CHUNK, first, last)
                moved = mid + c_out[s, r0 : r0 + CHUNK, :] * slope
                if k == ITERS - 1:
                    u_out[s - half, r0 : r0 + CHUNK, :] = moved
                    slopes[k, s - half, r0 : r0 + CHUNK, :] = slope
                else:
                    new[s, HALO + r0 : HALO + r0 + CHUNK, :] = moved
                    slopes[k, keep, r0 : r0 + CHUNK, :] = slope
            return carry

        for lo, hi in ((own[0] - wide, own[0]), (own[-1] + 1, own[-1] + 1 + wide), (own[0], own[-1] + 1)):
            if hi > lo:
                lax.fori_loop(lo, hi, plane, 0)


def resid_kernel(me_ref, m0, m1, m2, m3, u_ref, a_ref, b_ref, total_ref, acc_ref):
    me = me_ref[0]
    planes, rows, width = m0.shape[1], m0.shape[2], m0.shape[3]
    acc_ref[...] = jnp.zeros((HALO, width), F32)
    for r, m in zip(ROUNDS, (m0, m1, m2, m3)):
        for i in range(planes):
            block, at = slot(me, r, planes, i)
            for flag, dst in ((1, a_ref), (0, b_ref)):

                @pl.when(block == flag)
                def _(m=m, i=i, at=at, dst=dst, flag=flag):
                    acc = acc_ref[...]
                    for lo in range(0, rows, HALO):
                        s = slice(lo, lo + HALO)
                        resid = u_ref[2 * planes * flag + at, s, :] - m[0, i, s, :]
                        weighted = m[1, i, s, :] * resid
                        dst[at, s, :] = weighted
                        if 0 < lo < rows - HALO:
                            acc = acc + weighted * resid
                    acc_ref[...] = acc

    total_ref[0, 0] = jnp.sum(acc_ref[...])


def backward_kernel(me_ref, part_ref, a_ref, b_ref, ra_ref, rb_ref, c_ref, slopes, o0, o1, o2, o3, lam, mv0, mv1, grad):
    me = me_ref[0]
    half, rows = a_ref.shape[0], a_ref.shape[1]
    inner = rows - 2 * HALO
    clear_rims(mv0, rows)
    clear_rims(mv1, rows)
    for src, at, s in sequence(a_ref, b_ref, ra_ref, rb_ref, half):

        def fill(t, carry, src=src, at=at, s=s):
            r = pl.multiple_of(t * 16, 8)
            v = src[at, pl.ds(r, 16), :]
            lam[s, pl.ds(r, 16), :] = v
            mv0[s, pl.ds(r + HALO, 16), :] = c_ref[s, pl.ds(r, 16), :] * v
            return carry

        lax.fori_loop(0, rows // 16, fill, 0)
    first, last = edges((CHUNK, a_ref.shape[2]))
    first8, last8 = edges((HALO, a_ref.shape[2]))
    own = range(half, 3 * half)
    for k in reversed(range(ITERS)):
        old, new = (mv0, mv1) if (ITERS - 1 - k) % 2 == 0 else (mv1, mv0)
        wide = k

        def halo_plane(s, carry, old=old, new=new):
            for r0 in range(0, rows, CHUNK):
                change, _ = lap_rows(old, s, r0, CHUNK, first, last)
                after = lam[s, r0 : r0 + CHUNK, :] + change
                lam[s, r0 : r0 + CHUNK, :] = after
                new[s, HALO + r0 : HALO + r0 + CHUNK, :] = c_ref[s, r0 : r0 + CHUNK, :] * after
            return carry

        def own_plane(s, carry, k=k, old=old, new=new):
            for r0 in range(HALO, rows - HALO, CHUNK):
                change, _ = lap_rows(old, s, r0, CHUNK, first, last)
                before = lam[s, r0 : r0 + CHUNK, :]
                g = before * slopes[k, s - half, r0 : r0 + CHUNK, :]
                at = slice(r0 - HALO, r0 - HALO + CHUNK)
                grad[s - half, at, :] = g if k == ITERS - 1 else grad[s - half, at, :] + g
                after = before + change
                lam[s, r0 : r0 + CHUNK, :] = after
                if k:
                    new[s, HALO + r0 : HALO + r0 + CHUNK, :] = c_ref[s, r0 : r0 + CHUNK, :] * after
            if k:
                for r0 in (0, rows - HALO):
                    change, _ = lap_rows(old, s, r0, HALO, first8, last8)
                    after = lam[s, r0 : r0 + HALO, :] + change
                    lam[s, r0 : r0 + HALO, :] = after
                    new[s, HALO + r0 : 2 * HALO + r0, :] = c_ref[s, r0 : r0 + HALO, :] * after
            return carry

        if wide:
            lax.fori_loop(own[0] - wide, own[0], halo_plane, 0)
            lax.fori_loop(own[-1] + 1, own[-1] + 1 + wide, halo_plane, 0)
        lax.fori_loop(own[0], own[-1] + 1, own_plane, 0)
    planes = half // 2
    for r, out in zip(ROUNDS, (o0, o1, o2, o3)):
        for i in range(planes):
            block, at = slot(me, r, planes, i)
            pos = half * block + at

            def one(t, carry, out=out, i=i, pos=pos):
                s = pl.multiple_of(t * 16, 8)
                out[0, i, pl.ds(s, 16), :] = grad[pos, pl.ds(s, 16), :]
                out[1, i, pl.ds(s, 16), :] = lam[half + pos, pl.ds(s + HALO, 16), :]
                return carry

            lax.fori_loop(0, inner // 16, one, 0)


def home_kernel(me_ref, scale_ref, m0, m1, m2, m3, g_ref, a_ref):
    _, x, c = bits(me_ref[0])
    planes, rows = m0.shape[1], m0.shape[2]
    for (r1, r0), m in zip(ROUNDS, (m0, m1, m2, m3)):
        start = part(c ^ r1, x ^ r0) * rows
        for k, out in enumerate((g_ref, a_ref)):
            scale = scale_ref[k]
            for i in range(planes):

                def one(t, carry, m=m, k=k, i=i, out=out, start=start, scale=scale):
                    s = pl.multiple_of(t * 16, 8)
                    out[i, pl.ds(pl.multiple_of(start + s, 8), 16), :] = m[k, i, pl.ds(s, 16), :] * scale
                    return carry

                lax.fori_loop(0, rows // 16, one, 0)


def shape(*dims):
    return jax.ShapeDtypeStruct(dims, F32)


def exchange_sum(value, axis, count, steps):
    for step in steps:
        value = value + lax.ppermute(value, axis, [(i, i ^ step) for i in range(count)])
    return value


def on_device(coefficient, initial_field, observed, misfit_weight):
    axis = "gz"
    count = lax.axis_size(axis)
    planes, height, width = coefficient.shape
    if count % GROUP or height % (16 * PARTS) or 2 * planes < ITERS or ITERS * 2 > HALO:
        raise ValueError("unsupported sizes")
    rows = height // PARTS
    tall = rows + 2 * HALO
    half = 2 * planes
    me = lax.axis_index(axis).astype(jnp.int32).reshape(1)

    partner = [(i, i ^ 1) for i in range(count)]
    beyond = []
    for i in range(count - GROUP + 1):
        if i % 2:
            if i + GROUP - 1 < count:
                beyond += [(i, i + GROUP - 1), (i + GROUP - 1, i)]

    def regroup(a, b):
        msgs = call(pack_kernel, [shape(2, planes, tall, width)] * 4, 2)(me, a, b)
        got = []
        for m, r in zip(msgs, ROUNDS):
            got.append(lax.ppermute(m, axis, send_pairs(count, *r)))
        return got

    first = regroup(initial_field, coefficient)
    second = regroup(observed, misfit_weight)

    pair = [shape(2, half, tall, width)] * 2
    blk_a, blk_b = call(place_kernel, pair, 4)(me, *first)
    far_a = lax.ppermute(blk_a, axis, partner)
    far_b = lax.ppermute(blk_b, axis, beyond)
    final, coef, slopes = call(
        forward_kernel,
        [shape(2 * half, tall, width), shape(4 * half, tall, width), shape(ITERS, 2 * half, tall, width)],
        4,
        [pltpu.VMEM((4 * half, tall + 2 * HALO, width), F32)] * 2,
    )(me, blk_a, blk_b, far_a, far_b)

    lam_a, lam_b, part_total = call(
        resid_kernel,
        [shape(half, tall, width)] * 2 + [shape(1, 1)],
        5,
        [pltpu.VMEM((HALO, width), F32)],
        out_specs=[VM, VM, SM],
    )(me, *second, final)
    far_la = lax.ppermute(lam_a, axis, partner)
    far_lb = lax.ppermute(lam_b, axis, beyond)
    near = [2, 4]
    far = [1] + [1 << k for k in range(3, count.bit_length() - 1)]
    part_total = exchange_sum(part_total, axis, count, near)
    outs = pl.pallas_call(
        backward_kernel,
        name="backward",
        out_shape=[shape(2, planes, rows, width)] * 4,
        in_specs=[SM, SM] + [VM] * 6,
        out_specs=[VM] * 4,
        compiler_params=PARAMS,
        scratch_shapes=[pltpu.VMEM((4 * half, tall, width), F32)]
        + [pltpu.VMEM((4 * half, tall + 2 * HALO, width), F32)] * 2
        + [pltpu.VMEM((2 * half, rows, width), F32)],
    )(me, part_total, lam_a, lam_b, far_la, far_lb, coef, slopes)
    back = [
        lax.ppermute(m, axis, [(j, i) for i, j in send_pairs(count, *r)]) for m, r in zip(outs, ROUNDS)
    ]

    if count & (count - 1):
        total = lax.psum(part_total, axis) / 4
    else:
        total = exchange_sum(part_total, axis, count, far)
    cells = count * planes * height * width
    misfit = jnp.sqrt(total[0, 0] / cells + 1e-06)
    inverse = 1.0 / misfit
    scale = jnp.stack([time_step * inverse, inverse])
    gradient, adjoint = pl.pallas_call(
        home_kernel,
        name="home",
        out_shape=[shape(planes, height, width)] * 2,
        in_specs=[SM, SM] + [VM] * 4,
        out_specs=[VM] * 2,
        compiler_params=PARAMS,
    )(me, scale, *back)
    return gradient, adjoint, misfit


def solution(mesh):
    placed = P("gz", None, None)
    return jax.shard_map(
        on_device,
        mesh=mesh,
        in_specs=(placed,) * 4,
        out_specs=(placed, placed, P()),
        check_vma=False,
    )
```

```python
import jax
import jax.numpy as jnp
from jax import lax
from jax.experimental import pallas as pl
from jax.experimental.pallas import tpu as pltpu
from jax.sharding import PartitionSpec as P


ITERS = 4
time_step = 0.125

GROUP = 8
PARTS = 4
HALO = 8
ROUNDS = ((0, 0), (0, 1), (1, 0), (1, 1))


VM = pl.BlockSpec(memory_space=pltpu.VMEM)
SM = pl.BlockSpec(memory_space=pltpu.SMEM)
PARAMS = pltpu.CompilerParams(vmem_limit_bytes=32 * 1024 * 1024)
F32 = jnp.float32


def call(kernel, outs, scalars, arrays, scratch=(), total=False, **options):
    return pl.pallas_call(
        kernel,
        out_shape=outs,
        in_specs=[SM] * len(scalars) + [VM] * len(arrays),
        out_specs=[VM] * (len(outs) - total) + [SM] * total,
        scratch_shapes=scratch,
        compiler_params=PARAMS,
        **options,
    )(*scalars, *arrays)


def inside(*arrays):
    return [pltpu.with_memory_space_constraint(a, pltpu.VMEM) for a in arrays]


def outside(*arrays):
    return [pltpu.with_memory_space_constraint(a, pltpu.HBM) for a in arrays]


def bits(me):
    return (me >> 2) & 1, (me >> 1) & 1, me & 1


def part(y, x):
    return 2 * y + x


def send_pairs(count, r1, r0):
    pairs = []
    for i in range(count):
        y, x, c = bits(i)
        pairs.append((i, (i & ~7) + 4 * (c ^ r1) + 2 * (x ^ r0) + y))
    return pairs


def row_loop(rows, body, step=16):
    def one(t, carry):
        body(pl.ds(pl.multiple_of(t * step, 8), step))
        return carry

    lax.fori_loop(0, rows // step, one, 0)


def pack_kernel(me_ref, a_ref, b_ref, *out_refs):
    _, x, c = bits(me_ref[0])
    height = a_ref.shape[1]
    rows = height // PARTS
    planes = a_ref.shape[0]
    for (r1, r0), out in zip(ROUNDS, out_refs):
        q = part(c ^ r1, x ^ r0)
        start = pl.multiple_of(q * rows, 8)
        above = pl.multiple_of(jnp.maximum(start - HALO, 0), 8)
        below = pl.multiple_of(jnp.minimum(start + rows, height - HALO), 8)
        for k, src in enumerate((a_ref, b_ref)):
            for i in range(planes):
                top = src[i, pl.ds(above, HALO), :]
                out[k, i, :HALO, :] = jnp.where(q > 0, top, 0.0)
                low = src[i, pl.ds(below, HALO), :]
                out[k, i, HALO + rows :, :] = jnp.where(q < PARTS - 1, low, 0.0)

                def one(t, carry, src=src, out=out, k=k, i=i, start=start):
                    at = pl.multiple_of(t * 16, 8)
                    out[k, i, pl.ds(at + HALO, 16), :] = src[i, pl.ds(pl.multiple_of(start + at, 8), 16), :]
                    return carry

                lax.fori_loop(0, rows // 16, one, 0, unroll=True)


def slot(me, r, planes, i):
    y, x, c = bits(me)
    r1, r0 = r
    from_c = y ^ r1
    block = x ^ r0 ^ c
    ahead = planes * from_c + i
    return block, jnp.where(c == 0, ahead, 2 * planes - 1 - ahead)


def place_kernel(me_ref, m0, m1, m2, m3, a_ref, b_ref):
    me = me_ref[0]
    planes, rows = m0.shape[1], m0.shape[2]
    for r, m in zip(ROUNDS, (m0, m1, m2, m3)):
        for i in range(planes):
            block, at = slot(me, r, planes, i)
            for flag, dst in ((1, a_ref), (0, b_ref)):

                @pl.when(block == flag)
                def _(dst=dst, m=m, i=i, at=at):
                    for k in range(2):
                        row_loop(rows, lambda s, k=k: dst.__setitem__((k, at, s), m[k, i, s]))


def edges(shape):
    col = lax.broadcasted_iota(jnp.int32, shape, 1)
    return col == 0, col == shape[1] - 1


def lap_rows(ref, s, r0, n, first, last):
    lo = HALO + r0
    mid = ref[s, lo : lo + n, :]
    width = mid.shape[1]
    beside = ref[s + 1, lo : lo + n, :] + ref[s - 1, lo : lo + n, :]
    beside = beside + (ref[s, lo + 1 : lo + n + 1, :] + ref[s, lo - 1 : lo + n - 1, :])
    right = jnp.where(last, 0.0, pltpu.roll(mid, width - 1, 1))
    left = jnp.where(first, 0.0, pltpu.roll(mid, 1, 1))
    return beside + (right + left) - 6.0 * mid, mid


def clear_rims(ref, rows):
    width = ref.shape[2]

    def one(s, carry):
        ref[s, :HALO, :] = jnp.zeros((HALO, width), F32)
        ref[s, HALO + rows :, :] = jnp.zeros((HALO, width), F32)
        return carry

    lax.fori_loop(0, ref.shape[0], one, 0)


CHUNK = 16


def copy_rows(rows, move):
    def one(t, carry):
        r = pl.multiple_of(t * CHUNK, 8)
        move(pl.ds(r, CHUNK), pl.ds(r + HALO, CHUNK))
        return carry

    lax.fori_loop(0, rows // CHUNK, one, 0)


def spans(lo, hi, body):
    if hi > lo:
        lax.fori_loop(lo, hi, body, 0)


def forward_main(me_ref, a_ref, b_ref, ra_ref, u_out, c_out, slopes, saved, u0, u1):
    half, rows = a_ref.shape[1], a_ref.shape[2]
    clear_rims(u0, rows)
    clear_rims(u1, rows)
    for i in range(half):
        for src, at, t in ((b_ref, i, i), (a_ref, i, half + i), (ra_ref, half - 1 - i, 2 * half + i)):

            def fill(r, rh, src=src, at=at, t=t):
                u0[t, rh, :] = src[0, at, r, :]
                c_out[t, r, :] = time_step * src[1, at, r, :]

            copy_rows(rows, fill)
    first, last = edges((CHUNK, a_ref.shape[3]))
    for k in range(ITERS):
        old, new = (u0, u1) if k % 2 == 0 else (u1, u0)

        def plane(t, carry, own, k=k, old=old, new=new):
            for r0 in range(0, rows, CHUNK):
                slope, mid = lap_rows(old, t, r0, CHUNK, first, last)
                moved = mid + c_out[t, r0 : r0 + CHUNK, :] * slope
                if own:
                    slopes[k, t, r0 : r0 + CHUNK, :] = slope
                if k == ITERS - 1:
                    u_out[t, r0 : r0 + CHUNK, :] = moved
                else:
                    new[t, HALO + r0 : HALO + r0 + CHUNK, :] = moved
            return carry

        spans(1 + k, 2 * half, lambda t, c: plane(t, c, True))
        spans(2 * half, 2 * half + ITERS - 1 - k, lambda t, c: plane(t, c, False))
        if k < ITERS - 1:
            for i in range(2):

                def keep(r, rh, k=k, i=i, new=new):
                    saved[k, i, r, :] = new[k + 1 + i, rh, :]

                copy_rows(rows, keep)


def forward_wedge(me_ref, b_ref, rb_ref, c_ref, saved, u_in, slopes_in, u_out, slopes, w0, w1, cw):
    half, rows = b_ref.shape[1], b_ref.shape[2]
    clear_rims(w0, rows)
    clear_rims(w1, rows)
    for i in range(half):

        def fill(r, rh, i=i):
            w0[i, rh, :] = rb_ref[0, half - 1 - i, r, :]
            cw[i, r, :] = time_step * rb_ref[1, half - 1 - i, r, :]

        copy_rows(rows, fill)
    for i in range(2):
        copy_rows(rows, lambda r, rh, i=i: w0.__setitem__((half + i, rh), b_ref[0, i, r, :]))
    first, last = edges((CHUNK, b_ref.shape[3]))
    for k in range(ITERS):
        old, new = (w0, w1) if k % 2 == 0 else (w1, w0)
        if k:
            for i in range(2):
                copy_rows(rows, lambda r, rh, i=i: old.__setitem__((half + k + i, rh), saved[k - 1, i, r, :]))

        def plane(s, carry, own, k=k, old=old, new=new):
            for r0 in range(0, rows, CHUNK):
                slope, mid = lap_rows(old, s, r0, CHUNK, first, last)
                at = slice(r0, r0 + CHUNK)
                coef = c_ref[s - half, at, :] if own else cw[s, at, :]
                moved = mid + coef * slope
                if own:
                    slopes[k, s - half, at, :] = slope
                if k == ITERS - 1:
                    u_out[s - half, at, :] = moved
                else:
                    new[s, HALO + r0 : HALO + r0 + CHUNK, :] = moved
            return carry

        spans(half - ITERS + 1 + k, half, lambda s, c: plane(s, c, False))
        spans(half, half + k + 1, lambda s, c: plane(s, c, True))


def resid_kernel(me_ref, m0, m1, m2, m3, u_ref, a_ref, b_ref, total_ref, acc_ref):
    me = me_ref[0]
    planes, rows, width = m0.shape[1], m0.shape[2], m0.shape[3]
    acc_ref[...] = jnp.zeros((HALO, width), F32)
    for r, m in zip(ROUNDS, (m0, m1, m2, m3)):
        for i in range(planes):
            block, at = slot(me, r, planes, i)
            for flag, dst in ((1, a_ref), (0, b_ref)):

                @pl.when(block == flag)
                def _(m=m, i=i, at=at, dst=dst, flag=flag):
                    acc = acc_ref[...]
                    for lo in range(0, rows, HALO):
                        s = slice(lo, lo + HALO)
                        resid = u_ref[2 * planes * flag + at, s, :] - m[0, i, s, :]
                        weighted = m[1, i, s, :] * resid
                        dst[at, s, :] = weighted
                        if 0 < lo < rows - HALO:
                            acc = acc + weighted * resid
                    acc_ref[...] = acc

    total_ref[0, 0] = jnp.sum(acc_ref[...])


def pack_block(me, g_first, l_first, grad, lam, outs):
    y, _, c = bits(me)
    planes, rows = outs[0].shape[1], outs[0].shape[2]
    for r1, out in enumerate(outs):
        for i in range(planes):
            ahead = planes * (y ^ r1) + i
            at = jnp.where(c == 0, ahead, 2 * planes - 1 - ahead)

            def one(t, carry, out=out, i=i, at=at):
                r = pl.multiple_of(t * CHUNK, 8)
                out[0, i, pl.ds(r, CHUNK), :] = grad[g_first + at, pl.ds(r, CHUNK), :]
                out[1, i, pl.ds(r, CHUNK), :] = lam[l_first + at, pl.ds(r + HALO, CHUNK), :]
                return carry

            lax.fori_loop(0, rows // CHUNK, one, 0, unroll=True)


def backward_main(me_ref, part_ref, a_ref, b_ref, ra_ref, c_ref, slopes, o0, o1, lam_out, grad_out, saved, lam, mv0, mv1, grad):
    half, rows = a_ref.shape[0], a_ref.shape[1]
    clear_rims(mv0, rows)
    clear_rims(mv1, rows)
    for i in range(half):
        for src, at, t in ((b_ref, i, i), (a_ref, i, half + i), (ra_ref, half - 1 - i, 2 * half + i)):

            def fill(r, rh, src=src, at=at, t=t):
                v = src[at, r, :]
                lam[t, r, :] = v
                mv0[t, rh, :] = c_ref[t, r, :] * v

            copy_rows(rows, fill)
    first, last = edges((CHUNK, a_ref.shape[2]))
    first8, last8 = edges((HALO, a_ref.shape[2]))

    for j in range(ITERS):
        k = ITERS - 1 - j
        old, new = (mv0, mv1) if j % 2 == 0 else (mv1, mv0)

        def gain(t, r0, j=j, k=k):
            g = lam[t, r0 : r0 + CHUNK, :] * slopes[k, t, r0 : r0 + CHUNK, :]
            at = slice(r0 - HALO, r0 - HALO + CHUNK)
            grad[t, at, :] = grad[t, at, :] + g if j else g

        def gain_plane(t, carry, gain=gain):
            for r0 in range(HALO, rows - HALO, CHUNK):
                gain(t, r0)
            return carry

        def step(t, r0, n, f, l, j=j, old=old, new=new):
            change, _ = lap_rows(old, t, r0, n, f, l)
            after = lam[t, r0 : r0 + n, :] + change
            lam[t, r0 : r0 + n, :] = after
            if j < ITERS - 1:
                new[t, HALO + r0 : HALO + r0 + n, :] = c_ref[t, r0 : r0 + n, :] * after

        def own_plane(t, carry, gain=gain, step=step, j=j):
            for r0 in range(HALO, rows - HALO, CHUNK):
                gain(t, r0)
                step(t, r0, CHUNK, first, last)
            if j < ITERS - 1:
                step(t, 0, HALO, first8, last8)
                step(t, rows - HALO, HALO, first8, last8)
            return carry

        def halo_plane(t, carry, step=step):
            for r0 in range(0, rows, CHUNK):
                step(t, r0, CHUNK, first, last)
            return carry

        gain_plane(j, 0)
        spans(1 + j, 2 * half, own_plane)
        spans(2 * half, 2 * half + ITERS - 1 - j, halo_plane)
        if j < ITERS - 1:
            for i in range(2):

                def keep(r, rh, j=j, i=i, new=new):
                    saved[j, i, r, :] = new[j + 1 + i, rh, :]

                copy_rows(rows, keep)
    pack_block(me_ref[0], half, half, grad, lam, (o0, o1))
    for i in range(half):
        copy_rows(rows, lambda r, rh, i=i: lam_out.__setitem__((i, r), lam[i, r, :]))

        def one(t, carry, i=i):
            r = pl.multiple_of(t * CHUNK, 8)
            grad_out[i, pl.ds(r, CHUNK), :] = grad[i, pl.ds(r, CHUNK), :]
            return carry

        lax.fori_loop(0, (rows - 2 * HALO) // CHUNK, one, 0)


def backward_wedge(me_ref, b_ref, rb_ref, far_ref, c_ref, slopes, saved, lam_in, grad_in, o0, o1, lam, cw, mv0, mv1, grad):
    half, rows = b_ref.shape[0], b_ref.shape[1]
    clear_rims(mv0, rows)
    clear_rims(mv1, rows)
    for i in range(half):

        def fill(r, rh, i=i):
            v = rb_ref[half - 1 - i, r, :]
            coef = time_step * far_ref[1, half - 1 - i, r, :]
            lam[i, r, :] = v
            cw[i, r, :] = coef
            mv0[i, rh, :] = coef * v
            lam[half + i, r, :] = lam_in[i, r, :]

        copy_rows(rows, fill)
        if i < 2:
            copy_rows(rows, lambda r, rh, i=i: mv0.__setitem__((half + i, rh), c_ref[i, r, :] * b_ref[i, r, :]))

        def one(t, carry, i=i):
            r = pl.multiple_of(t * CHUNK, 8)
            grad[i, pl.ds(r, CHUNK), :] = grad_in[i, pl.ds(r, CHUNK), :]
            return carry

        lax.fori_loop(0, (rows - 2 * HALO) // CHUNK, one, 0)
    first, last = edges((CHUNK, b_ref.shape[2]))
    for j in range(ITERS):
        k = ITERS - 1 - j
        old, new = (mv0, mv1) if j % 2 == 0 else (mv1, mv0)
        if j:
            for i in range(2):
                copy_rows(rows, lambda r, rh, i=i: old.__setitem__((half + j + i, rh), saved[j - 1, i, r, :]))

        def plane(s, carry, own, j=j, k=k, old=old, new=new):
            if own:
                for r0 in range(HALO, rows - HALO, CHUNK):

                    @pl.when(s < half + j)
                    def _(r0=r0):
                        at = slice(r0 - HALO, r0 - HALO + CHUNK)
                        g = lam[s, r0 : r0 + CHUNK, :] * slopes[k, s - half, r0 : r0 + CHUNK, :]
                        grad[s - half, at, :] = grad[s - half, at, :] + g

            for r0 in range(0, rows, CHUNK):
                change, _ = lap_rows(old, s, r0, CHUNK, first, last)
                at = slice(r0, r0 + CHUNK)
                after = lam[s, at, :] + change
                lam[s, at, :] = after
                if j < ITERS - 1:
                    coef = c_ref[s - half, at, :] if own else cw[s, at, :]
                    new[s, HALO + r0 : HALO + r0 + CHUNK, :] = coef * after
            return carry

        spans(half - ITERS + 1 + j, half, lambda s, c: plane(s, c, False))
        spans(half, half + j + 1, lambda s, c: plane(s, c, True))
    pack_block(me_ref[0], 0, half, grad, lam, (o0, o1))


def home_kernel(me_ref, scale_ref, *refs):
    msgs, (g_ref, a_ref) = refs[:-2], refs[-2:]
    y, x, c = bits(me_ref[0])
    planes, rows = msgs[0].shape[1], msgs[0].shape[2]
    for flag in (0, 1):

        @pl.when(x ^ y == flag)
        def _(flag=flag):
            for (r1, r0), m in zip(ROUNDS, msgs[4 * flag : 4 * flag + 4]):
                start = part(c ^ r1, x ^ r0) * rows
                for k, out in enumerate((g_ref, a_ref)):
                    scale = scale_ref[k]
                    for i in range(planes):

                        def one(t, carry, m=m, k=k, i=i, out=out, start=start, scale=scale):
                            s = pl.multiple_of(t * CHUNK, 8)
                            out[i, pl.ds(pl.multiple_of(start + s, 8), CHUNK), :] = m[k, i, pl.ds(s, CHUNK), :] * scale
                            return carry

                        lax.fori_loop(0, rows // CHUNK, one, 0, unroll=True)


def shape(*dims):
    return pltpu.VMEM(dims, F32)


def exchange_sum(value, axis, count, steps):
    for step in steps:
        value = value + lax.ppermute(value, axis, [(i, i ^ step) for i in range(count)])
    return value


def on_device(coefficient, initial_field, observed, misfit_weight):
    axis = "gz"
    count = lax.axis_size(axis)
    planes, height, width = coefficient.shape
    if count % GROUP or height % (16 * PARTS) or 2 * planes < ITERS or ITERS * 2 > HALO:
        raise ValueError("unsupported sizes")
    rows = height // PARTS
    tall = rows + 2 * HALO
    half = 2 * planes
    me = lax.axis_index(axis).astype(jnp.int32).reshape(1)

    partner = [(i, i ^ 1) for i in range(count)]
    beyond = []
    for i in range(count - GROUP + 1):
        if i % 2:
            if i + GROUP - 1 < count:
                beyond += [(i, i + GROUP - 1), (i + GROUP - 1, i)]

    def regroup(a, b):
        msgs = call(pack_kernel, [shape(2, planes, tall, width)] * 4, [me], [a, b])
        got = []
        for m, r in zip(msgs, ROUNDS):
            got.append(lax.ppermute(m, axis, send_pairs(count, *r)))
        return outside(*got)

    first = regroup(initial_field, coefficient)
    second = regroup(observed, misfit_weight)

    plane_set = (tall, width)
    padded = (tall + 2 * HALO, width)
    saved_shape = shape(ITERS - 1, 2, *plane_set)
    blk_a, blk_b = call(place_kernel, [shape(2, half, *plane_set)] * 2, [me], first)
    far_b = lax.ppermute(blk_b, axis, beyond)
    far_a = lax.ppermute(blk_a, axis, partner)
    (far_a,), (far_b,) = outside(far_a), outside(far_b)
    final, coef, slopes, saved = call(
        forward_main,
        [shape(2 * half, *plane_set), shape(3 * half, *plane_set), shape(ITERS, 2 * half, *plane_set), saved_shape],
        [me],
        inside(blk_a, blk_b) + [far_a],
        [pltpu.VMEM((3 * half, *padded), F32)] * 2,
    )
    final, slopes = call(
        forward_wedge,
        [shape(2 * half, *plane_set), shape(ITERS, 2 * half, *plane_set)],
        [me],
        inside(blk_b) + [far_b] + inside(coef, saved, final, slopes),
        [pltpu.VMEM((half + ITERS + 2, *padded), F32)] * 2 + [pltpu.VMEM((half, *plane_set), F32)],
        input_output_aliases={5: 0, 6: 1},
    )

    lam_a, lam_b, part_total = call(
        resid_kernel,
        [shape(half, *plane_set)] * 2 + [jax.ShapeDtypeStruct((1, 1), F32)],
        [me],
        second + inside(final),
        [pltpu.VMEM((HALO, width), F32)],
        total=True,
    )
    far_lb = lax.ppermute(lam_b, axis, beyond)
    far_la = lax.ppermute(lam_a, axis, partner)
    (far_la,), (far_lb,) = outside(far_la), outside(far_lb)
    near = [2, 4]
    far = [1] + [1 << k for k in range(3, count.bit_length() - 1)]
    part_total = exchange_sum(part_total, axis, count, near)
    msg = [shape(2, planes, rows, width)] * 2
    *outs_a, lam_left, grad_left, saved = call(
        backward_main,
        msg + [shape(half, *plane_set), shape(half, rows, width), saved_shape],
        [me, part_total],
        inside(lam_a, lam_b) + [far_la] + inside(coef, slopes),
        [pltpu.VMEM((3 * half, *plane_set), F32)]
        + [pltpu.VMEM((3 * half, *padded), F32)] * 2
        + [pltpu.VMEM((2 * half, rows, width), F32)],
    )

    def send_home(outs, block):
        got = {}
        for r1, r0 in sorted(ROUNDS, key=lambda r: (-r[1], r[0])):
            pairs = [(j, i) for i, j in send_pairs(count, r1, r0) if (i >> 1 ^ i >> 2) & 1 == block]
            got[r1, r0] = lax.ppermute(outs[r1], axis, pairs)
        return outside(*[got[r] for r in ROUNDS])

    back_a = send_home(outs_a, 1)
    outs_b = call(
        backward_wedge,
        msg,
        [me],
        inside(lam_b) + [far_lb, far_b] + inside(coef, slopes, saved, lam_left, grad_left),
        [pltpu.VMEM((2 * half, *plane_set), F32), pltpu.VMEM((half, *plane_set), F32)]
        + [pltpu.VMEM((half + ITERS + 2, *padded), F32)] * 2
        + [pltpu.VMEM((half, rows, width), F32)],
    )
    back_b = send_home(outs_b, 0)

    if count & (count - 1):
        total = lax.psum(part_total, axis) / 4
    else:
        total = exchange_sum(part_total, axis, count, far)
    cells = count * planes * height * width
    misfit = jnp.sqrt(total[0, 0] / cells + 1e-06)
    inverse = 1.0 / misfit
    scale = jnp.stack([time_step * inverse, inverse])
    gradient, adjoint = call(
        home_kernel, [jax.ShapeDtypeStruct((planes, height, width), F32)] * 2, [me, scale], back_b + back_a
    )
    return gradient, adjoint, misfit


def solution(mesh):
    placed = P("gz", None, None)
    return jax.shard_map(
        on_device,
        mesh=mesh,
        in_specs=(placed,) * 4,
        out_specs=(placed, placed, P()),
        check_vma=False,
    )
```

```python
import jax
import jax.numpy as jnp
from jax import lax
from jax.experimental import pallas as pl
from jax.experimental.pallas import tpu as pltpu
from jax.sharding import PartitionSpec as P


ITERS = 4
time_step = 0.125

GROUP = 8
PARTS = 4
HALO = 8
ROUNDS = ((0, 1), (0, 0), (1, 1), (1, 0))


VM = pl.BlockSpec(memory_space=pltpu.VMEM)
SM = pl.BlockSpec(memory_space=pltpu.SMEM)
PARAMS = pltpu.CompilerParams(vmem_limit_bytes=14 * 1024 * 1024)
F32 = jnp.float32


def call(kernel, outs, scalars, arrays, scratch=(), total=False, **options):
    return pl.pallas_call(
        kernel,
        out_shape=outs,
        in_specs=[SM] * len(scalars) + [VM] * len(arrays),
        out_specs=[VM] * (len(outs) - total) + [SM] * total,
        scratch_shapes=scratch,
        compiler_params=PARAMS,
        **options,
    )(*scalars, *arrays)


def inside(*arrays):
    return [pltpu.with_memory_space_constraint(a, pltpu.VMEM) for a in arrays]


def outside(*arrays):
    return [pltpu.with_memory_space_constraint(a, pltpu.HBM) for a in arrays]


def bits(me):
    return (me >> 2) & 1, (me >> 1) & 1, me & 1


def part(y, x):
    return 2 * y + x


def send_pairs(count, r1, r0):
    pairs = []
    for i in range(count):
        y, x, c = bits(i)
        pairs.append((i, (i & ~7) + 4 * (c ^ r1) + 2 * (x ^ r0) + y))
    return pairs


def pack_kernel(me_ref, a_ref, b_ref, *out_refs):
    _, x, c = bits(me_ref[0])
    height = a_ref.shape[1]
    rows = height // PARTS
    planes = a_ref.shape[0]
    for (r1, r0), out in zip(ROUNDS, out_refs):
        q = part(c ^ r1, x ^ r0)
        start = pl.multiple_of(q * rows, 8)
        above = pl.multiple_of(jnp.maximum(start - HALO, 0), 8)
        below = pl.multiple_of(jnp.minimum(start + rows, height - HALO), 8)
        for k, src in enumerate((a_ref, b_ref)):
            for i in range(planes):
                top = src[i, pl.ds(above, HALO), :]
                out[k, i, :HALO, :] = jnp.where(q > 0, top, 0.0)
                low = src[i, pl.ds(below, HALO), :]
                out[k, i, HALO + rows :, :] = jnp.where(q < PARTS - 1, low, 0.0)

                def one(t, carry, src=src, out=out, k=k, i=i, start=start):
                    at = pl.multiple_of(t * 16, 8)
                    out[k, i, pl.ds(at + HALO, 16), :] = src[i, pl.ds(pl.multiple_of(start + at, 8), 16), :]
                    return carry

                lax.fori_loop(0, rows // 16, one, 0, unroll=True)


def slot(me, r, planes, i):
    y, x, c = bits(me)
    r1, r0 = r
    from_c = y ^ r1
    block = x ^ r0 ^ c
    ahead = planes * from_c + i
    return block, jnp.where(c == 0, ahead, 2 * planes - 1 - ahead)


def early_kernel(me_ref, m0, m1, early_ref):
    me = me_ref[0]
    for r, m in zip(ROUNDS, (m0, m1)):
        block, _ = slot(me, r, m.shape[1], 0)

        @pl.when(block == 0)
        def _(m=m):
            early_ref[...] = m[...]


def place_kernel(me_ref, m0, m1, m2, m3, late_ref, a_ref, b_ref):
    me = me_ref[0]
    planes = m0.shape[1]
    for r, m in zip(ROUNDS, (m0, m1, m2, m3)):
        block, _ = slot(me, r, planes, 0)

        @pl.when(block == 0)
        def _(r=r, m=m):
            if r[0]:
                late_ref[...] = m[...]
            for i in range(planes):
                _, at = slot(me, r, planes, i)
                for k in range(2):
                    b_ref[k, at] = m[k, i]

        @pl.when(block == 1)
        def _(r=r, m=m):
            for i in range(planes):
                _, at = slot(me, r, planes, i)
                for k in range(2):
                    a_ref[k, at] = m[k, i]


def edges(shape):
    col = lax.broadcasted_iota(jnp.int32, shape, 1)
    return col == 0, col == shape[1] - 1


def lap_rows(ref, s, r0, n, first, last):
    lo = HALO + r0
    mid = ref[s, lo : lo + n, :]
    width = mid.shape[1]
    beside = ref[s + 1, lo : lo + n, :] + ref[s - 1, lo : lo + n, :]
    beside = beside + (ref[s, lo + 1 : lo + n + 1, :] + ref[s, lo - 1 : lo + n - 1, :])
    right = jnp.where(last, 0.0, pltpu.roll(mid, width - 1, 1))
    left = jnp.where(first, 0.0, pltpu.roll(mid, 1, 1))
    return beside + (right + left) - 6.0 * mid, mid


def clear_rims(ref, rows):
    width = ref.shape[2]

    def one(s, carry):
        ref[s, :HALO, :] = jnp.zeros((HALO, width), F32)
        ref[s, HALO + rows :, :] = jnp.zeros((HALO, width), F32)
        return carry

    lax.fori_loop(0, ref.shape[0], one, 0)


CHUNK = 16


def copy_rows(rows, move):
    def one(t, carry):
        r = pl.multiple_of(t * CHUNK, 8)
        move(pl.ds(r, CHUNK), pl.ds(r + HALO, CHUNK))
        return carry

    lax.fori_loop(0, rows // CHUNK, one, 0)


def spans(lo, hi, body):
    if hi > lo:
        lax.fori_loop(lo, hi, body, 0)


def forward_main(me_ref, a_ref, b_ref, ra_ref, u_out, c_out, slopes, saved, u0, u1):
    half, rows = a_ref.shape[1], a_ref.shape[2]
    clear_rims(u0, rows)
    clear_rims(u1, rows)
    for i in range(half):
        for src, at, t in ((b_ref, i, i), (a_ref, i, half + i), (ra_ref, half - 1 - i, 2 * half + i)):

            def fill(r, rh, src=src, at=at, t=t):
                u0[t, rh, :] = src[0, at, r, :]
                c_out[t, r, :] = time_step * src[1, at, r, :]

            copy_rows(rows, fill)
    first, last = edges((CHUNK, a_ref.shape[3]))
    for k in range(ITERS):
        old, new = (u0, u1) if k % 2 == 0 else (u1, u0)

        def plane(t, carry, own, k=k, old=old, new=new):
            for r0 in range(0, rows, CHUNK):
                slope, mid = lap_rows(old, t, r0, CHUNK, first, last)
                moved = mid + c_out[t, r0 : r0 + CHUNK, :] * slope
                if own:
                    slopes[k, t, r0 : r0 + CHUNK, :] = slope
                if k == ITERS - 1:
                    u_out[t, r0 : r0 + CHUNK, :] = moved
                else:
                    new[t, HALO + r0 : HALO + r0 + CHUNK, :] = moved
            return carry

        spans(1 + k, 2 * half, lambda t, c: plane(t, c, True))
        spans(2 * half, 2 * half + ITERS - 1 - k, lambda t, c: plane(t, c, False))
        if k < ITERS - 1:
            for i in range(2):

                def keep(r, rh, k=k, i=i, new=new):
                    saved[k, i, r, :] = new[k + 1 + i, rh, :]

                copy_rows(rows, keep)


def forward_wedge(me_ref, early, late, b_ref, c_ref, saved, u_in, slopes_in, u_out, slopes, cw, w0, w1):
    y, _, c = bits(me_ref[0])
    half, rows = b_ref.shape[1], b_ref.shape[2]
    planes = early.shape[1]
    clear_rims(w0, rows)
    clear_rims(w1, rows)
    for r1, far in enumerate((early, late)):
        for i in range(planes):
            ahead = planes * (y ^ r1) + i
            s = half - 1 - jnp.where(c == 1, ahead, half - 1 - ahead)

            def fill(r, rh, far=far, i=i, s=s):
                w0[s, rh, :] = far[0, i, r, :]
                cw[s, r, :] = time_step * far[1, i, r, :]

            copy_rows(rows, fill)
    for i in range(2):
        copy_rows(rows, lambda r, rh, i=i: w0.__setitem__((half + i, rh), b_ref[0, i, r, :]))
    first, last = edges((CHUNK, b_ref.shape[3]))
    for k in range(ITERS):
        old, new = (w0, w1) if k % 2 == 0 else (w1, w0)
        if k:
            for i in range(2):
                copy_rows(rows, lambda r, rh, i=i: old.__setitem__((half + k + i, rh), saved[k - 1, i, r, :]))

        def plane(s, carry, own, k=k, old=old, new=new):
            for r0 in range(0, rows, CHUNK):
                slope, mid = lap_rows(old, s, r0, CHUNK, first, last)
                at = slice(r0, r0 + CHUNK)
                coef = c_ref[s - half, at, :] if own else cw[s, at, :]
                moved = mid + coef * slope
                if own:
                    slopes[k, s - half, at, :] = slope
                if k == ITERS - 1:
                    u_out[s - half, at, :] = moved
                else:
                    new[s, HALO + r0 : HALO + r0 + CHUNK, :] = moved
            return carry

        spans(half - ITERS + 1 + k, half, lambda s, c: plane(s, c, False))
        spans(half, half + k + 1, lambda s, c: plane(s, c, True))


def resid_kernel(me_ref, m0, m1, m2, m3, u_ref, a_ref, b_ref, total_ref, acc_ref):
    me = me_ref[0]
    planes, rows, width = m0.shape[1], m0.shape[2], m0.shape[3]
    acc_ref[...] = jnp.zeros((HALO, width), F32)
    for r, m in zip(ROUNDS, (m0, m1, m2, m3)):
        for i in range(planes):
            block, at = slot(me, r, planes, i)
            for flag, dst in ((1, a_ref), (0, b_ref)):

                @pl.when(block == flag)
                def _(m=m, i=i, at=at, dst=dst, flag=flag):
                    acc = acc_ref[...]
                    for lo in range(0, rows, HALO):
                        s = slice(lo, lo + HALO)
                        resid = u_ref[2 * planes * flag + at, s, :] - m[0, i, s, :]
                        weighted = m[1, i, s, :] * resid
                        dst[at, s, :] = weighted
                        if 0 < lo < rows - HALO:
                            acc = acc + weighted * resid
                    acc_ref[...] = acc

    total_ref[0, 0] = jnp.sum(acc_ref[...])


def backward_main(me_ref, ra_ref, a_ref, b_ref, c_ref, slopes, lam, grad, saved, mv0, mv1):
    half, rows = a_ref.shape[0], a_ref.shape[1]
    clear_rims(mv0, rows)
    clear_rims(mv1, rows)
    for i in range(half):
        for src, at, t in ((b_ref, i, i), (a_ref, i, half + i), (ra_ref, half - 1 - i, 2 * half + i)):

            def fill(r, rh, src=src, at=at, t=t):
                v = src[at, r, :]
                lam[t, r, :] = v
                mv0[t, rh, :] = c_ref[t, r, :] * v

            copy_rows(rows, fill)
    first, last = edges((CHUNK, a_ref.shape[2]))
    first8, last8 = edges((HALO, a_ref.shape[2]))

    for j in range(ITERS):
        k = ITERS - 1 - j
        old, new = (mv0, mv1) if j % 2 == 0 else (mv1, mv0)

        def gain(t, r0, j=j, k=k):
            g = lam[t, r0 : r0 + CHUNK, :] * slopes[k, t, r0 : r0 + CHUNK, :]
            at = slice(r0 - HALO, r0 - HALO + CHUNK)
            grad[t, at, :] = grad[t, at, :] + g if j else g

        def gain_plane(t, carry, gain=gain):
            for r0 in range(HALO, rows - HALO, CHUNK):
                gain(t, r0)
            return carry

        def step(t, r0, n, f, l, j=j, old=old, new=new):
            change, _ = lap_rows(old, t, r0, n, f, l)
            after = lam[t, r0 : r0 + n, :] + change
            lam[t, r0 : r0 + n, :] = after
            if j < ITERS - 1:
                new[t, HALO + r0 : HALO + r0 + n, :] = c_ref[t, r0 : r0 + n, :] * after

        def own_plane(t, carry, gain=gain, step=step, j=j):
            for r0 in range(HALO, rows - HALO, CHUNK):
                gain(t, r0)
                step(t, r0, CHUNK, first, last)
            if j < ITERS - 1:
                step(t, 0, HALO, first8, last8)
                step(t, rows - HALO, HALO, first8, last8)
            return carry

        def halo_plane(t, carry, step=step):
            for r0 in range(0, rows, CHUNK):
                step(t, r0, CHUNK, first, last)
            return carry

        gain_plane(j, 0)
        spans(1 + j, 2 * half, own_plane)
        spans(2 * half, 2 * half + ITERS - 1 - j, halo_plane)
        if j < ITERS - 1:
            for i in range(2):

                def keep(r, rh, j=j, i=i, new=new):
                    saved[j, i, r, :] = new[j + 1 + i, rh, :]

                copy_rows(rows, keep)


def backward_wedge(me_ref, rb_ref, b_ref, cw, c_ref, slopes, saved, lam_in, grad_in, o0, o1, o2, o3, lam, mv0, mv1, grad):
    half, rows = b_ref.shape[0], b_ref.shape[1]
    clear_rims(mv0, rows)
    clear_rims(mv1, rows)
    for i in range(half):

        def fill(r, rh, i=i):
            v = rb_ref[half - 1 - i, r, :]
            lam[i, r, :] = v
            mv0[i, rh, :] = cw[i, r, :] * v
            lam[half + i, r, :] = lam_in[i, r, :]

        copy_rows(rows, fill)
        if i < 2:
            copy_rows(rows, lambda r, rh, i=i: mv0.__setitem__((half + i, rh), c_ref[i, r, :] * b_ref[i, r, :]))

        def one(t, carry, i=i):
            r = pl.multiple_of(t * CHUNK, 8)
            grad[i, pl.ds(r, CHUNK), :] = grad_in[i, pl.ds(r, CHUNK), :]
            return carry

        lax.fori_loop(0, (rows - 2 * HALO) // CHUNK, one, 0)
    first, last = edges((CHUNK, b_ref.shape[2]))
    for j in range(ITERS):
        k = ITERS - 1 - j
        old, new = (mv0, mv1) if j % 2 == 0 else (mv1, mv0)
        if j:
            for i in range(2):
                copy_rows(rows, lambda r, rh, i=i: old.__setitem__((half + j + i, rh), saved[j - 1, i, r, :]))

        def plane(s, carry, own, j=j, old=old, new=new):
            for r0 in range(0, rows, CHUNK):
                change, _ = lap_rows(old, s, r0, CHUNK, first, last)
                at = slice(r0, r0 + CHUNK)
                after = lam[s, at, :] + change
                if j < ITERS - 1:
                    coef = c_ref[s - half, at, :] if own else cw[s, at, :]
                    new[s, HALO + r0 : HALO + r0 + CHUNK, :] = coef * after
                lam[s, at, :] = after
            return carry

        def gain(s, carry, j=j, k=k):
            for r0 in range(HALO, rows - HALO, CHUNK):
                at = slice(r0 - HALO, r0 - HALO + CHUNK)
                g = lam[s, r0 : r0 + CHUNK, :] * slopes[k, s - half, r0 : r0 + CHUNK, :]
                grad[s - half, at, :] = grad[s - half, at, :] + g
            return carry

        spans(half, half + j, gain)
        spans(half - ITERS + 1 + j, half, lambda s, c: plane(s, c, False))
        spans(half, half + j + 1, lambda s, c: plane(s, c, True))
    me = me_ref[0]
    planes = half // 2
    for r, out in zip(ROUNDS, (o0, o1, o2, o3)):
        block, _ = slot(me, r, planes, 0)
        for flag, g_src, l_src in ((0, grad, lam), (1, grad_in, lam_in)):

            @pl.when(block == flag)
            def _(r=r, out=out, g_src=g_src, l_src=l_src):
                for i in range(planes):
                    _, at = slot(me, r, planes, i)
                    out[0, i] = g_src[at if g_src is grad else half + at]
                    out[1, i] = l_src[half + at, HALO : rows - HALO, :]


def home_kernel(me_ref, scale_ref, m0, m1, m2, m3, g_ref, a_ref):
    _, x, c = bits(me_ref[0])
    planes, rows = m0.shape[1], m0.shape[2]
    for (r1, r0), m in zip(ROUNDS, (m0, m1, m2, m3)):
        start = pl.multiple_of(part(c ^ r1, x ^ r0) * rows, 8)
        for k, out in enumerate((g_ref, a_ref)):
            for i in range(planes):
                out[i, pl.ds(start, rows), :] = m[k, i] * scale_ref[k]


def shape(*dims):
    return pltpu.VMEM(dims, F32)


def exchange_sum(value, axis, count, steps):
    for step in steps:
        value = value + lax.ppermute(value, axis, [(i, i ^ step) for i in range(count)])
    return value


def on_device(coefficient, initial_field, observed, misfit_weight):
    axis = "gz"
    count = lax.axis_size(axis)
    planes, height, width = coefficient.shape
    if count % GROUP or height % (16 * PARTS) or 2 * planes < ITERS or ITERS * 2 > HALO:
        raise ValueError("unsupported sizes")
    rows = height // PARTS
    tall = rows + 2 * HALO
    half = 2 * planes
    me = lax.axis_index(axis).astype(jnp.int32).reshape(1)

    partner = [(i, i ^ 1) for i in range(count)]
    beyond = []
    for i in range(count - GROUP + 1):
        if i % 2:
            if i + GROUP - 1 < count:
                beyond += [(i, i + GROUP - 1), (i + GROUP - 1, i)]

    def regroup(a, b):
        msgs = call(pack_kernel, [shape(2, planes, tall, width)] * 4, [me], [a, b])
        got = []
        for m, r in zip(msgs, ROUNDS):
            got.append(lax.ppermute(m, axis, send_pairs(count, *r)))
        return outside(*got)

    first = regroup(*outside(initial_field, coefficient))
    second = regroup(*outside(observed, misfit_weight))

    plane_set = (tall, width)
    padded = (tall + 2 * HALO, width)
    saved_shape = shape(ITERS - 1, 2, *plane_set)
    quarter = shape(2, planes, *plane_set)
    (early,) = call(early_kernel, [quarter], [me], first[:2])
    early = lax.ppermute(early, axis, beyond)
    late, blk_a, blk_b = call(place_kernel, [quarter] + [shape(2, half, *plane_set)] * 2, [me], first)
    late = lax.ppermute(late, axis, beyond)
    far_a = lax.ppermute(blk_a, axis, partner)
    far_a, early, late = outside(far_a, early, late)
    final, coef, slopes, saved = call(
        forward_main,
        [shape(2 * half, *plane_set), shape(3 * half, *plane_set), shape(ITERS, 2 * half, *plane_set), saved_shape],
        [me],
        inside(blk_a, blk_b) + [far_a],
        [pltpu.VMEM((3 * half, *padded), F32)] * 2,
    )
    final, slopes, far_coef = call(
        forward_wedge,
        [shape(2 * half, *plane_set), shape(ITERS, 2 * half, *plane_set), shape(half, *plane_set)],
        [me],
        [early, late] + inside(blk_b, coef, saved, final, slopes),
        [pltpu.VMEM((half + ITERS + 2, *padded), F32)] * 2,
        input_output_aliases={6: 0, 7: 1},
    )

    lam_a, lam_b, part_total = call(
        resid_kernel,
        [shape(half, *plane_set)] * 2 + [jax.ShapeDtypeStruct((1, 1), F32)],
        [me],
        second + inside(final),
        [pltpu.VMEM((HALO, width), F32)],
        total=True,
    )
    far_lb = lax.ppermute(lam_b, axis, beyond)
    far_la = lax.ppermute(lam_a, axis, partner)
    (far_la,), (far_lb,) = outside(far_la), outside(far_lb)
    far = [1] + [1 << k for k in range(3, count.bit_length() - 1)]
    part_total = exchange_sum(part_total, axis, count, [2])
    lam, grad, saved = call(
        backward_main,
        [shape(3 * half, *plane_set), shape(2 * half, rows, width), saved_shape],
        [me],
        [far_la] + inside(lam_a, lam_b, coef, slopes),
        [pltpu.VMEM((3 * half, *padded), F32)] * 2,
    )
    part_total = exchange_sum(part_total, axis, count, [4])
    outs = call(
        backward_wedge,
        [shape(2, planes, rows, width)] * 4,
        [me],
        [far_lb] + inside(lam_b, far_coef, coef, slopes, saved, lam, grad),
        [pltpu.VMEM((2 * half, *plane_set), F32)]
        + [pltpu.VMEM((half + ITERS + 2, *padded), F32)] * 2
        + [pltpu.VMEM((half, rows, width), F32)],
    )
    back = []
    for m, r in zip(outs, ROUNDS):
        back.append(lax.ppermute(m, axis, [(j, i) for i, j in send_pairs(count, *r)]))
    back = outside(*back)

    if count & (count - 1):
        total = lax.psum(part_total, axis) / 4
    else:
        total = exchange_sum(part_total, axis, count, far)
    cells = count * planes * height * width
    misfit = jnp.sqrt(total[0, 0] / cells + 1e-06)
    inverse = 1.0 / misfit
    scale = jnp.stack([time_step * inverse, inverse])
    gradient, adjoint = call(home_kernel, [jax.ShapeDtypeStruct((planes, height, width), F32)] * 2, [me, scale], back)
    return gradient, adjoint, misfit


def solution(mesh):
    placed = P("gz", None, None)
    return jax.shard_map(
        on_device,
        mesh=mesh,
        in_specs=(placed,) * 4,
        out_specs=(placed, placed, P()),
        check_vma=False,
    )
```

```python
from functools import partial

import jax
import jax.numpy as jnp
from jax import lax
from jax.experimental import pallas as pl
from jax.experimental.pallas import tpu as pltpu
from jax.sharding import PartitionSpec as P


ITERS = 4
time_step = 0.125

GROUP = 8
PARTS = 4
HALO = 8
LANES = 128
ROUNDS = ((0, 1), (0, 0), (1, 1), (1, 0))


VM = pl.BlockSpec(memory_space=pltpu.VMEM)
SM = pl.BlockSpec(memory_space=pltpu.SMEM)
PARAMS = pltpu.CompilerParams(vmem_limit_bytes=14 * 1024 * 1024)
F32 = jnp.float32


def call(kernel, outs, scalars, arrays, scratch=(), total=False, **options):
    return pl.pallas_call(
        kernel,
        out_shape=outs,
        in_specs=[SM] * len(scalars) + [VM] * len(arrays),
        out_specs=[VM] * (len(outs) - total) + [SM] * total,
        scratch_shapes=scratch,
        compiler_params=PARAMS,
        **options,
    )(*scalars, *arrays)


def inside(*arrays):
    return [pltpu.with_memory_space_constraint(a, pltpu.VMEM) for a in arrays]


def outside(*arrays):
    return [pltpu.with_memory_space_constraint(a, pltpu.HBM) for a in arrays]


def bits(me):
    return (me >> 2) & 1, (me >> 1) & 1, me & 1


def part(y, x):
    return 2 * y + x


def send_pairs(count, r1, r0):
    pairs = []
    for i in range(count):
        y, x, c = bits(i)
        pairs.append((i, (i & ~7) + 4 * (c ^ r1) + 2 * (x ^ r0) + y))
    return pairs


def pack_kernel(rim, me_ref, a_ref, b_ref, *out_refs):
    _, x, c = bits(me_ref[0])
    planes, height, width = a_ref.shape
    rows = height // PARTS
    for (r1, r0), out in zip(ROUNDS, out_refs):
        q = part(c ^ r1, x ^ r0)
        start = pl.multiple_of(q * rows, 8)
        above = pl.multiple_of(jnp.maximum(start - HALO, 0), 8)
        below = pl.multiple_of(jnp.minimum(start + rows, height - HALO), 8)
        for k, src in enumerate((a_ref, b_ref)):
            for i in range(planes):
                for b in range(width // LANES):
                    cols = slice(b * LANES, (b + 1) * LANES)
                    top = src[i, pl.ds(above, HALO), cols]
                    out[k, i, b, :rim, :] = jnp.where(q > 0, top[HALO - rim :], 0.0)
                    low = src[i, pl.ds(below, HALO), cols]
                    out[k, i, b, rim + rows :, :] = jnp.where(q < PARTS - 1, low[:rim], 0.0)
                    for at in range(0, rows, HALO):
                        here = pl.ds(pl.multiple_of(start + at, 8), HALO)
                        out[k, i, b, rim + at : rim + at + HALO, :] = src[i, here, cols]


def slot(me, r, planes, i):
    y, x, c = bits(me)
    r1, r0 = r
    from_c = y ^ r1
    block = x ^ r0 ^ c
    ahead = planes * from_c + i
    return block, jnp.where(c == 0, ahead, 2 * planes - 1 - ahead)


def early_kernel(me_ref, m0, m1, early_ref):
    me = me_ref[0]
    for r, m in zip(ROUNDS, (m0, m1)):
        block, _ = slot(me, r, m.shape[1], 0)

        @pl.when(block == 0)
        def _(m=m):
            early_ref[...] = m[...]


def place_kernel(me_ref, m0, m1, m2, m3, late_ref, a_ref, b_ref):
    me = me_ref[0]
    planes = m0.shape[1]
    for r, m in zip(ROUNDS, (m0, m1, m2, m3)):
        block, _ = slot(me, r, planes, 0)

        @pl.when(block == 0)
        def _(r=r, m=m):
            if r[0]:
                late_ref[...] = m[...]
            for i in range(planes):
                _, at = slot(me, r, planes, i)
                for k in range(2):
                    b_ref[k, at] = m[k, i]

        @pl.when(block == 1)
        def _(r=r, m=m):
            for i in range(planes):
                _, at = slot(me, r, planes, i)
                for k in range(2):
                    a_ref[k, at] = m[k, i]


def edges(shape):
    col = lax.broadcasted_iota(jnp.int32, shape, 2)
    return col == 0, col == shape[2] - 1


def lap_rows(ref, s, r0, n, first, last):
    lo = HALO + r0
    mid = ref[s, :, lo : lo + n, :]
    none = jnp.zeros((1,) + mid.shape[1:], F32)
    beside = ref[s + 1, :, lo : lo + n, :] + ref[s - 1, :, lo : lo + n, :]
    beside = beside + (ref[s, :, lo + 1 : lo + n + 1, :] + ref[s, :, lo - 1 : lo + n - 1, :])
    right = pltpu.roll(mid, LANES - 1, 2)
    right = jnp.where(last, jnp.concatenate([right[1:], none], axis=0), right)
    left = pltpu.roll(mid, 1, 2)
    left = jnp.where(first, jnp.concatenate([none, left[:-1]], axis=0), left)
    return beside + (right + left) - 6.0 * mid, mid


def clear_rims(ref, rows):
    none = jnp.zeros((ref.shape[1], HALO, LANES), F32)

    def one(s, carry):
        ref[s, :, :HALO, :] = none
        ref[s, :, HALO + rows :, :] = none
        return carry

    lax.fori_loop(0, ref.shape[0], one, 0)


CHUNK = 16


def copy_rows(rows, move):
    def one(t, carry):
        r = pl.multiple_of(t * CHUNK, 8)
        move(pl.ds(r, CHUNK), pl.ds(r + HALO, CHUNK))
        return carry

    lax.fori_loop(0, rows // CHUNK, one, 0)


def spans(lo, hi, body):
    if hi > lo:
        lax.fori_loop(lo, hi, body, 0)


def forward_main(me_ref, a_ref, b_ref, ra_ref, u_out, c_out, slopes, saved, u0, u1):
    half, blocks, rows = a_ref.shape[1:4]
    clear_rims(u0, rows)
    clear_rims(u1, rows)
    for i in range(half):
        for src, at, t in ((b_ref, i, i), (a_ref, i, half + i), (ra_ref, half - 1 - i, 2 * half + i)):

            def fill(r, rh, src=src, at=at, t=t):
                u0[t, :, rh, :] = src[0, at, :, r, :]
                c_out[t, :, r, :] = time_step * src[1, at, :, r, :]

            copy_rows(rows, fill)
    first, last = edges((blocks, CHUNK, LANES))
    for k in range(ITERS):
        old, new = (u0, u1) if k % 2 == 0 else (u1, u0)

        def plane(t, carry, own, k=k, old=old, new=new):
            for r0 in range(0, rows, CHUNK):
                slope, mid = lap_rows(old, t, r0, CHUNK, first, last)
                moved = mid + c_out[t, :, r0 : r0 + CHUNK, :] * slope
                if own:
                    slopes[k, t, :, r0 : r0 + CHUNK, :] = slope
                if k == ITERS - 1:
                    u_out[t, :, r0 : r0 + CHUNK, :] = moved
                else:
                    new[t, :, HALO + r0 : HALO + r0 + CHUNK, :] = moved
            return carry

        spans(1 + k, 2 * half, lambda t, c: plane(t, c, True))
        spans(2 * half, 2 * half + ITERS - 1 - k, lambda t, c: plane(t, c, False))
        if k < ITERS - 1:
            for i in range(2):

                def keep(r, rh, k=k, i=i, new=new):
                    saved[k, i, :, r, :] = new[k + 1 + i, :, rh, :]

                copy_rows(rows, keep)


def forward_wedge(me_ref, early, late, b_ref, c_ref, saved, u_in, slopes_in, u_out, slopes, cw, w0, w1):
    y, _, c = bits(me_ref[0])
    half, blocks, rows = b_ref.shape[1:4]
    planes = early.shape[1]
    clear_rims(w0, rows)
    clear_rims(w1, rows)
    for r1, far in enumerate((early, late)):
        for i in range(planes):
            ahead = planes * (y ^ r1) + i
            s = half - 1 - jnp.where(c == 1, ahead, half - 1 - ahead)

            def fill(r, rh, far=far, i=i, s=s):
                w0[s, :, rh, :] = far[0, i, :, r, :]
                cw[s, :, r, :] = time_step * far[1, i, :, r, :]

            copy_rows(rows, fill)
    for i in range(2):
        copy_rows(rows, lambda r, rh, i=i: w0.__setitem__((half + i, slice(None), rh), b_ref[0, i, :, r, :]))
    first, last = edges((blocks, CHUNK, LANES))
    for k in range(ITERS):
        old, new = (w0, w1) if k % 2 == 0 else (w1, w0)
        if k:
            for i in range(2):
                copy_rows(rows, lambda r, rh, i=i: old.__setitem__((half + k + i, slice(None), rh), saved[k - 1, i, :, r, :]))

        def plane(s, carry, own, k=k, old=old, new=new):
            for r0 in range(0, rows, CHUNK):
                slope, mid = lap_rows(old, s, r0, CHUNK, first, last)
                at = slice(r0, r0 + CHUNK)
                coef = c_ref[s - half, :, at, :] if own else cw[s, :, at, :]
                moved = mid + coef * slope
                if own:
                    slopes[k, s - half, :, at, :] = slope
                if k == ITERS - 1:
                    u_out[s - half, :, at, :] = moved
                else:
                    new[s, :, HALO + r0 : HALO + r0 + CHUNK, :] = moved
            return carry

        spans(half - ITERS + 1 + k, half, lambda s, c: plane(s, c, False))
        spans(half, half + k + 1, lambda s, c: plane(s, c, True))


def resid_kernel(me_ref, m0, m1, m2, m3, u_ref, a_ref, b_ref, total_ref, acc_ref):
    me = me_ref[0]
    planes, blocks, short = m0.shape[1:4]
    rows = u_ref.shape[2]
    rim = (rows - short) // 2
    shape = (blocks, HALO, LANES)
    row = lax.broadcasted_iota(jnp.int32, shape, 1)
    acc_ref[...] = jnp.zeros(shape, F32)
    for r, m in zip(ROUNDS, (m0, m1, m2, m3)):
        for i in range(planes):
            block, at = slot(me, r, planes, i)
            for flag, dst in ((1, a_ref), (0, b_ref)):

                @pl.when(block == flag)
                def _(m=m, i=i, at=at, dst=dst, flag=flag):
                    acc = acc_ref[...]
                    dst[at, :, :rim, :] = jnp.zeros((blocks, rim, LANES), F32)
                    dst[at, :, rows - rim :, :] = jnp.zeros((blocks, rim, LANES), F32)
                    for lo in range(0, short, HALO):
                        here = slice(lo + rim, lo + rim + HALO)
                        resid = u_ref[2 * planes * flag + at, :, here, :] - m[0, i, :, lo : lo + HALO, :]
                        weighted = m[1, i, :, lo : lo + HALO, :] * resid
                        dst[at, :, here, :] = weighted
                        share = weighted * resid
                        if lo + rim < HALO:
                            share = jnp.where(row >= HALO - rim, share, 0.0)
                        if lo + rim + HALO > rows - HALO:
                            share = jnp.where(row < HALO - rim, share, 0.0)
                        acc = acc + share
                    acc_ref[...] = acc

    total_ref[0, 0] = jnp.sum(acc_ref[...])


def backward_main(me_ref, ra_ref, a_ref, b_ref, c_ref, slopes, lam, grad, saved, mv0, mv1):
    half, blocks, rows = a_ref.shape[:3]
    clear_rims(mv0, rows)
    clear_rims(mv1, rows)
    for i in range(half):
        for src, at, t in ((b_ref, i, i), (a_ref, i, half + i), (ra_ref, half - 1 - i, 2 * half + i)):

            def fill(r, rh, src=src, at=at, t=t):
                v = src[at, :, r, :]
                lam[t, :, r, :] = v
                mv0[t, :, rh, :] = c_ref[t, :, r, :] * v

            copy_rows(rows, fill)
    first, last = edges((blocks, CHUNK, LANES))
    first8, last8 = edges((blocks, HALO, LANES))

    for j in range(ITERS):
        k = ITERS - 1 - j
        old, new = (mv0, mv1) if j % 2 == 0 else (mv1, mv0)

        def gain(t, r0, j=j, k=k):
            g = lam[t, :, r0 : r0 + CHUNK, :] * slopes[k, t, :, r0 : r0 + CHUNK, :]
            at = slice(r0 - HALO, r0 - HALO + CHUNK)
            grad[t, :, at, :] = grad[t, :, at, :] + g if j else g

        def gain_plane(t, carry, gain=gain):
            for r0 in range(HALO, rows - HALO, CHUNK):
                gain(t, r0)
            return carry

        def step(t, r0, n, f, l, j=j, old=old, new=new):
            change, _ = lap_rows(old, t, r0, n, f, l)
            after = lam[t, :, r0 : r0 + n, :] + change
            lam[t, :, r0 : r0 + n, :] = after
            if j < ITERS - 1:
                new[t, :, HALO + r0 : HALO + r0 + n, :] = c_ref[t, :, r0 : r0 + n, :] * after

        def own_plane(t, carry, gain=gain, step=step, j=j):
            for r0 in range(HALO, rows - HALO, CHUNK):
                gain(t, r0)
                step(t, r0, CHUNK, first, last)
            if j < ITERS - 1:
                step(t, 0, HALO, first8, last8)
                step(t, rows - HALO, HALO, first8, last8)
            return carry

        def halo_plane(t, carry, step=step):
            for r0 in range(0, rows, CHUNK):
                step(t, r0, CHUNK, first, last)
            return carry

        gain_plane(j, 0)
        spans(1 + j, 2 * half, own_plane)
        spans(2 * half, 2 * half + ITERS - 1 - j, halo_plane)
        if j < ITERS - 1:
            for i in range(2):

                def keep(r, rh, j=j, i=i, new=new):
                    saved[j, i, :, r, :] = new[j + 1 + i, :, rh, :]

                copy_rows(rows, keep)


def backward_wedge(me_ref, rb_ref, b_ref, cw, c_ref, slopes, saved, lam_in, grad_in, *refs):
    outs, (lam, mv0, mv1, grad) = refs[:-4], refs[-4:]
    half, blocks, rows = b_ref.shape[:3]
    clear_rims(mv0, rows)
    clear_rims(mv1, rows)
    for i in range(half):

        def fill(r, rh, i=i):
            v = rb_ref[half - 1 - i, :, r, :]
            lam[i, :, r, :] = v
            mv0[i, :, rh, :] = cw[i, :, r, :] * v
            lam[half + i, :, r, :] = lam_in[i, :, r, :]

        copy_rows(rows, fill)
        if i < 2:
            copy_rows(rows, lambda r, rh, i=i: mv0.__setitem__((half + i, slice(None), rh), c_ref[i, :, r, :] * b_ref[i, :, r, :]))

        def one(t, carry, i=i):
            r = pl.multiple_of(t * CHUNK, 8)
            grad[i, :, pl.ds(r, CHUNK), :] = grad_in[i, :, pl.ds(r, CHUNK), :]
            return carry

        lax.fori_loop(0, (rows - 2 * HALO) // CHUNK, one, 0)
    first, last = edges((blocks, CHUNK, LANES))
    for j in range(ITERS):
        k = ITERS - 1 - j
        old, new = (mv0, mv1) if j % 2 == 0 else (mv1, mv0)
        if j:
            for i in range(2):
                copy_rows(rows, lambda r, rh, i=i: old.__setitem__((half + j + i, slice(None), rh), saved[j - 1, i, :, r, :]))

        def plane(s, carry, own, j=j, old=old, new=new):
            for r0 in range(0, rows, CHUNK):
                change, _ = lap_rows(old, s, r0, CHUNK, first, last)
                at = slice(r0, r0 + CHUNK)
                after = lam[s, :, at, :] + change
                if j < ITERS - 1:
                    coef = c_ref[s - half, :, at, :] if own else cw[s, :, at, :]
                    new[s, :, HALO + r0 : HALO + r0 + CHUNK, :] = coef * after
                lam[s, :, at, :] = after
            return carry

        def gain(s, carry, j=j, k=k):
            for r0 in range(HALO, rows - HALO, CHUNK):
                at = slice(r0 - HALO, r0 - HALO + CHUNK)
                g = lam[s, :, r0 : r0 + CHUNK, :] * slopes[k, s - half, :, r0 : r0 + CHUNK, :]
                grad[s - half, :, at, :] = grad[s - half, :, at, :] + g
            return carry

        spans(half, half + j, gain)
        spans(half - ITERS + 1 + j, half, lambda s, c: plane(s, c, False))
        spans(half, half + j + 1, lambda s, c: plane(s, c, True))
    me = me_ref[0]
    planes = half // 2
    for n, r in enumerate(ROUNDS):
        block, _ = slot(me, r, planes, 0)
        for flag, g_src, l_src in ((0, grad, lam), (1, grad_in, lam_in)):

            @pl.when(block == flag)
            def _(n=n, r=r, g_src=g_src, l_src=l_src):
                for i in range(planes):
                    _, at = slot(me, r, planes, i)
                    outs[n][i] = g_src[at if g_src is grad else half + at]
                    outs[4 + n][i] = l_src[half + at, :, HALO : rows - HALO, :]


def home_kernel(me_ref, scale_ref, m0, m1, m2, m3, out):
    _, x, c = bits(me_ref[0])
    planes, blocks, rows = m0.shape[:3]
    scale = scale_ref[0, 0]
    for (r1, r0), m in zip(ROUNDS, (m0, m1, m2, m3)):
        start = pl.multiple_of(part(c ^ r1, x ^ r0) * rows, 8)
        for i in range(planes):
            for b in range(blocks):
                out[i, pl.ds(start, rows), b * LANES : (b + 1) * LANES] = m[i, b] * scale


def shape(*dims):
    return pltpu.VMEM(dims, F32)


def exchange_sum(value, axis, count, steps):
    for step in steps:
        value = value + lax.ppermute(value, axis, [(i, i ^ step) for i in range(count)])
    return value


def on_device(coefficient, initial_field, observed, misfit_weight):
    axis = "gz"
    count = lax.axis_size(axis)
    planes, height, width = coefficient.shape
    if count % GROUP or width % LANES or height % (16 * PARTS) or 2 * planes < ITERS or ITERS * 2 > HALO:
        raise ValueError("unsupported sizes")
    rows = height // PARTS
    tall = rows + 2 * HALO
    half = 2 * planes
    blocks = width // LANES
    me = lax.axis_index(axis).astype(jnp.int32).reshape(1)

    partner = [(i, i ^ 1) for i in range(count)]
    beyond = []
    for i in range(count - GROUP + 1):
        if i % 2:
            if i + GROUP - 1 < count:
                beyond += [(i, i + GROUP - 1), (i + GROUP - 1, i)]

    def regroup(a, b, rim):
        message = shape(2, planes, blocks, rows + 2 * rim, LANES)
        msgs = call(partial(pack_kernel, rim), [message] * 4, [me], [a, b])
        got = []
        for m, r in zip(msgs, ROUNDS):
            got.append(lax.ppermute(m, axis, send_pairs(count, *r)))
        return outside(*got)

    first = regroup(*outside(initial_field, coefficient), HALO)
    second = regroup(*outside(observed, misfit_weight), HALO - ITERS)

    plane_set = (blocks, tall, LANES)
    padded = (blocks, tall + 2 * HALO, LANES)
    inner = (blocks, rows, LANES)
    saved_shape = shape(ITERS - 1, 2, *plane_set)
    quarter = shape(2, planes, *plane_set)
    (early,) = call(early_kernel, [quarter], [me], first[:2])
    early = lax.ppermute(early, axis, beyond)
    late, blk_a, blk_b = call(place_kernel, [quarter] + [shape(2, half, *plane_set)] * 2, [me], first)
    late = lax.ppermute(late, axis, beyond)
    far_a = lax.ppermute(blk_a, axis, partner)
    far_a, early, late = outside(far_a, early, late)
    final, coef, slopes, saved = call(
        forward_main,
        [shape(2 * half, *plane_set), shape(3 * half, *plane_set), shape(ITERS, 2 * half, *plane_set), saved_shape],
        [me],
        inside(blk_a, blk_b) + [far_a],
        [pltpu.VMEM((3 * half, *padded), F32)] * 2,
    )
    final, slopes, far_coef = call(
        forward_wedge,
        [shape(2 * half, *plane_set), shape(ITERS, 2 * half, *plane_set), shape(half, *plane_set)],
        [me],
        [early, late] + inside(blk_b, coef, saved, final, slopes),
        [pltpu.VMEM((half + ITERS + 2, *padded), F32)] * 2,
        input_output_aliases={6: 0, 7: 1},
    )

    lam_a, lam_b, part_total = call(
        resid_kernel,
        [shape(half, *plane_set)] * 2 + [jax.ShapeDtypeStruct((1, 1), F32)],
        [me],
        second + inside(final),
        [pltpu.VMEM((blocks, HALO, LANES), F32)],
        total=True,
    )
    far_lb = lax.ppermute(lam_b, axis, beyond)
    far_la = lax.ppermute(lam_a, axis, partner)
    (far_la,), (far_lb,) = outside(far_la), outside(far_lb)
    far = [1] + [1 << k for k in range(3, count.bit_length() - 1)]
    part_total = exchange_sum(part_total, axis, count, [2])
    lam, grad, saved = call(
        backward_main,
        [shape(3 * half, *plane_set), shape(2 * half, *inner), saved_shape],
        [me],
        [far_la] + inside(lam_a, lam_b, coef, slopes),
        [pltpu.VMEM((3 * half, *padded), F32)] * 2,
    )
    part_total = exchange_sum(part_total, axis, count, [4])
    outs = call(
        backward_wedge,
        [shape(planes, *inner)] * 8,
        [me],
        [far_lb] + inside(lam_b, far_coef, coef, slopes, saved, lam, grad),
        [pltpu.VMEM((2 * half, *plane_set), F32)]
        + [pltpu.VMEM((half + ITERS + 2, *padded), F32)] * 2
        + [pltpu.VMEM((half, *inner), F32)],
    )
    back = []
    for m, r in zip(outs, ROUNDS * 2):
        back.append(lax.ppermute(m, axis, [(j, i) for i, j in send_pairs(count, *r)]))
    back = outside(*back)

    if count & (count - 1):
        total = lax.psum(part_total, axis) / 4
    else:
        total = exchange_sum(part_total, axis, count, far)
    cells = count * planes * height * width
    misfit = jnp.sqrt(total[0, 0] / cells + 1e-06)
    inverse = 1.0 / misfit
    whole = [jax.ShapeDtypeStruct((planes, height, width), F32)]
    (gradient,) = call(home_kernel, whole, [me, (time_step * inverse).reshape(1, 1)], back[:4])
    (adjoint,) = call(home_kernel, whole, [me, inverse.reshape(1, 1)], back[4:])
    return gradient, adjoint, misfit


def solution(mesh):
    placed = P("gz", None, None)
    return jax.shard_map(
        on_device,
        mesh=mesh,
        in_specs=(placed,) * 4,
        out_specs=(placed, placed, P()),
        check_vma=False,
    )
```

```python
from functools import partial

import jax
import jax.numpy as jnp
from jax import lax
from jax.experimental import pallas as pl
from jax.experimental.pallas import tpu as pltpu
from jax.sharding import PartitionSpec as P


ITERS = 4
time_step = 0.125

GROUP = 8
PARTS = 4
HALO = 8
LANES = 128
ROUNDS = ((0, 1), (0, 0), (1, 1), (1, 0))


VM = pl.BlockSpec(memory_space=pltpu.VMEM)
SM = pl.BlockSpec(memory_space=pltpu.SMEM)
ANY = pl.BlockSpec(memory_space=pl.ANY)
SHARE = {"forward_main": 30, "forward_wedge": 30, "backward_main": 14}
F32 = jnp.float32


def call(kernel, name, outs, scalars, arrays, scratch=(), total=False, far=0, **options):
    return pl.pallas_call(
        kernel,
        out_shape=outs,
        in_specs=[SM] * len(scalars) + [ANY] * far + [VM] * (len(arrays) - far),
        out_specs=[VM] * (len(outs) - total) + [SM] * total,
        scratch_shapes=scratch,
        compiler_params=pltpu.CompilerParams(vmem_limit_bytes=SHARE.get(name, 14) << 20),
        **options,
    )(*scalars, *arrays)


def inside(*arrays):
    return [pltpu.with_memory_space_constraint(a, pltpu.VMEM) for a in arrays]


def outside(*arrays):
    return [pltpu.with_memory_space_constraint(a, pltpu.HBM) for a in arrays]


def bits(me):
    return (me >> 2) & 1, (me >> 1) & 1, me & 1


def part(y, x):
    return 2 * y + x


def send_pairs(count, r1, r0):
    pairs = []
    for i in range(count):
        y, x, c = bits(i)
        pairs.append((i, (i & ~7) + 4 * (c ^ r1) + 2 * (x ^ r0) + y))
    return pairs


def pack_kernel(rim, me_ref, a_ref, b_ref, *out_refs):
    _, x, c = bits(me_ref[0])
    planes, height, width = a_ref.shape
    rows = height // PARTS
    for (r1, r0), out in zip(ROUNDS, out_refs):
        q = part(c ^ r1, x ^ r0)
        start = pl.multiple_of(q * rows, 8)
        above = pl.multiple_of(jnp.maximum(start - HALO, 0), 8)
        below = pl.multiple_of(jnp.minimum(start + rows, height - HALO), 8)
        for k, src in enumerate((a_ref, b_ref)):
            for i in range(planes):
                for b in range(width // LANES):
                    cols = slice(b * LANES, (b + 1) * LANES)
                    top = src[i, pl.ds(above, HALO), cols]
                    out[k, i, b, :rim, :] = jnp.where(q > 0, top[HALO - rim :], 0.0)
                    low = src[i, pl.ds(below, HALO), cols]
                    out[k, i, b, rim + rows :, :] = jnp.where(q < PARTS - 1, low[:rim], 0.0)
                    for at in range(0, rows, HALO):
                        here = pl.ds(pl.multiple_of(start + at, 8), HALO)
                        out[k, i, b, rim + at : rim + at + HALO, :] = src[i, here, cols]


def slot(me, r, planes, i):
    y, x, c = bits(me)
    r1, r0 = r
    from_c = y ^ r1
    block = x ^ r0 ^ c
    ahead = planes * from_c + i
    return block, jnp.where(c == 0, ahead, 2 * planes - 1 - ahead)


def early_kernel(me_ref, m0, m1, early_ref):
    me = me_ref[0]
    for r, m in zip(ROUNDS, (m0, m1)):
        block, _ = slot(me, r, m.shape[1], 0)

        @pl.when(block == 0)
        def _(m=m):
            early_ref[...] = m[...]


def place_kernel(me_ref, m0, m1, m2, m3, late_ref, a_ref, b_ref):
    me = me_ref[0]
    planes = m0.shape[1]
    for r, m in zip(ROUNDS, (m0, m1, m2, m3)):
        block, _ = slot(me, r, planes, 0)

        @pl.when(block == 0)
        def _(r=r, m=m):
            if r[0]:
                late_ref[...] = m[...]
            for i in range(planes):
                _, at = slot(me, r, planes, i)
                for k in range(2):
                    b_ref[k, at] = m[k, i]

        @pl.when(block == 1)
        def _(r=r, m=m):
            for i in range(planes):
                _, at = slot(me, r, planes, i)
                for k in range(2):
                    a_ref[k, at] = m[k, i]


def edges(shape):
    col = lax.broadcasted_iota(jnp.int32, shape, 2)
    return col == 0, col == shape[2] - 1


def lap_rows(ref, s, r0, n, first, last):
    lo = HALO + r0
    mid = ref[s, :, lo : lo + n, :]
    none = jnp.zeros((1,) + mid.shape[1:], F32)
    beside = ref[s + 1, :, lo : lo + n, :] + ref[s - 1, :, lo : lo + n, :]
    beside = beside + (ref[s, :, lo + 1 : lo + n + 1, :] + ref[s, :, lo - 1 : lo + n - 1, :])
    right = pltpu.roll(mid, LANES - 1, 2)
    right = jnp.where(last, jnp.concatenate([right[1:], none], axis=0), right)
    left = pltpu.roll(mid, 1, 2)
    left = jnp.where(first, jnp.concatenate([none, left[:-1]], axis=0), left)
    return beside + (right + left) - 6.0 * mid, mid


def clear_rims(ref, rows):
    none = jnp.zeros((ref.shape[1], HALO, LANES), F32)

    def one(s, carry):
        ref[s, :, :HALO, :] = none
        ref[s, :, HALO + rows :, :] = none
        return carry

    lax.fori_loop(0, ref.shape[0], one, 0)


CHUNK = 16


def copy_rows(rows, move):
    def one(t, carry):
        r = pl.multiple_of(t * CHUNK, 8)
        move(pl.ds(r, CHUNK), pl.ds(r + HALO, CHUNK))
        return carry

    lax.fori_loop(0, rows // CHUNK, one, 0)


def spans(lo, hi, body):
    if hi > lo:
        lax.fori_loop(lo, hi, body, 0)


def forward_main(me_ref, a_ref, b_ref, ra_ref, u_out, c_out, slopes, saved, u0, u1):
    half, blocks, rows = a_ref.shape[1:4]
    clear_rims(u0, rows)
    clear_rims(u1, rows)
    for i in range(half):
        for src, at, t in ((b_ref, i, i), (a_ref, i, half + i), (ra_ref, half - 1 - i, 2 * half + i)):

            def fill(r, rh, src=src, at=at, t=t):
                u0[t, :, rh, :] = src[0, at, :, r, :]
                c_out[t, :, r, :] = time_step * src[1, at, :, r, :]

            copy_rows(rows, fill)
    first, last = edges((blocks, CHUNK, LANES))
    for k in range(ITERS):
        old, new = (u0, u1) if k % 2 == 0 else (u1, u0)

        def plane(t, carry, own, k=k, old=old, new=new):
            for r0 in range(0, rows, CHUNK):
                slope, mid = lap_rows(old, t, r0, CHUNK, first, last)
                moved = mid + c_out[t, :, r0 : r0 + CHUNK, :] * slope
                if own:
                    slopes[k, t, :, r0 : r0 + CHUNK, :] = slope
                if k == ITERS - 1:
                    u_out[t, :, r0 : r0 + CHUNK, :] = moved
                else:
                    new[t, :, HALO + r0 : HALO + r0 + CHUNK, :] = moved
            return carry

        spans(1 + k, 2 * half, lambda t, c: plane(t, c, True))
        spans(2 * half, 2 * half + ITERS - 1 - k, lambda t, c: plane(t, c, False))
        if k < ITERS - 1:
            for i in range(2):

                def keep(r, rh, k=k, i=i, new=new):
                    saved[k, i, :, r, :] = new[k + 1 + i, :, rh, :]

                copy_rows(rows, keep)


def forward_wedge(me_ref, early, late, b_ref, c_ref, saved, u_in, slopes_in, u_out, slopes, cw, w0, w1):
    y, _, c = bits(me_ref[0])
    half, blocks, rows = b_ref.shape[1:4]
    planes = early.shape[1]
    clear_rims(w0, rows)
    clear_rims(w1, rows)
    for r1, far in enumerate((early, late)):
        for i in range(planes):
            ahead = planes * (y ^ r1) + i
            s = half - 1 - jnp.where(c == 1, ahead, half - 1 - ahead)

            def fill(r, rh, far=far, i=i, s=s):
                w0[s, :, rh, :] = far[0, i, :, r, :]
                cw[s, :, r, :] = time_step * far[1, i, :, r, :]

            copy_rows(rows, fill)
    for i in range(2):
        copy_rows(rows, lambda r, rh, i=i: w0.__setitem__((half + i, slice(None), rh), b_ref[0, i, :, r, :]))
    first, last = edges((blocks, CHUNK, LANES))
    for k in range(ITERS):
        old, new = (w0, w1) if k % 2 == 0 else (w1, w0)
        if k:
            for i in range(2):
                copy_rows(rows, lambda r, rh, i=i: old.__setitem__((half + k + i, slice(None), rh), saved[k - 1, i, :, r, :]))

        def plane(s, carry, own, k=k, old=old, new=new):
            for r0 in range(0, rows, CHUNK):
                slope, mid = lap_rows(old, s, r0, CHUNK, first, last)
                at = slice(r0, r0 + CHUNK)
                coef = c_ref[s - half, :, at, :] if own else cw[s, :, at, :]
                moved = mid + coef * slope
                if own:
                    slopes[k, s - half, :, at, :] = slope
                if k == ITERS - 1:
                    u_out[s - half, :, at, :] = moved
                else:
                    new[s, :, HALO + r0 : HALO + r0 + CHUNK, :] = moved
            return carry

        spans(half - ITERS + 1 + k, half, lambda s, c: plane(s, c, False))
        spans(half, half + k + 1, lambda s, c: plane(s, c, True))


def resid_kernel(me_ref, f0, f1, f2, f3, u_ref, a_ref, b_ref, total_ref, acc_ref, near, sems):
    me = me_ref[0]
    copies = [pltpu.make_async_copy(f, near.at[n], sems.at[n]) for n, f in enumerate((f0, f1, f2, f3))]
    for copy in copies:
        copy.start()
    planes, blocks, short = near.shape[2:5]
    rows = u_ref.shape[2]
    rim = (rows - short) // 2
    shape = (blocks, HALO, LANES)
    row = lax.broadcasted_iota(jnp.int32, shape, 1)
    acc_ref[...] = jnp.zeros(shape, F32)
    for n, r in enumerate(ROUNDS):
        copies[n].wait()
        for i in range(planes):
            block, at = slot(me, r, planes, i)
            for flag, dst in ((1, a_ref), (0, b_ref)):

                @pl.when(block == flag)
                def _(n=n, i=i, at=at, dst=dst, flag=flag):
                    dst[at, :, :rim, :] = jnp.zeros((blocks, rim, LANES), F32)
                    dst[at, :, rows - rim :, :] = jnp.zeros((blocks, rim, LANES), F32)
                    acc = jnp.zeros(shape, F32)
                    for lo in range(0, short, HALO):
                        here = slice(lo + rim, lo + rim + HALO)
                        resid = u_ref[2 * planes * flag + at, :, here, :] - near[n, 0, i, :, lo : lo + HALO, :]
                        weighted = near[n, 1, i, :, lo : lo + HALO, :] * resid
                        dst[at, :, here, :] = weighted
                        share = weighted * resid
                        if lo + rim < HALO:
                            share = jnp.where(row >= HALO - rim, share, 0.0)
                        if lo + rim + HALO > rows - HALO:
                            share = jnp.where(row < HALO - rim, share, 0.0)
                        acc = acc + share
                    acc_ref[...] = acc_ref[...] + acc

    total_ref[0, 0] = jnp.sum(acc_ref[...])


def backward_main(me_ref, ra_ref, a_ref, b_ref, c_ref, slopes, lam, grad, saved, mv0, mv1):
    half, blocks, rows = a_ref.shape[:3]
    clear_rims(mv0, rows)
    clear_rims(mv1, rows)
    for i in range(half):
        for src, at, t in ((b_ref, i, i), (a_ref, i, half + i), (ra_ref, half - 1 - i, 2 * half + i)):

            def fill(r, rh, src=src, at=at, t=t):
                v = src[at, :, r, :]
                lam[t, :, r, :] = v
                mv0[t, :, rh, :] = c_ref[t, :, r, :] * v

            copy_rows(rows, fill)
    first, last = edges((blocks, CHUNK, LANES))
    first8, last8 = edges((blocks, HALO, LANES))

    for j in range(ITERS):
        k = ITERS - 1 - j
        old, new = (mv0, mv1) if j % 2 == 0 else (mv1, mv0)

        def gain(t, r0, j=j, k=k):
            g = lam[t, :, r0 : r0 + CHUNK, :] * slopes[k, t, :, r0 : r0 + CHUNK, :]
            at = slice(r0 - HALO, r0 - HALO + CHUNK)
            grad[t, :, at, :] = grad[t, :, at, :] + g if j else g

        def gain_plane(t, carry, gain=gain):
            for r0 in range(HALO, rows - HALO, CHUNK):
                gain(t, r0)
            return carry

        def step(t, r0, n, f, l, j=j, old=old, new=new):
            change, _ = lap_rows(old, t, r0, n, f, l)
            after = lam[t, :, r0 : r0 + n, :] + change
            lam[t, :, r0 : r0 + n, :] = after
            if j < ITERS - 1:
                new[t, :, HALO + r0 : HALO + r0 + n, :] = c_ref[t, :, r0 : r0 + n, :] * after

        def own_plane(t, carry, gain=gain, step=step, j=j):
            for r0 in range(HALO, rows - HALO, CHUNK):
                gain(t, r0)
                step(t, r0, CHUNK, first, last)
            if j < ITERS - 1:
                step(t, 0, HALO, first8, last8)
                step(t, rows - HALO, HALO, first8, last8)
            return carry

        def halo_plane(t, carry, step=step):
            for r0 in range(0, rows, CHUNK):
                step(t, r0, CHUNK, first, last)
            return carry

        gain_plane(j, 0)
        spans(1 + j, 2 * half, own_plane)
        spans(2 * half, 2 * half + ITERS - 1 - j, halo_plane)
        if j < ITERS - 1:
            for i in range(2):

                def keep(r, rh, j=j, i=i, new=new):
                    saved[j, i, :, r, :] = new[j + 1 + i, :, rh, :]

                copy_rows(rows, keep)


def backward_wedge(me_ref, rb_ref, b_ref, cw, c_ref, slopes, saved, lam_in, grad_in, *refs):
    outs, (lam, mv0, mv1, grad) = refs[:-4], refs[-4:]
    half, blocks, rows = b_ref.shape[:3]
    clear_rims(mv0, rows)
    clear_rims(mv1, rows)
    for i in range(half):

        def fill(r, rh, i=i):
            v = rb_ref[half - 1 - i, :, r, :]
            lam[i, :, r, :] = v
            mv0[i, :, rh, :] = cw[i, :, r, :] * v
            lam[half + i, :, r, :] = lam_in[i, :, r, :]

        copy_rows(rows, fill)
        if i < 2:
            copy_rows(rows, lambda r, rh, i=i: mv0.__setitem__((half + i, slice(None), rh), c_ref[i, :, r, :] * b_ref[i, :, r, :]))

        def one(t, carry, i=i):
            r = pl.multiple_of(t * CHUNK, 8)
            grad[i, :, pl.ds(r, CHUNK), :] = grad_in[i, :, pl.ds(r, CHUNK), :]
            return carry

        lax.fori_loop(0, (rows - 2 * HALO) // CHUNK, one, 0)
    first, last = edges((blocks, CHUNK, LANES))
    for j in range(ITERS):
        k = ITERS - 1 - j
        old, new = (mv0, mv1) if j % 2 == 0 else (mv1, mv0)
        if j:
            for i in range(2):
                copy_rows(rows, lambda r, rh, i=i: old.__setitem__((half + j + i, slice(None), rh), saved[j - 1, i, :, r, :]))

        def plane(s, carry, own, j=j, old=old, new=new):
            for r0 in range(0, rows, CHUNK):
                change, _ = lap_rows(old, s, r0, CHUNK, first, last)
                at = slice(r0, r0 + CHUNK)
                after = lam[s, :, at, :] + change
                if j < ITERS - 1:
                    coef = c_ref[s - half, :, at, :] if own else cw[s, :, at, :]
                    new[s, :, HALO + r0 : HALO + r0 + CHUNK, :] = coef * after
                lam[s, :, at, :] = after
            return carry

        def gain(s, carry, j=j, k=k):
            for r0 in range(HALO, rows - HALO, CHUNK):
                at = slice(r0 - HALO, r0 - HALO + CHUNK)
                g = lam[s, :, r0 : r0 + CHUNK, :] * slopes[k, s - half, :, r0 : r0 + CHUNK, :]
                grad[s - half, :, at, :] = grad[s - half, :, at, :] + g
            return carry

        spans(half, half + j, gain)
        spans(half - ITERS + 1 + j, half, lambda s, c: plane(s, c, False))
        spans(half, half + j + 1, lambda s, c: plane(s, c, True))
    me = me_ref[0]
    planes = half // 2
    for n, r in enumerate(ROUNDS):
        block, _ = slot(me, r, planes, 0)
        for flag, g_src, l_src in ((0, grad, lam), (1, grad_in, lam_in)):

            @pl.when(block == flag)
            def _(n=n, r=r, g_src=g_src, l_src=l_src):
                for i in range(planes):
                    _, at = slot(me, r, planes, i)
                    outs[n][i] = g_src[at if g_src is grad else half + at]
                    outs[4 + n][i] = l_src[half + at, :, HALO : rows - HALO, :]


def home_kernel(rounds, me_ref, scale_ref, *refs):
    count = len(rounds)
    msgs, (out, near, ready, sems, done) = refs[:count], refs[-5:]
    _, x, c = bits(me_ref[0])
    planes, blocks, rows = near.shape[1:4]
    scale = scale_ref[0, 0]
    come = [pltpu.make_async_copy(m, near.at[n], sems.at[n]) for n, m in enumerate(msgs)]
    for copy in come:
        copy.start()
    go = []
    for n, (r1, r0) in enumerate(rounds):
        start = pl.multiple_of(part(c ^ r1, x ^ r0) * rows, 8)
        come[n].wait()
        for i in range(planes):
            for b in range(blocks):
                ready[n, i, :, b * LANES : (b + 1) * LANES] = near[n, i, b] * scale
        go.append(pltpu.make_async_copy(ready.at[n], out.at[:, pl.ds(start, rows), :], done.at[n]))
        go[-1].start()
    for copy in go:
        copy.wait()


def shape(*dims):
    return pltpu.VMEM(dims, F32)


def exchange_sum(value, axis, count, steps):
    for step in steps:
        value = value + lax.ppermute(value, axis, [(i, i ^ step) for i in range(count)])
    return value


def on_device(coefficient, initial_field, observed, misfit_weight):
    axis = "gz"
    count = lax.axis_size(axis)
    planes, height, width = coefficient.shape
    if count % GROUP or width % LANES or height % (16 * PARTS) or 2 * planes < ITERS or ITERS * 2 > HALO:
        raise ValueError("unsupported sizes")
    rows = height // PARTS
    tall = rows + 2 * HALO
    half = 2 * planes
    blocks = width // LANES
    me = lax.axis_index(axis).astype(jnp.int32).reshape(1)

    partner = [(i, i ^ 1) for i in range(count)]
    beyond = []
    for i in range(count - GROUP + 1):
        if i % 2:
            if i + GROUP - 1 < count:
                beyond += [(i, i + GROUP - 1), (i + GROUP - 1, i)]

    def regroup(a, b, rim, name):
        message = shape(2, planes, blocks, rows + 2 * rim, LANES)
        msgs = call(partial(pack_kernel, rim), name, [message] * 4, [me], [a, b])
        got = []
        for m, r in zip(msgs, ROUNDS):
            got.append(lax.ppermute(m, axis, send_pairs(count, *r)))
        return outside(*got)

    first = regroup(*outside(initial_field, coefficient), HALO, "pack_state")
    second = regroup(*outside(observed, misfit_weight), HALO - ITERS, "pack_data")

    plane_set = (blocks, tall, LANES)
    padded = (blocks, tall + 2 * HALO, LANES)
    inner = (blocks, rows, LANES)
    saved_shape = shape(ITERS - 1, 2, *plane_set)
    quarter = shape(2, planes, *plane_set)
    (early,) = call(early_kernel, "early", [quarter], [me], first[:2])
    early = lax.ppermute(early, axis, beyond)
    late, blk_a, blk_b = call(place_kernel, "place", [quarter] + [shape(2, half, *plane_set)] * 2, [me], first)
    late = lax.ppermute(late, axis, beyond)
    far_a = lax.ppermute(blk_a, axis, partner)
    far_a, early, late = outside(far_a, early, late)
    final, coef, slopes, saved = call(
        forward_main,
        "forward_main",
        [shape(2 * half, *plane_set), shape(3 * half, *plane_set), shape(ITERS, 2 * half, *plane_set), saved_shape],
        [me],
        inside(blk_a, blk_b) + [far_a],
        [pltpu.VMEM((3 * half, *padded), F32)] * 2,
    )
    final, slopes, far_coef = call(
        forward_wedge,
        "forward_wedge",
        [shape(2 * half, *plane_set), shape(ITERS, 2 * half, *plane_set), shape(half, *plane_set)],
        [me],
        [early, late] + inside(blk_b, coef, saved, final, slopes),
        [pltpu.VMEM((half + ITERS + 2, *padded), F32)] * 2,
        input_output_aliases={6: 0, 7: 1},
    )

    lam_a, lam_b, part_total = call(
        resid_kernel,
        "resid",
        [shape(half, *plane_set)] * 2 + [jax.ShapeDtypeStruct((1, 1), F32)],
        [me],
        second + inside(final),
        [
            pltpu.VMEM((blocks, HALO, LANES), F32),
            pltpu.VMEM((4,) + second[0].shape, F32),
            pltpu.SemaphoreType.DMA((4,)),
        ],
        total=True,
        far=4,
    )
    far_lb = lax.ppermute(lam_b, axis, beyond)
    far_la = lax.ppermute(lam_a, axis, partner)
    (far_la,), (far_lb,) = outside(far_la), outside(far_lb)
    far = [1] + [1 << k for k in range(3, count.bit_length() - 1)]
    part_total = exchange_sum(part_total, axis, count, [2])
    lam, grad, saved = call(
        backward_main,
        "backward_main",
        [shape(3 * half, *plane_set), shape(2 * half, *inner), saved_shape],
        [me],
        [far_la] + inside(lam_a, lam_b, coef, slopes),
        [pltpu.VMEM((3 * half, *padded), F32)] * 2,
    )
    part_total = exchange_sum(part_total, axis, count, [4])
    outs = call(
        backward_wedge,
        "backward_wedge",
        [shape(planes, *inner)] * 8,
        [me],
        [far_lb] + inside(lam_b, far_coef, coef, slopes, saved, lam, grad),
        [pltpu.VMEM((2 * half, *plane_set), F32)]
        + [pltpu.VMEM((half + ITERS + 2, *padded), F32)] * 2
        + [pltpu.VMEM((half, *inner), F32)],
    )
    back = []
    for m, r in zip(outs, ROUNDS * 2):
        back.append(lax.ppermute(m, axis, [(j, i) for i, j in send_pairs(count, *r)]))
    back = outside(*back)

    if count & (count - 1):
        total = lax.psum(part_total, axis) / 4
    else:
        total = exchange_sum(part_total, axis, count, far)
    cells = count * planes * height * width
    misfit = jnp.sqrt(total[0, 0] / cells + 1e-06)
    inverse = 1.0 / misfit

    def assemble(scale, msgs):
        held = ()
        for n in range(0, 4, 2):
            held = pl.pallas_call(
                partial(home_kernel, ROUNDS[n : n + 2]),
                out_shape=[jax.ShapeDtypeStruct((planes, height, width), F32)],
                in_specs=[SM, SM, ANY, ANY] + [ANY] * len(held),
                out_specs=[ANY],
                scratch_shapes=[
                    pltpu.VMEM((2, planes, *inner), F32),
                    pltpu.VMEM((2, planes, rows, width), F32),
                    pltpu.SemaphoreType.DMA((2,)),
                    pltpu.SemaphoreType.DMA((2,)),
                ],
                input_output_aliases={4: 0} if held else {},
                compiler_params=pltpu.CompilerParams(vmem_limit_bytes=14 << 20),
            )(me, scale.reshape(1, 1), *msgs[n : n + 2], *held)
        return held[0]

    gradient = assemble(time_step * inverse, back[:4])
    adjoint = assemble(inverse, back[4:])
    return gradient, adjoint, misfit


def solution(mesh):
    placed = P("gz", None, None)
    return jax.shard_map(
        on_device,
        mesh=mesh,
        in_specs=(placed,) * 4,
        out_specs=(placed, placed, P()),
        check_vma=False,
    )
```

```python
from functools import partial

import jax
import jax.numpy as jnp
from jax import lax
from jax.experimental import pallas as pl
from jax.experimental.pallas import tpu as pltpu
from jax.sharding import PartitionSpec as P


ITERS = 4
time_step = 0.125

GROUP = 8
PARTS = 4
HALO = 8
LANES = 128
ROUNDS = ((0, 1), (0, 0), (1, 1), (1, 0))


VM = pl.BlockSpec(memory_space=pltpu.VMEM)
SM = pl.BlockSpec(memory_space=pltpu.SMEM)
ANY = pl.BlockSpec(memory_space=pl.ANY)
SHARE = {"forward_main": 30, "forward_wedge": 30, "backward_main": 14}
F32 = jnp.float32


def call(kernel, name, outs, scalars, arrays, scratch=(), total=False, far=0, **options):
    return pl.pallas_call(
        kernel,
        out_shape=outs,
        in_specs=[SM] * len(scalars) + [ANY] * far + [VM] * (len(arrays) - far),
        out_specs=[VM] * (len(outs) - total) + [SM] * total,
        scratch_shapes=scratch,
        compiler_params=pltpu.CompilerParams(vmem_limit_bytes=SHARE.get(name, 14) << 20),
        **options,
    )(*scalars, *arrays)


def inside(*arrays):
    return [pltpu.with_memory_space_constraint(a, pltpu.VMEM) for a in arrays]


def outside(*arrays):
    return [pltpu.with_memory_space_constraint(a, pltpu.HBM) for a in arrays]


def bits(me):
    return (me >> 2) & 1, (me >> 1) & 1, me & 1


def part(y, x):
    return 2 * y + x


def send_pairs(count, r1, r0):
    pairs = []
    for i in range(count):
        y, x, c = bits(i)
        pairs.append((i, (i & ~7) + 4 * (c ^ r1) + 2 * (x ^ r0) + y))
    return pairs


def pack_kernel(rim, me_ref, a_ref, b_ref, *out_refs):
    _, x, c = bits(me_ref[0])
    planes, height, width = a_ref.shape
    rows = height // PARTS
    for (r1, r0), out in zip(ROUNDS, out_refs):
        q = part(c ^ r1, x ^ r0)
        start = pl.multiple_of(q * rows, 8)
        above = pl.multiple_of(jnp.maximum(start - HALO, 0), 8)
        below = pl.multiple_of(jnp.minimum(start + rows, height - HALO), 8)
        for k, src in enumerate((a_ref, b_ref)):
            for i in range(planes):
                for b in range(width // LANES):
                    cols = slice(b * LANES, (b + 1) * LANES)
                    top = src[i, pl.ds(above, HALO), cols]
                    out[k, i, b, :rim, :] = jnp.where(q > 0, top[HALO - rim :], 0.0)
                    low = src[i, pl.ds(below, HALO), cols]
                    out[k, i, b, rim + rows :, :] = jnp.where(q < PARTS - 1, low[:rim], 0.0)
                    for at in range(0, rows, HALO):
                        here = pl.ds(pl.multiple_of(start + at, 8), HALO)
                        out[k, i, b, rim + at : rim + at + HALO, :] = src[i, here, cols]


def slot(me, r, planes, i):
    y, x, c = bits(me)
    r1, r0 = r
    from_c = y ^ r1
    block = x ^ r0 ^ c
    ahead = planes * from_c + i
    return block, jnp.where(c == 0, ahead, 2 * planes - 1 - ahead)


def early_kernel(me_ref, m0, m1, early_ref):
    me = me_ref[0]
    for r, m in zip(ROUNDS, (m0, m1)):
        block, _ = slot(me, r, m.shape[1], 0)

        @pl.when(block == 0)
        def _(m=m):
            early_ref[...] = m[...]


def place_kernel(me_ref, m0, m1, m2, m3, late_ref, a_ref, b_ref):
    me = me_ref[0]
    planes = m0.shape[1]
    for r, m in zip(ROUNDS, (m0, m1, m2, m3)):
        block, _ = slot(me, r, planes, 0)

        @pl.when(block == 0)
        def _(r=r, m=m):
            if r[0]:
                late_ref[...] = m[...]
            for i in range(planes):
                _, at = slot(me, r, planes, i)
                for k in range(2):
                    b_ref[k, at] = m[k, i]

        @pl.when(block == 1)
        def _(r=r, m=m):
            for i in range(planes):
                _, at = slot(me, r, planes, i)
                for k in range(2):
                    a_ref[k, at] = m[k, i]


def edges(shape):
    col = lax.broadcasted_iota(jnp.int32, shape, 2)
    return col == 0, col == shape[2] - 1


def lap_rows(ref, s, r0, n, first, last):
    lo = HALO + r0
    mid = ref[s, :, lo : lo + n, :]
    none = jnp.zeros((1,) + mid.shape[1:], F32)
    beside = ref[s + 1, :, lo : lo + n, :] + ref[s - 1, :, lo : lo + n, :]
    beside = beside + (ref[s, :, lo + 1 : lo + n + 1, :] + ref[s, :, lo - 1 : lo + n - 1, :])
    right = pltpu.roll(mid, LANES - 1, 2)
    right = jnp.where(last, jnp.concatenate([right[1:], none], axis=0), right)
    left = pltpu.roll(mid, 1, 2)
    left = jnp.where(first, jnp.concatenate([none, left[:-1]], axis=0), left)
    return beside + (right + left) - 6.0 * mid, mid


def clear_rims(ref, rows):
    none = jnp.zeros((ref.shape[1], HALO, LANES), F32)

    def one(s, carry):
        ref[s, :, :HALO, :] = none
        ref[s, :, HALO + rows :, :] = none
        return carry

    lax.fori_loop(0, ref.shape[0], one, 0)


CHUNK = 16


def copy_rows(rows, move):
    def one(t, carry):
        r = pl.multiple_of(t * CHUNK, 8)
        move(pl.ds(r, CHUNK), pl.ds(r + HALO, CHUNK))
        return carry

    lax.fori_loop(0, rows // CHUNK, one, 0)


def spans(lo, hi, body):
    if hi > lo:
        lax.fori_loop(lo, hi, body, 0)


def forward_main(me_ref, a_ref, b_ref, ra_ref, u_out, c_out, slopes, saved, u0, u1):
    half, blocks, rows = a_ref.shape[1:4]
    clear_rims(u0, rows)
    clear_rims(u1, rows)
    for i in range(half):
        for src, at, t in ((b_ref, i, i), (a_ref, i, half + i), (ra_ref, half - 1 - i, 2 * half + i)):

            def fill(r, rh, src=src, at=at, t=t):
                u0[t, :, rh, :] = src[0, at, :, r, :]
                c_out[t, :, r, :] = time_step * src[1, at, :, r, :]

            copy_rows(rows, fill)
    first, last = edges((blocks, CHUNK, LANES))
    for k in range(ITERS):
        old, new = (u0, u1) if k % 2 == 0 else (u1, u0)

        def plane(t, carry, own, k=k, old=old, new=new):
            for r0 in range(0, rows, CHUNK):
                slope, mid = lap_rows(old, t, r0, CHUNK, first, last)
                moved = mid + c_out[t, :, r0 : r0 + CHUNK, :] * slope
                if own:
                    slopes[k, t, :, r0 : r0 + CHUNK, :] = slope
                if k == ITERS - 1:
                    u_out[t, :, r0 : r0 + CHUNK, :] = moved
                else:
                    new[t, :, HALO + r0 : HALO + r0 + CHUNK, :] = moved
            return carry

        spans(1 + k, 2 * half, lambda t, c: plane(t, c, True))
        spans(2 * half, 2 * half + ITERS - 1 - k, lambda t, c: plane(t, c, False))
        if k < ITERS - 1:
            for i in range(2):

                def keep(r, rh, k=k, i=i, new=new):
                    saved[k, i, :, r, :] = new[k + 1 + i, :, rh, :]

                copy_rows(rows, keep)


def forward_wedge(me_ref, early, late, b_ref, c_ref, saved, u_in, slopes_in, u_out, slopes, cw, w0, w1):
    y, _, c = bits(me_ref[0])
    half, blocks, rows = b_ref.shape[1:4]
    planes = early.shape[1]
    clear_rims(w0, rows)
    clear_rims(w1, rows)
    for r1, far in enumerate((early, late)):
        for i in range(planes):
            ahead = planes * (y ^ r1) + i
            s = half - 1 - jnp.where(c == 1, ahead, half - 1 - ahead)

            def fill(r, rh, far=far, i=i, s=s):
                w0[s, :, rh, :] = far[0, i, :, r, :]
                cw[s, :, r, :] = time_step * far[1, i, :, r, :]

            copy_rows(rows, fill)
    for i in range(2):
        copy_rows(rows, lambda r, rh, i=i: w0.__setitem__((half + i, slice(None), rh), b_ref[0, i, :, r, :]))
    first, last = edges((blocks, CHUNK, LANES))
    for k in range(ITERS):
        old, new = (w0, w1) if k % 2 == 0 else (w1, w0)
        if k:
            for i in range(2):
                copy_rows(rows, lambda r, rh, i=i: old.__setitem__((half + k + i, slice(None), rh), saved[k - 1, i, :, r, :]))

        def plane(s, carry, own, k=k, old=old, new=new):
            for r0 in range(0, rows, CHUNK):
                slope, mid = lap_rows(old, s, r0, CHUNK, first, last)
                at = slice(r0, r0 + CHUNK)
                coef = c_ref[s - half, :, at, :] if own else cw[s, :, at, :]
                moved = mid + coef * slope
                if own:
                    slopes[k, s - half, :, at, :] = slope
                if k == ITERS - 1:
                    u_out[s - half, :, at, :] = moved
                else:
                    new[s, :, HALO + r0 : HALO + r0 + CHUNK, :] = moved
            return carry

        spans(half - ITERS + 1 + k, half, lambda s, c: plane(s, c, False))
        spans(half, half + k + 1, lambda s, c: plane(s, c, True))


def resid_kernel(me_ref, f0, f1, f2, f3, u_ref, a_ref, b_ref, total_ref, acc_ref, near, sems):
    me = me_ref[0]
    copies = [pltpu.make_async_copy(f, near.at[n], sems.at[n]) for n, f in enumerate((f0, f1, f2, f3))]
    for copy in copies:
        copy.start()
    planes, blocks, short = near.shape[2:5]
    rows = u_ref.shape[2]
    rim = (rows - short) // 2
    shape = (blocks, HALO, LANES)
    row = lax.broadcasted_iota(jnp.int32, shape, 1)
    acc_ref[...] = jnp.zeros(shape, F32)
    for n, r in enumerate(ROUNDS):
        copies[n].wait()
        for i in range(planes):
            block, at = slot(me, r, planes, i)
            for flag, dst in ((1, a_ref), (0, b_ref)):

                @pl.when(block == flag)
                def _(n=n, i=i, at=at, dst=dst, flag=flag):
                    dst[at, :, :rim, :] = jnp.zeros((blocks, rim, LANES), F32)
                    dst[at, :, rows - rim :, :] = jnp.zeros((blocks, rim, LANES), F32)
                    acc = jnp.zeros(shape, F32)
                    for lo in range(0, short, HALO):
                        here = slice(lo + rim, lo + rim + HALO)
                        resid = u_ref[2 * planes * flag + at, :, here, :] - near[n, 0, i, :, lo : lo + HALO, :]
                        weighted = near[n, 1, i, :, lo : lo + HALO, :] * resid
                        dst[at, :, here, :] = weighted
                        share = weighted * resid
                        if lo + rim < HALO:
                            share = jnp.where(row >= HALO - rim, share, 0.0)
                        if lo + rim + HALO > rows - HALO:
                            share = jnp.where(row < HALO - rim, share, 0.0)
                        acc = acc + share
                    acc_ref[...] = acc_ref[...] + acc

    total_ref[0, 0] = jnp.sum(acc_ref[...])


def backward_main(me_ref, ra_ref, a_ref, b_ref, c_ref, slopes, lam, grad, saved, mv0, mv1):
    half, blocks, rows = a_ref.shape[:3]
    clear_rims(mv0, rows)
    clear_rims(mv1, rows)
    for i in range(half):
        for src, at, t in ((b_ref, i, i), (a_ref, i, half + i), (ra_ref, half - 1 - i, 2 * half + i)):

            def fill(r, rh, src=src, at=at, t=t):
                v = src[at, :, r, :]
                lam[t, :, r, :] = v
                mv0[t, :, rh, :] = c_ref[t, :, r, :] * v

            copy_rows(rows, fill)
    first, last = edges((blocks, CHUNK, LANES))
    first8, last8 = edges((blocks, HALO, LANES))

    for j in range(ITERS):
        k = ITERS - 1 - j
        old, new = (mv0, mv1) if j % 2 == 0 else (mv1, mv0)

        def gain(t, r0, j=j, k=k):
            g = lam[t, :, r0 : r0 + CHUNK, :] * slopes[k, t, :, r0 : r0 + CHUNK, :]
            at = slice(r0 - HALO, r0 - HALO + CHUNK)
            grad[t, :, at, :] = grad[t, :, at, :] + g if j else g

        def gain_plane(t, carry, gain=gain):
            for r0 in range(HALO, rows - HALO, CHUNK):
                gain(t, r0)
            return carry

        def step(t, r0, n, f, l, j=j, old=old, new=new):
            change, _ = lap_rows(old, t, r0, n, f, l)
            after = lam[t, :, r0 : r0 + n, :] + change
            lam[t, :, r0 : r0 + n, :] = after
            if j < ITERS - 1:
                new[t, :, HALO + r0 : HALO + r0 + n, :] = c_ref[t, :, r0 : r0 + n, :] * after

        def own_plane(t, carry, gain=gain, step=step, j=j):
            for r0 in range(HALO, rows - HALO, CHUNK):
                gain(t, r0)
                step(t, r0, CHUNK, first, last)
            if j < ITERS - 1:
                step(t, 0, HALO, first8, last8)
                step(t, rows - HALO, HALO, first8, last8)
            return carry

        def halo_plane(t, carry, step=step):
            for r0 in range(0, rows, CHUNK):
                step(t, r0, CHUNK, first, last)
            return carry

        gain_plane(j, 0)
        spans(1 + j, 2 * half, own_plane)
        spans(2 * half, 2 * half + ITERS - 1 - j, halo_plane)
        if j < ITERS - 1:
            for i in range(2):

                def keep(r, rh, j=j, i=i, new=new):
                    saved[j, i, :, r, :] = new[j + 1 + i, :, rh, :]

                copy_rows(rows, keep)


def backward_wedge(off, me_ref, rb_ref, b_ref, cw, c_ref, slopes, saved, lam_in, grad_in, o0, o1, o2, o3, lam, mv0, mv1, grad):
    inner = o0.shape[3]
    rows = inner + 2 * HALO
    half, blocks = b_ref.shape[:2]
    clear_rims(mv0, rows)
    clear_rims(mv1, rows)

    def there(r):
        return pl.ds(pl.multiple_of(r.start + off, 8), r.size)

    for i in range(half):

        def fill(r, rh, i=i):
            v = rb_ref[half - 1 - i, :, there(r), :]
            lam[i, :, r, :] = v
            mv0[i, :, rh, :] = cw[i, :, there(r), :] * v
            lam[half + i, :, r, :] = lam_in[i, :, there(r), :]
            if i < 2:
                mv0[half + i, :, rh, :] = c_ref[i, :, there(r), :] * b_ref[i, :, there(r), :]

        copy_rows(rows, fill)
        copy_rows(inner, lambda r, rh, i=i: grad.__setitem__((i, slice(None), r), grad_in[i, :, there(r), :]))
    first, last = edges((blocks, CHUNK, LANES))
    for j in range(ITERS):
        k = ITERS - 1 - j
        old, new = (mv0, mv1) if j % 2 == 0 else (mv1, mv0)
        if j:
            for i in range(2):

                def recall(r, rh, j=j, i=i, old=old):
                    old[half + j + i, :, rh, :] = saved[j - 1, i, :, there(r), :]

                copy_rows(rows, recall)

        def plane(s, carry, own, j=j, old=old, new=new):
            for r0 in range(0, rows, CHUNK):
                change, _ = lap_rows(old, s, r0, CHUNK, first, last)
                after = lam[s, :, r0 : r0 + CHUNK, :] + change
                if j < ITERS - 1:
                    at = slice(off + r0, off + r0 + CHUNK)
                    coef = c_ref[s - half, :, at, :] if own else cw[s, :, at, :]
                    new[s, :, HALO + r0 : HALO + r0 + CHUNK, :] = coef * after
                lam[s, :, r0 : r0 + CHUNK, :] = after
            return carry

        def gain(s, carry, k=k):
            for r0 in range(HALO, rows - HALO, CHUNK):
                at = slice(r0 - HALO, r0 - HALO + CHUNK)
                g = lam[s, :, r0 : r0 + CHUNK, :] * slopes[k, s - half, :, off + r0 : off + r0 + CHUNK, :]
                grad[s - half, :, at, :] = grad[s - half, :, at, :] + g
            return carry

        spans(half, half + j, gain)
        spans(half - ITERS + 1 + j, half, lambda s, c: plane(s, c, False))
        spans(half, half + j + 1, lambda s, c: plane(s, c, True))
    me = me_ref[0]
    planes = half // 2
    for r, out in zip(ROUNDS, (o0, o1, o2, o3)):
        block, _ = slot(me, r, planes, 0)

        @pl.when(block == 0)
        def _(r=r, out=out):
            for i in range(planes):
                _, at = slot(me, r, planes, i)
                out[0, i] = grad[at]
                out[1, i] = lam[half + at, :, HALO : HALO + inner, :]

        @pl.when(block == 1)
        def _(r=r, out=out):
            for i in range(planes):
                _, at = slot(me, r, planes, i)
                out[0, i] = grad_in[half + at, :, off : off + inner, :]
                out[1, i] = lam_in[half + at, :, off + HALO : off + HALO + inner, :]


def home_kernel(off, rounds, me_ref, scale_ref, *refs):
    count = len(rounds)
    msgs, (g_out, a_out, near, ready, sems, done) = refs[:count], refs[-6:]
    _, x, c = bits(me_ref[0])
    _, planes, blocks, inner = near.shape[1:5]
    rows = g_out.shape[1] // PARTS
    come = [pltpu.make_async_copy(m, near.at[n], sems.at[n]) for n, m in enumerate(msgs)]
    for copy in come:
        copy.start()
    go = []
    for n, (r1, r0) in enumerate(rounds):
        start = pl.multiple_of(part(c ^ r1, x ^ r0) * rows + off, 8)
        come[n].wait()
        for k, out in enumerate((g_out, a_out)):
            scale = scale_ref[0, k]
            for i in range(planes):
                for b in range(blocks):
                    ready[n, k, i, :, b * LANES : (b + 1) * LANES] = near[n, k, i, b] * scale
            go.append(pltpu.make_async_copy(ready.at[n, k], out.at[:, pl.ds(start, inner), :], done.at[n, k]))
            go[-1].start()
    for copy in go:
        copy.wait()


def shape(*dims):
    return pltpu.VMEM(dims, F32)


def exchange_sum(value, axis, count, steps):
    for step in steps:
        value = value + lax.ppermute(value, axis, [(i, i ^ step) for i in range(count)])
    return value


def on_device(coefficient, initial_field, observed, misfit_weight):
    axis = "gz"
    count = lax.axis_size(axis)
    planes, height, width = coefficient.shape
    if count % GROUP or width % LANES or height % (32 * PARTS) or 2 * planes < ITERS or ITERS * 2 > HALO:
        raise ValueError("unsupported sizes")
    rows = height // PARTS
    tall = rows + 2 * HALO
    half = 2 * planes
    blocks = width // LANES
    me = lax.axis_index(axis).astype(jnp.int32).reshape(1)

    partner = [(i, i ^ 1) for i in range(count)]
    beyond = []
    for i in range(count - GROUP + 1):
        if i % 2:
            if i + GROUP - 1 < count:
                beyond += [(i, i + GROUP - 1), (i + GROUP - 1, i)]

    def regroup(a, b, rim, name):
        message = shape(2, planes, blocks, rows + 2 * rim, LANES)
        msgs = call(partial(pack_kernel, rim), name, [message] * 4, [me], [a, b])
        got = []
        for m, r in zip(msgs, ROUNDS):
            got.append(lax.ppermute(m, axis, send_pairs(count, *r)))
        return outside(*got)

    first = regroup(*outside(initial_field, coefficient), HALO, "pack_state")
    second = regroup(*outside(observed, misfit_weight), HALO - ITERS, "pack_data")

    plane_set = (blocks, tall, LANES)
    padded = (blocks, tall + 2 * HALO, LANES)
    inner = (blocks, rows, LANES)
    saved_shape = shape(ITERS - 1, 2, *plane_set)
    quarter = shape(2, planes, *plane_set)
    (early,) = call(early_kernel, "early", [quarter], [me], first[:2])
    early = lax.ppermute(early, axis, beyond)
    late, blk_a, blk_b = call(place_kernel, "place", [quarter] + [shape(2, half, *plane_set)] * 2, [me], first)
    late = lax.ppermute(late, axis, beyond)
    far_a = lax.ppermute(blk_a, axis, partner)
    far_a, early, late = outside(far_a, early, late)
    final, coef, slopes, saved = call(
        forward_main,
        "forward_main",
        [shape(2 * half, *plane_set), shape(3 * half, *plane_set), shape(ITERS, 2 * half, *plane_set), saved_shape],
        [me],
        inside(blk_a, blk_b) + [far_a],
        [pltpu.VMEM((3 * half, *padded), F32)] * 2,
    )
    final, slopes, far_coef = call(
        forward_wedge,
        "forward_wedge",
        [shape(2 * half, *plane_set), shape(ITERS, 2 * half, *plane_set), shape(half, *plane_set)],
        [me],
        [early, late] + inside(blk_b, coef, saved, final, slopes),
        [pltpu.VMEM((half + ITERS + 2, *padded), F32)] * 2,
        input_output_aliases={6: 0, 7: 1},
    )

    lam_a, lam_b, part_total = call(
        resid_kernel,
        "resid",
        [shape(half, *plane_set)] * 2 + [jax.ShapeDtypeStruct((1, 1), F32)],
        [me],
        second + inside(final),
        [
            pltpu.VMEM((blocks, HALO, LANES), F32),
            pltpu.VMEM((4,) + second[0].shape, F32),
            pltpu.SemaphoreType.DMA((4,)),
        ],
        total=True,
        far=4,
    )
    far_lb = lax.ppermute(lam_b, axis, beyond)
    far_la = lax.ppermute(lam_a, axis, partner)
    (far_la,), (far_lb,) = outside(far_la), outside(far_lb)
    far = [1] + [1 << k for k in range(3, count.bit_length() - 1)]
    part_total = exchange_sum(part_total, axis, count, [2])
    lam, grad, saved = call(
        backward_main,
        "backward_main",
        [shape(3 * half, *plane_set), shape(2 * half, *inner), saved_shape],
        [me],
        [far_la] + inside(lam_a, lam_b, coef, slopes),
        [pltpu.VMEM((3 * half, *padded), F32)] * 2,
    )
    part_total = exchange_sum(part_total, axis, count, [4])
    strip = rows // 2
    back = []
    for n in range(2):
        outs = call(
            partial(backward_wedge, n * strip),
            f"backward_wedge_{n}",
            [shape(2, planes, blocks, strip, LANES)] * 4,
            [me],
            [far_lb] + inside(lam_b, far_coef, coef, slopes, saved, lam, grad),
            [pltpu.VMEM((2 * half, blocks, strip + 2 * HALO, LANES), F32)]
            + [pltpu.VMEM((half + ITERS + 2, blocks, strip + 4 * HALO, LANES), F32)] * 2
            + [pltpu.VMEM((half, blocks, strip, LANES), F32)],
        )
        for m, r in zip(outs, ROUNDS):
            back.append(lax.ppermute(m, axis, [(j, i) for i, j in send_pairs(count, *r)]))
    back = outside(*back)

    if count & (count - 1):
        total = lax.psum(part_total, axis) / 4
    else:
        total = exchange_sum(part_total, axis, count, far)
    cells = count * planes * height * width
    misfit = jnp.sqrt(total[0, 0] / cells + 1e-06)
    inverse = 1.0 / misfit
    scale = jnp.stack([time_step * inverse, inverse]).reshape(1, 2)
    held = []
    for n in range(0, 8, 2):
        held = pl.pallas_call(
            partial(home_kernel, n // 4 * strip, ROUNDS[n % 4 : n % 4 + 2]),
            out_shape=[jax.ShapeDtypeStruct((planes, height, width), F32)] * 2,
            in_specs=[SM, SM, ANY, ANY] + [ANY] * len(held),
            out_specs=[ANY] * 2,
            scratch_shapes=[
                pltpu.VMEM((2, 2, planes, blocks, strip, LANES), F32),
                pltpu.VMEM((2, 2, planes, strip, width), F32),
                pltpu.SemaphoreType.DMA((2,)),
                pltpu.SemaphoreType.DMA((2, 2)),
            ],
            input_output_aliases={4: 0, 5: 1} if held else {},
            compiler_params=pltpu.CompilerParams(vmem_limit_bytes=14 << 20),
        )(me, scale, *back[n : n + 2], *held)
    gradient, adjoint = held
    return gradient, adjoint, misfit


def solution(mesh):
    placed = P("gz", None, None)
    return jax.shard_map(
        on_device,
        mesh=mesh,
        in_specs=(placed,) * 4,
        out_specs=(placed, placed, P()),
        check_vma=False,
    )
```

```python
from functools import partial

import jax
import jax.numpy as jnp
from jax import lax
from jax.experimental import pallas as pl
from jax.experimental.pallas import tpu as pltpu
from jax.sharding import PartitionSpec as P


ITERS = 4
time_step = 0.125

GROUP = 8
PARTS = 4
HALO = 8
LANES = 128
ROUNDS = ((0, 1), (0, 0), (1, 1), (1, 0))


VM = pl.BlockSpec(memory_space=pltpu.VMEM)
SM = pl.BlockSpec(memory_space=pltpu.SMEM)
ANY = pl.BlockSpec(memory_space=pl.ANY)
SHARE = {"forward_main": 30, "forward_wedge": 30, "backward_main": 11, "backward_wedge_0": 9, "backward_wedge_1": 9, "resid": 8}
F32 = jnp.float32


def call(kernel, name, outs, scalars, arrays, scratch=(), total=False, far=0, **options):
    return pl.pallas_call(
        kernel,
        out_shape=outs,
        in_specs=[SM] * len(scalars) + [ANY] * far + [VM] * (len(arrays) - far),
        out_specs=[VM] * (len(outs) - total) + [SM] * total,
        scratch_shapes=scratch,
        compiler_params=pltpu.CompilerParams(vmem_limit_bytes=SHARE.get(name, 14) << 20),
        **options,
    )(*scalars, *arrays)


def inside(*arrays):
    return [pltpu.with_memory_space_constraint(a, pltpu.VMEM) for a in arrays]


def outside(*arrays):
    return [pltpu.with_memory_space_constraint(a, pltpu.HBM) for a in arrays]


def bits(me):
    return (me >> 2) & 1, (me >> 1) & 1, me & 1


def part(y, x):
    return 2 * y + x


def send_pairs(count, r1, r0):
    pairs = []
    for i in range(count):
        y, x, c = bits(i)
        pairs.append((i, (i & ~7) + 4 * (c ^ r1) + 2 * (x ^ r0) + y))
    return pairs


def pack_kernel(rim, me_ref, a_ref, b_ref, *out_refs):
    _, x, c = bits(me_ref[0])
    planes, height, width = a_ref.shape
    rows = height // PARTS
    for (r1, r0), out in zip(ROUNDS, out_refs):
        q = part(c ^ r1, x ^ r0)
        start = pl.multiple_of(q * rows, 8)
        above = pl.multiple_of(jnp.maximum(start - HALO, 0), 8)
        below = pl.multiple_of(jnp.minimum(start + rows, height - HALO), 8)
        for k, src in enumerate((a_ref, b_ref)):
            for i in range(planes):
                for b in range(width // LANES):
                    cols = slice(b * LANES, (b + 1) * LANES)
                    top = src[i, pl.ds(above, HALO), cols]
                    out[k, i, b, :rim, :] = jnp.where(q > 0, top[HALO - rim :], 0.0)
                    low = src[i, pl.ds(below, HALO), cols]
                    out[k, i, b, rim + rows :, :] = jnp.where(q < PARTS - 1, low[:rim], 0.0)
                    for at in range(0, rows, HALO):
                        here = pl.ds(pl.multiple_of(start + at, 8), HALO)
                        out[k, i, b, rim + at : rim + at + HALO, :] = src[i, here, cols]


def slot(me, r, planes, i):
    y, x, c = bits(me)
    r1, r0 = r
    from_c = y ^ r1
    block = x ^ r0 ^ c
    ahead = planes * from_c + i
    return block, jnp.where(c == 0, ahead, 2 * planes - 1 - ahead)


def early_kernel(me_ref, m0, m1, early_ref):
    me = me_ref[0]
    for r, m in zip(ROUNDS, (m0, m1)):
        block, _ = slot(me, r, m.shape[1], 0)

        @pl.when(block == 0)
        def _(m=m):
            early_ref[...] = m[...]


def place_kernel(me_ref, m0, m1, m2, m3, late_ref, a_ref, b_ref):
    me = me_ref[0]
    planes = m0.shape[1]
    for r, m in zip(ROUNDS, (m0, m1, m2, m3)):
        block, _ = slot(me, r, planes, 0)

        @pl.when(block == 0)
        def _(r=r, m=m):
            if r[0]:
                late_ref[...] = m[...]
            for i in range(planes):
                _, at = slot(me, r, planes, i)
                for k in range(2):
                    b_ref[k, at] = m[k, i]

        @pl.when(block == 1)
        def _(r=r, m=m):
            for i in range(planes):
                _, at = slot(me, r, planes, i)
                for k in range(2):
                    a_ref[k, at] = m[k, i]


def edges(shape):
    col = lax.broadcasted_iota(jnp.int32, shape, 2)
    return col == 0, col == shape[2] - 1


def lap_rows(ref, s, r0, n, first, last):
    lo = HALO + r0
    mid = ref[s, :, lo : lo + n, :]
    none = jnp.zeros((1,) + mid.shape[1:], F32)
    beside = ref[s + 1, :, lo : lo + n, :] + ref[s - 1, :, lo : lo + n, :]
    beside = beside + (ref[s, :, lo + 1 : lo + n + 1, :] + ref[s, :, lo - 1 : lo + n - 1, :])
    right = pltpu.roll(mid, LANES - 1, 2)
    right = jnp.where(last, jnp.concatenate([right[1:], none], axis=0), right)
    left = pltpu.roll(mid, 1, 2)
    left = jnp.where(first, jnp.concatenate([none, left[:-1]], axis=0), left)
    return beside + (right + left) - 6.0 * mid, mid


def clear_rims(ref, rows):
    none = jnp.zeros((ref.shape[1], HALO, LANES), F32)

    def one(s, carry):
        ref[s, :, :HALO, :] = none
        ref[s, :, HALO + rows :, :] = none
        return carry

    lax.fori_loop(0, ref.shape[0], one, 0)


CHUNK = 16


def copy_rows(rows, move):
    def one(t, carry):
        r = pl.multiple_of(t * CHUNK, 8)
        move(pl.ds(r, CHUNK), pl.ds(r + HALO, CHUNK))
        return carry

    lax.fori_loop(0, rows // CHUNK, one, 0)


def spans(lo, hi, body):
    if (hi - lo) % 2:
        body(lo, 0)
        lo += 1

    def two(t, carry):
        body(lo + 2 * t, carry)
        body(lo + 2 * t + 1, carry)
        return carry

    if hi > lo:
        lax.fori_loop(0, (hi - lo) // 2, two, 0)


def forward_main(me_ref, a_ref, b_ref, ra_ref, u_out, c_out, slopes, saved, u0, u1):
    half, blocks, rows = a_ref.shape[1:4]
    clear_rims(u0, rows)
    clear_rims(u1, rows)
    for i in range(half):
        for src, at, t in ((b_ref, i, i), (a_ref, i, half + i), (ra_ref, half - 1 - i, 2 * half + i)):

            def fill(r, rh, src=src, at=at, t=t):
                u0[t, :, rh, :] = src[0, at, :, r, :]
                c_out[t, :, r, :] = time_step * src[1, at, :, r, :]

            copy_rows(rows, fill)
    first, last = edges((blocks, CHUNK, LANES))
    for k in range(ITERS):
        old, new = (u0, u1) if k % 2 == 0 else (u1, u0)

        def plane(t, carry, own, k=k, old=old, new=new):
            for r0 in range(0, rows, CHUNK):
                slope, mid = lap_rows(old, t, r0, CHUNK, first, last)
                moved = mid + c_out[t, :, r0 : r0 + CHUNK, :] * slope
                if own:
                    slopes[k, t, :, r0 : r0 + CHUNK, :] = slope
                if k == ITERS - 1:
                    u_out[t, :, r0 : r0 + CHUNK, :] = moved
                else:
                    new[t, :, HALO + r0 : HALO + r0 + CHUNK, :] = moved
            return carry

        spans(1 + k, 2 * half, lambda t, c: plane(t, c, True))
        spans(2 * half, 2 * half + ITERS - 1 - k, lambda t, c: plane(t, c, False))
        if k < ITERS - 1:
            for i in range(2):

                def keep(r, rh, k=k, i=i, new=new):
                    saved[k, i, :, r, :] = new[k + 1 + i, :, rh, :]

                copy_rows(rows, keep)


def forward_wedge(me_ref, early, late, b_ref, c_ref, saved, u_in, slopes_in, u_out, slopes, cw, w0, w1):
    y, _, c = bits(me_ref[0])
    half, blocks, rows = b_ref.shape[1:4]
    planes = early.shape[1]
    clear_rims(w0, rows)
    clear_rims(w1, rows)
    for r1, far in enumerate((early, late)):
        for i in range(planes):
            ahead = planes * (y ^ r1) + i
            s = half - 1 - jnp.where(c == 1, ahead, half - 1 - ahead)

            def fill(r, rh, far=far, i=i, s=s):
                w0[s, :, rh, :] = far[0, i, :, r, :]
                cw[s, :, r, :] = time_step * far[1, i, :, r, :]

            copy_rows(rows, fill)
    for i in range(2):
        copy_rows(rows, lambda r, rh, i=i: w0.__setitem__((half + i, slice(None), rh), b_ref[0, i, :, r, :]))
    first, last = edges((blocks, CHUNK, LANES))
    for k in range(ITERS):
        old, new = (w0, w1) if k % 2 == 0 else (w1, w0)
        if k:
            for i in range(2):
                copy_rows(rows, lambda r, rh, i=i: old.__setitem__((half + k + i, slice(None), rh), saved[k - 1, i, :, r, :]))

        def plane(s, carry, own, k=k, old=old, new=new):
            for r0 in range(0, rows, CHUNK):
                slope, mid = lap_rows(old, s, r0, CHUNK, first, last)
                at = slice(r0, r0 + CHUNK)
                coef = c_ref[s - half, :, at, :] if own else cw[s, :, at, :]
                moved = mid + coef * slope
                if own:
                    slopes[k, s - half, :, at, :] = slope
                if k == ITERS - 1:
                    u_out[s - half, :, at, :] = moved
                else:
                    new[s, :, HALO + r0 : HALO + r0 + CHUNK, :] = moved
            return carry

        spans(half - ITERS + 1 + k, half, lambda s, c: plane(s, c, False))
        spans(half, half + k + 1, lambda s, c: plane(s, c, True))


def resid_kernel(me_ref, f0, f1, f2, f3, u_ref, a_ref, b_ref, total_ref, acc_ref, near, sems):
    me = me_ref[0]
    copies = [pltpu.make_async_copy(f, near.at[n], sems.at[n]) for n, f in enumerate((f0, f1, f2, f3))]
    for copy in copies:
        copy.start()
    planes, blocks, short = near.shape[2:5]
    rows = u_ref.shape[2]
    rim = (rows - short) // 2
    shape = (blocks, HALO, LANES)
    row = lax.broadcasted_iota(jnp.int32, shape, 1)
    acc_ref[...] = jnp.zeros(shape, F32)
    for n, r in enumerate(ROUNDS):
        copies[n].wait()
        for i in range(planes):
            block, at = slot(me, r, planes, i)
            for flag, dst in ((1, a_ref), (0, b_ref)):

                @pl.when(block == flag)
                def _(n=n, i=i, at=at, dst=dst, flag=flag):
                    dst[at, :, :rim, :] = jnp.zeros((blocks, rim, LANES), F32)
                    dst[at, :, rows - rim :, :] = jnp.zeros((blocks, rim, LANES), F32)
                    acc = jnp.zeros(shape, F32)
                    for lo in range(0, short, HALO):
                        here = slice(lo + rim, lo + rim + HALO)
                        resid = u_ref[2 * planes * flag + at, :, here, :] - near[n, 0, i, :, lo : lo + HALO, :]
                        weighted = near[n, 1, i, :, lo : lo + HALO, :] * resid
                        dst[at, :, here, :] = weighted
                        share = weighted * resid
                        if lo + rim < HALO:
                            share = jnp.where(row >= HALO - rim, share, 0.0)
                        if lo + rim + HALO > rows - HALO:
                            share = jnp.where(row < HALO - rim, share, 0.0)
                        acc = acc + share
                    acc_ref[...] = acc_ref[...] + acc

    total_ref[0, 0] = jnp.sum(acc_ref[...])


def backward_main(me_ref, ra_ref, a_ref, b_ref, c_ref, slopes, lam, grad, saved, mv0, mv1):
    half, blocks, rows = a_ref.shape[:3]
    clear_rims(mv0, rows)
    clear_rims(mv1, rows)
    for i in range(half):
        for src, at, t in ((b_ref, i, i), (a_ref, i, half + i), (ra_ref, half - 1 - i, 2 * half + i)):

            def fill(r, rh, src=src, at=at, t=t):
                v = src[at, :, r, :]
                lam[t, :, r, :] = v
                mv0[t, :, rh, :] = c_ref[t, :, r, :] * v

            copy_rows(rows, fill)
    first, last = edges((blocks, CHUNK, LANES))
    first8, last8 = edges((blocks, HALO, LANES))

    for j in range(ITERS):
        k = ITERS - 1 - j
        old, new = (mv0, mv1) if j % 2 == 0 else (mv1, mv0)

        def gain(t, r0, j=j, k=k):
            g = lam[t, :, r0 : r0 + CHUNK, :] * slopes[k, t, :, r0 : r0 + CHUNK, :]
            at = slice(r0 - HALO, r0 - HALO + CHUNK)
            grad[t, :, at, :] = grad[t, :, at, :] + g if j else g

        def gain_plane(t, carry, gain=gain):
            for r0 in range(HALO, rows - HALO, CHUNK):
                gain(t, r0)
            return carry

        def step(t, r0, n, f, l, j=j, old=old, new=new):
            change, _ = lap_rows(old, t, r0, n, f, l)
            after = lam[t, :, r0 : r0 + n, :] + change
            lam[t, :, r0 : r0 + n, :] = after
            if j < ITERS - 1:
                new[t, :, HALO + r0 : HALO + r0 + n, :] = c_ref[t, :, r0 : r0 + n, :] * after

        def own_plane(t, carry, gain=gain, step=step, j=j):
            for r0 in range(HALO, rows - HALO, CHUNK):
                gain(t, r0)
                step(t, r0, CHUNK, first, last)
            if j < ITERS - 1:
                step(t, 0, HALO, first8, last8)
                step(t, rows - HALO, HALO, first8, last8)
            return carry

        def halo_plane(t, carry, step=step):
            for r0 in range(0, rows, CHUNK):
                step(t, r0, CHUNK, first, last)
            return carry

        gain_plane(j, 0)
        spans(1 + j, 2 * half, own_plane)
        spans(2 * half, 2 * half + ITERS - 1 - j, halo_plane)
        if j < ITERS - 1:
            for i in range(2):

                def keep(r, rh, j=j, i=i, new=new):
                    saved[j, i, :, r, :] = new[j + 1 + i, :, rh, :]

                copy_rows(rows, keep)


def backward_wedge(off, me_ref, rb_ref, b_ref, cw, c_ref, slopes, saved, lam_in, grad_in, o0, o1, o2, o3, lam, mv0, mv1, grad):
    inner = o0.shape[3]
    rows = inner + 2 * HALO
    half, blocks = b_ref.shape[:2]
    clear_rims(mv0, rows)
    clear_rims(mv1, rows)

    def there(r):
        return pl.ds(pl.multiple_of(r.start + off, 8), r.size)

    for i in range(half):

        def fill(r, rh, i=i):
            v = rb_ref[half - 1 - i, :, there(r), :]
            lam[i, :, r, :] = v
            mv0[i, :, rh, :] = cw[i, :, there(r), :] * v
            lam[half + i, :, r, :] = lam_in[i, :, there(r), :]
            if i < 2:
                mv0[half + i, :, rh, :] = c_ref[i, :, there(r), :] * b_ref[i, :, there(r), :]

        copy_rows(rows, fill)
        copy_rows(inner, lambda r, rh, i=i: grad.__setitem__((i, slice(None), r), grad_in[i, :, there(r), :]))
    first, last = edges((blocks, CHUNK, LANES))
    for j in range(ITERS):
        k = ITERS - 1 - j
        old, new = (mv0, mv1) if j % 2 == 0 else (mv1, mv0)
        if j:
            for i in range(2):

                def recall(r, rh, j=j, i=i, old=old):
                    old[half + j + i, :, rh, :] = saved[j - 1, i, :, there(r), :]

                copy_rows(rows, recall)

        def plane(s, carry, own, j=j, old=old, new=new):
            for r0 in range(0, rows, CHUNK):
                change, _ = lap_rows(old, s, r0, CHUNK, first, last)
                after = lam[s, :, r0 : r0 + CHUNK, :] + change
                if j < ITERS - 1:
                    at = slice(off + r0, off + r0 + CHUNK)
                    coef = c_ref[s - half, :, at, :] if own else cw[s, :, at, :]
                    new[s, :, HALO + r0 : HALO + r0 + CHUNK, :] = coef * after
                lam[s, :, r0 : r0 + CHUNK, :] = after
            return carry

        def gain(s, carry, k=k):
            for r0 in range(HALO, rows - HALO, CHUNK):
                at = slice(r0 - HALO, r0 - HALO + CHUNK)
                g = lam[s, :, r0 : r0 + CHUNK, :] * slopes[k, s - half, :, off + r0 : off + r0 + CHUNK, :]
                grad[s - half, :, at, :] = grad[s - half, :, at, :] + g
            return carry

        spans(half, half + j, gain)
        spans(half - ITERS + 1 + j, half, lambda s, c: plane(s, c, False))
        spans(half, half + j + 1, lambda s, c: plane(s, c, True))
    me = me_ref[0]
    planes = half // 2
    for r, out in zip(ROUNDS, (o0, o1, o2, o3)):
        block, _ = slot(me, r, planes, 0)

        @pl.when(block == 0)
        def _(r=r, out=out):
            for i in range(planes):
                _, at = slot(me, r, planes, i)
                out[0, i] = grad[at]
                out[1, i] = lam[half + at, :, HALO : HALO + inner, :]

        @pl.when(block == 1)
        def _(r=r, out=out):
            for i in range(planes):
                _, at = slot(me, r, planes, i)
                out[0, i] = grad_in[half + at, :, off : off + inner, :]
                out[1, i] = lam_in[half + at, :, off + HALO : off + HALO + inner, :]


def home_kernel(off, rounds, me_ref, scale_ref, *refs):
    count = len(rounds)
    msgs, (g_out, a_out, near, ready, sems, done) = refs[:count], refs[-6:]
    _, x, c = bits(me_ref[0])
    _, planes, blocks, inner = near.shape[1:5]
    rows = g_out.shape[1] // PARTS
    come = [pltpu.make_async_copy(m, near.at[n], sems.at[n]) for n, m in enumerate(msgs)]
    for copy in come:
        copy.start()
    go = []
    for n, (r1, r0) in enumerate(rounds):
        start = pl.multiple_of(part(c ^ r1, x ^ r0) * rows + off, 8)
        come[n].wait()
        for k, out in enumerate((g_out, a_out)):
            scale = scale_ref[0, k]
            for i in range(planes):
                for b in range(blocks):
                    ready[n, k, i, :, b * LANES : (b + 1) * LANES] = near[n, k, i, b] * scale
            go.append(pltpu.make_async_copy(ready.at[n, k], out.at[:, pl.ds(start, inner), :], done.at[n, k]))
            go[-1].start()
    for copy in go:
        copy.wait()


def shape(*dims):
    return pltpu.VMEM(dims, F32)


def exchange_sum(value, axis, count, steps):
    for step in steps:
        value = value + lax.ppermute(value, axis, [(i, i ^ step) for i in range(count)])
    return value


def on_device(coefficient, initial_field, observed, misfit_weight):
    axis = "gz"
    count = lax.axis_size(axis)
    planes, height, width = coefficient.shape
    if count % GROUP or width % LANES or height % (32 * PARTS) or 2 * planes < ITERS or ITERS * 2 > HALO:
        raise ValueError("unsupported sizes")
    rows = height // PARTS
    tall = rows + 2 * HALO
    half = 2 * planes
    blocks = width // LANES
    me = lax.axis_index(axis).astype(jnp.int32).reshape(1)

    partner = [(i, i ^ 1) for i in range(count)]
    beyond = []
    for i in range(count - GROUP + 1):
        if i % 2:
            if i + GROUP - 1 < count:
                beyond += [(i, i + GROUP - 1), (i + GROUP - 1, i)]

    def regroup(a, b, rim, name):
        message = shape(2, planes, blocks, rows + 2 * rim, LANES)
        msgs = call(partial(pack_kernel, rim), name, [message] * 4, [me], [a, b])
        got = []
        for m, r in zip(msgs, ROUNDS):
            got.append(lax.ppermute(m, axis, send_pairs(count, *r)))
        return outside(*got)

    first = regroup(*outside(initial_field, coefficient), HALO, "pack_state")
    second = regroup(*outside(observed, misfit_weight), HALO - ITERS, "pack_data")

    plane_set = (blocks, tall, LANES)
    padded = (blocks, tall + 2 * HALO, LANES)
    inner = (blocks, rows, LANES)
    saved_shape = shape(ITERS - 1, 2, *plane_set)
    quarter = shape(2, planes, *plane_set)
    (early,) = call(early_kernel, "early", [quarter], [me], first[:2])
    early = lax.ppermute(early, axis, beyond)
    late, blk_a, blk_b = call(place_kernel, "place", [quarter] + [shape(2, half, *plane_set)] * 2, [me], first)
    late = lax.ppermute(late, axis, beyond)
    far_a = lax.ppermute(blk_a, axis, partner)
    far_a, early, late = outside(far_a, early, late)
    final, coef, slopes, saved = call(
        forward_main,
        "forward_main",
        [shape(2 * half, *plane_set), shape(3 * half, *plane_set), shape(ITERS, 2 * half, *plane_set), saved_shape],
        [me],
        inside(blk_a, blk_b) + [far_a],
        [pltpu.VMEM((3 * half, *padded), F32)] * 2,
    )
    final, slopes, far_coef = call(
        forward_wedge,
        "forward_wedge",
        [shape(2 * half, *plane_set), shape(ITERS, 2 * half, *plane_set), shape(half, *plane_set)],
        [me],
        [early, late] + inside(blk_b, coef, saved, final, slopes),
        [pltpu.VMEM((half + ITERS + 2, *padded), F32)] * 2,
        input_output_aliases={6: 0, 7: 1},
    )

    lam_a, lam_b, part_total = call(
        resid_kernel,
        "resid",
        [shape(half, *plane_set)] * 2 + [jax.ShapeDtypeStruct((1, 1), F32)],
        [me],
        second + inside(final),
        [
            pltpu.VMEM((blocks, HALO, LANES), F32),
            pltpu.VMEM((4,) + second[0].shape, F32),
            pltpu.SemaphoreType.DMA((4,)),
        ],
        total=True,
        far=4,
    )
    far_lb = lax.ppermute(lam_b, axis, beyond)
    far_la = lax.ppermute(lam_a, axis, partner)
    (far_la,), (far_lb,) = outside(far_la), outside(far_lb)
    far = [1] + [1 << k for k in range(3, count.bit_length() - 1)]
    part_total = exchange_sum(part_total, axis, count, [2])
    lam, grad, saved = call(
        backward_main,
        "backward_main",
        [shape(3 * half, *plane_set), shape(2 * half, *inner), saved_shape],
        [me],
        [far_la] + inside(lam_a, lam_b, coef, slopes),
        [pltpu.VMEM((3 * half, *padded), F32)] * 2,
    )
    part_total = exchange_sum(part_total, axis, count, [4])
    strip = rows // 2
    back = []
    for n in range(2):
        outs = call(
            partial(backward_wedge, n * strip),
            f"backward_wedge_{n}",
            [shape(2, planes, blocks, strip, LANES)] * 4,
            [me],
            [far_lb] + inside(lam_b, far_coef, coef, slopes, saved, lam, grad),
            [pltpu.VMEM((2 * half, blocks, strip + 2 * HALO, LANES), F32)]
            + [pltpu.VMEM((half + ITERS + 2, blocks, strip + 4 * HALO, LANES), F32)] * 2
            + [pltpu.VMEM((half, blocks, strip, LANES), F32)],
        )
        for m, r in zip(outs, ROUNDS):
            back.append(lax.ppermute(m, axis, [(j, i) for i, j in send_pairs(count, *r)]))
    back = outside(*back)

    if count & (count - 1):
        total = lax.psum(part_total, axis) / 4
    else:
        total = exchange_sum(part_total, axis, count, far)
    cells = count * planes * height * width
    misfit = jnp.sqrt(total[0, 0] / cells + 1e-06)
    inverse = 1.0 / misfit
    scale = jnp.stack([time_step * inverse, inverse]).reshape(1, 2)
    held = []
    for n in range(0, 8, 2):
        held = pl.pallas_call(
            partial(home_kernel, n // 4 * strip, ROUNDS[n % 4 : n % 4 + 2]),
            out_shape=[jax.ShapeDtypeStruct((planes, height, width), F32)] * 2,
            in_specs=[SM, SM, ANY, ANY] + [ANY] * len(held),
            out_specs=[ANY] * 2,
            scratch_shapes=[
                pltpu.VMEM((2, 2, planes, blocks, strip, LANES), F32),
                pltpu.VMEM((2, 2, planes, strip, width), F32),
                pltpu.SemaphoreType.DMA((2,)),
                pltpu.SemaphoreType.DMA((2, 2)),
            ],
            input_output_aliases={4: 0, 5: 1} if held else {},
            compiler_params=pltpu.CompilerParams(vmem_limit_bytes=14 << 20),
        )(me, scale, *back[n : n + 2], *held)
    gradient, adjoint = held
    return gradient, adjoint, misfit


def solution(mesh):
    placed = P("gz", None, None)
    return jax.shard_map(
        on_device,
        mesh=mesh,
        in_specs=(placed,) * 4,
        out_specs=(placed, placed, P()),
        check_vma=False,
    )
```

```python
from functools import partial

import jax
import jax.numpy as jnp
from jax import lax
from jax.experimental import pallas as pl
from jax.experimental.pallas import tpu as pltpu
from jax.sharding import PartitionSpec as P


ITERS = 4
time_step = 0.125

GROUP = 8
PARTS = 4
HALO = 8
LANES = 128
ROUNDS = ((0, 1), (0, 0), (1, 1), (1, 0))


VM = pl.BlockSpec(memory_space=pltpu.VMEM)
SM = pl.BlockSpec(memory_space=pltpu.SMEM)
ANY = pl.BlockSpec(memory_space=pl.ANY)
SHARE = {"forward_main": 30, "forward_wedge": 30, "backward_main": 11, "backward_wedge_0": 9, "backward_wedge_1": 9, "resid": 8}
F32 = jnp.float32


def call(kernel, name, outs, scalars, arrays, scratch=(), total=False, far=0, **options):
    return pl.pallas_call(
        kernel,
        out_shape=outs,
        in_specs=[SM] * len(scalars) + [ANY] * far + [VM] * (len(arrays) - far),
        out_specs=[VM] * (len(outs) - total) + [SM] * total,
        scratch_shapes=scratch,
        compiler_params=pltpu.CompilerParams(vmem_limit_bytes=SHARE.get(name, 14) << 20),
        **options,
    )(*scalars, *arrays)


def inside(*arrays):
    return [pltpu.with_memory_space_constraint(a, pltpu.VMEM) for a in arrays]


def outside(*arrays):
    return [pltpu.with_memory_space_constraint(a, pltpu.HBM) for a in arrays]


def bits(me):
    return (me >> 2) & 1, (me >> 1) & 1, me & 1


def part(y, x):
    return 2 * y + x


def send_pairs(count, r1, r0):
    pairs = []
    for i in range(count):
        y, x, c = bits(i)
        pairs.append((i, (i & ~7) + 4 * (c ^ r1) + 2 * (x ^ r0) + y))
    return pairs


def pack_kernel(rim, me_ref, a_ref, b_ref, *out_refs):
    _, x, c = bits(me_ref[0])
    planes, height, width = a_ref.shape
    rows = height // PARTS
    for (r1, r0), out in zip(ROUNDS, out_refs):
        q = part(c ^ r1, x ^ r0)
        start = pl.multiple_of(q * rows, 8)
        above = pl.multiple_of(jnp.maximum(start - HALO, 0), 8)
        below = pl.multiple_of(jnp.minimum(start + rows, height - HALO), 8)
        for k, src in enumerate((a_ref, b_ref)):
            for i in range(planes):
                for b in range(width // LANES):
                    cols = slice(b * LANES, (b + 1) * LANES)
                    top = src[i, pl.ds(above, HALO), cols]
                    out[k, i, b, :rim, :] = jnp.where(q > 0, top[HALO - rim :], 0.0)
                    low = src[i, pl.ds(below, HALO), cols]
                    out[k, i, b, rim + rows :, :] = jnp.where(q < PARTS - 1, low[:rim], 0.0)
                    for at in range(0, rows, HALO):
                        here = pl.ds(pl.multiple_of(start + at, 8), HALO)
                        out[k, i, b, rim + at : rim + at + HALO, :] = src[i, here, cols]


def slot(me, r, planes, i):
    y, x, c = bits(me)
    r1, r0 = r
    from_c = y ^ r1
    block = x ^ r0 ^ c
    ahead = planes * from_c + i
    return block, jnp.where(c == 0, ahead, 2 * planes - 1 - ahead)


def early_kernel(me_ref, m0, m1, early_ref):
    me = me_ref[0]
    for r, m in zip(ROUNDS, (m0, m1)):
        block, _ = slot(me, r, m.shape[1], 0)

        @pl.when(block == 0)
        def _(m=m):
            early_ref[...] = m[...]


def place_kernel(me_ref, m0, m1, m2, m3, late_ref, a_ref, b_ref):
    me = me_ref[0]
    planes = m0.shape[1]
    for r, m in zip(ROUNDS, (m0, m1, m2, m3)):
        block, _ = slot(me, r, planes, 0)

        @pl.when(block == 0)
        def _(r=r, m=m):
            if r[0]:
                late_ref[...] = m[...]
            for i in range(planes):
                _, at = slot(me, r, planes, i)
                for k in range(2):
                    b_ref[k, at] = m[k, i]

        @pl.when(block == 1)
        def _(r=r, m=m):
            for i in range(planes):
                _, at = slot(me, r, planes, i)
                for k in range(2):
                    a_ref[k, at] = m[k, i]


def edges(shape):
    col = lax.broadcasted_iota(jnp.int32, shape, 2)
    return col == 0, col == shape[2] - 1


def lap_rows(ref, s, r0, n, first, last):
    lo = HALO + r0
    mid = ref[s, :, lo : lo + n, :]
    none = jnp.zeros((1,) + mid.shape[1:], F32)
    beside = ref[s + 1, :, lo : lo + n, :] + ref[s - 1, :, lo : lo + n, :]
    beside = beside + (ref[s, :, lo + 1 : lo + n + 1, :] + ref[s, :, lo - 1 : lo + n - 1, :])
    right = pltpu.roll(mid, LANES - 1, 2)
    right = jnp.where(last, jnp.concatenate([right[1:], none], axis=0), right)
    left = pltpu.roll(mid, 1, 2)
    left = jnp.where(first, jnp.concatenate([none, left[:-1]], axis=0), left)
    return beside + (right + left) - 6.0 * mid, mid


def clear_rims(ref, rows):
    none = jnp.zeros((ref.shape[1], HALO, LANES), F32)

    def one(s, carry):
        ref[s, :, :HALO, :] = none
        ref[s, :, HALO + rows :, :] = none
        return carry

    lax.fori_loop(0, ref.shape[0], one, 0)


CHUNK = 16


def copy_rows(rows, move):
    def one(t, carry):
        r = pl.multiple_of(t * CHUNK, 8)
        move(pl.ds(r, CHUNK), pl.ds(r + HALO, CHUNK))
        return carry

    lax.fori_loop(0, rows // CHUNK, one, 0)


def spans(lo, hi, body):
    if (hi - lo) % 2:
        body(lo, 0)
        lo += 1

    def two(t, carry):
        body(lo + 2 * t, carry)
        body(lo + 2 * t + 1, carry)
        return carry

    if hi > lo:
        lax.fori_loop(0, (hi - lo) // 2, two, 0)


def forward_main(me_ref, a_ref, b_ref, ra_ref, u_out, c_out, slopes, saved, u0, u1):
    half, blocks, rows = a_ref.shape[1:4]
    clear_rims(u0, rows)
    clear_rims(u1, rows)
    for i in range(half):
        for src, at, t in ((b_ref, i, i), (a_ref, i, half + i), (ra_ref, half - 1 - i, 2 * half + i)):

            def fill(r, rh, src=src, at=at, t=t):
                u0[t, :, rh, :] = src[0, at, :, r, :]
                c_out[t, :, r, :] = time_step * src[1, at, :, r, :]

            copy_rows(rows, fill)
    first, last = edges((blocks, CHUNK, LANES))
    for k in range(ITERS):
        old, new = (u0, u1) if k % 2 == 0 else (u1, u0)

        def plane(t, carry, own, k=k, old=old, new=new):
            for r0 in range(0, rows, CHUNK):
                slope, mid = lap_rows(old, t, r0, CHUNK, first, last)
                moved = mid + c_out[t, :, r0 : r0 + CHUNK, :] * slope
                if own:
                    slopes[k, t, :, r0 : r0 + CHUNK, :] = slope
                if k == ITERS - 1:
                    u_out[t, :, r0 : r0 + CHUNK, :] = moved
                else:
                    new[t, :, HALO + r0 : HALO + r0 + CHUNK, :] = moved
            return carry

        spans(1 + k, 2 * half, lambda t, c: plane(t, c, True))
        spans(2 * half, 2 * half + ITERS - 1 - k, lambda t, c: plane(t, c, False))
        if k < ITERS - 1:
            for i in range(2):

                def keep(r, rh, k=k, i=i, new=new):
                    saved[k, i, :, r, :] = new[k + 1 + i, :, rh, :]

                copy_rows(rows, keep)


def forward_wedge(me_ref, early, late, b_ref, c_ref, saved, u_in, slopes_in, u_out, slopes, cw, w0, w1):
    y, _, c = bits(me_ref[0])
    half, blocks, rows = b_ref.shape[1:4]
    planes = early.shape[1]
    clear_rims(w0, rows)
    clear_rims(w1, rows)
    for r1, far in enumerate((early, late)):
        for i in range(planes):
            ahead = planes * (y ^ r1) + i
            s = half - 1 - jnp.where(c == 1, ahead, half - 1 - ahead)

            def fill(r, rh, far=far, i=i, s=s):
                w0[s, :, rh, :] = far[0, i, :, r, :]
                cw[s, :, r, :] = time_step * far[1, i, :, r, :]

            copy_rows(rows, fill)
    for i in range(2):
        copy_rows(rows, lambda r, rh, i=i: w0.__setitem__((half + i, slice(None), rh), b_ref[0, i, :, r, :]))
    first, last = edges((blocks, CHUNK, LANES))
    for k in range(ITERS):
        old, new = (w0, w1) if k % 2 == 0 else (w1, w0)
        if k:
            for i in range(2):
                copy_rows(rows, lambda r, rh, i=i: old.__setitem__((half + k + i, slice(None), rh), saved[k - 1, i, :, r, :]))

        def plane(s, carry, own, k=k, old=old, new=new):
            for r0 in range(0, rows, CHUNK):
                slope, mid = lap_rows(old, s, r0, CHUNK, first, last)
                at = slice(r0, r0 + CHUNK)
                coef = c_ref[s - half, :, at, :] if own else cw[s, :, at, :]
                moved = mid + coef * slope
                if own:
                    slopes[k, s - half, :, at, :] = slope
                if k == ITERS - 1:
                    u_out[s - half, :, at, :] = moved
                else:
                    new[s, :, HALO + r0 : HALO + r0 + CHUNK, :] = moved
            return carry

        spans(half - ITERS + 1 + k, half, lambda s, c: plane(s, c, False))
        spans(half, half + k + 1, lambda s, c: plane(s, c, True))


def resid_kernel(me_ref, f0, f1, f2, f3, u_ref, a_ref, b_ref, total_ref, acc_ref, near, sems):
    me = me_ref[0]
    copies = [pltpu.make_async_copy(f, near.at[n], sems.at[n]) for n, f in enumerate((f0, f1, f2, f3))]
    for copy in copies:
        copy.start()
    planes, blocks, short = near.shape[2:5]
    rows = u_ref.shape[2]
    rim = (rows - short) // 2
    shape = (blocks, HALO, LANES)
    row = lax.broadcasted_iota(jnp.int32, shape, 1)
    acc_ref[...] = jnp.zeros(shape, F32)
    for n, r in enumerate(ROUNDS):
        copies[n].wait()
        for i in range(planes):
            block, at = slot(me, r, planes, i)
            for flag, dst in ((1, a_ref), (0, b_ref)):

                @pl.when(block == flag)
                def _(n=n, i=i, at=at, dst=dst, flag=flag):
                    dst[at, :, :rim, :] = jnp.zeros((blocks, rim, LANES), F32)
                    dst[at, :, rows - rim :, :] = jnp.zeros((blocks, rim, LANES), F32)
                    acc = jnp.zeros(shape, F32)
                    for lo in range(0, short, HALO):
                        here = slice(lo + rim, lo + rim + HALO)
                        resid = u_ref[2 * planes * flag + at, :, here, :] - near[n, 0, i, :, lo : lo + HALO, :]
                        weighted = near[n, 1, i, :, lo : lo + HALO, :] * resid
                        dst[at, :, here, :] = weighted
                        share = weighted * resid
                        if lo + rim < HALO:
                            share = jnp.where(row >= HALO - rim, share, 0.0)
                        if lo + rim + HALO > rows - HALO:
                            share = jnp.where(row < HALO - rim, share, 0.0)
                        acc = acc + share
                    acc_ref[...] = acc_ref[...] + acc

    total_ref[0, 0] = jnp.sum(acc_ref[...])


def backward_main(me_ref, ra_ref, a_ref, b_ref, c_ref, slopes, lam, grad, saved, mv0, mv1):
    half, blocks, rows = a_ref.shape[:3]
    clear_rims(mv0, rows)
    clear_rims(mv1, rows)
    for i in range(half):
        for src, at, t in ((b_ref, i, i), (a_ref, i, half + i), (ra_ref, half - 1 - i, 2 * half + i)):

            def fill(r, rh, src=src, at=at, t=t):
                v = src[at, :, r, :]
                lam[t, :, r, :] = v
                mv0[t, :, rh, :] = c_ref[t, :, r, :] * v

            copy_rows(rows, fill)
    first, last = edges((blocks, CHUNK, LANES))
    first8, last8 = edges((blocks, HALO, LANES))

    for j in range(ITERS):
        k = ITERS - 1 - j
        old, new = (mv0, mv1) if j % 2 == 0 else (mv1, mv0)

        def gain(t, r0, j=j, k=k):
            g = lam[t, :, r0 : r0 + CHUNK, :] * slopes[k, t, :, r0 : r0 + CHUNK, :]
            at = slice(r0 - HALO, r0 - HALO + CHUNK)
            grad[t, :, at, :] = grad[t, :, at, :] + g if j else g

        def gain_plane(t, carry, gain=gain):
            for r0 in range(HALO, rows - HALO, CHUNK):
                gain(t, r0)
            return carry

        def step(t, r0, n, f, l, j=j, old=old, new=new):
            change, _ = lap_rows(old, t, r0, n, f, l)
            after = lam[t, :, r0 : r0 + n, :] + change
            lam[t, :, r0 : r0 + n, :] = after
            if j < ITERS - 1:
                new[t, :, HALO + r0 : HALO + r0 + n, :] = c_ref[t, :, r0 : r0 + n, :] * after

        def own_plane(t, carry, gain=gain, step=step, j=j):
            for r0 in range(HALO, rows - HALO, CHUNK):
                gain(t, r0)
                step(t, r0, CHUNK, first, last)
            if j < ITERS - 1:
                step(t, 0, HALO, first8, last8)
                step(t, rows - HALO, HALO, first8, last8)
            return carry

        def halo_plane(t, carry, step=step):
            for r0 in range(0, rows, CHUNK):
                step(t, r0, CHUNK, first, last)
            return carry

        gain_plane(j, 0)
        spans(1 + j, 2 * half, own_plane)
        spans(2 * half, 2 * half + ITERS - 1 - j, halo_plane)
        if j < ITERS - 1:
            for i in range(2):

                def keep(r, rh, j=j, i=i, new=new):
                    saved[j, i, :, r, :] = new[j + 1 + i, :, rh, :]

                copy_rows(rows, keep)


def backward_wedge(off, me_ref, rb_ref, b_ref, cw, c_ref, slopes, saved, lam_in, grad_in, o0, o1, o2, o3, lam, mv0, mv1, grad):
    inner = o0.shape[3]
    rows = inner + 2 * HALO
    half, blocks = b_ref.shape[:2]
    clear_rims(mv0, rows)
    clear_rims(mv1, rows)

    def there(r):
        return pl.ds(pl.multiple_of(r.start + off, 8), r.size)

    for i in range(half):

        def fill(r, rh, i=i):
            v = rb_ref[half - 1 - i, :, there(r), :]
            lam[i, :, r, :] = v
            mv0[i, :, rh, :] = cw[i, :, there(r), :] * v
            lam[half + i, :, r, :] = lam_in[i, :, there(r), :]
            if i < 2:
                mv0[half + i, :, rh, :] = c_ref[i, :, there(r), :] * b_ref[i, :, there(r), :]

        copy_rows(rows, fill)
        copy_rows(inner, lambda r, rh, i=i: grad.__setitem__((i, slice(None), r), grad_in[i, :, there(r), :]))
    first, last = edges((blocks, CHUNK, LANES))
    for j in range(ITERS):
        k = ITERS - 1 - j
        old, new = (mv0, mv1) if j % 2 == 0 else (mv1, mv0)
        if j:
            for i in range(2):

                def recall(r, rh, j=j, i=i, old=old):
                    old[half + j + i, :, rh, :] = saved[j - 1, i, :, there(r), :]

                copy_rows(rows, recall)

        def plane(s, carry, own, j=j, old=old, new=new):
            for r0 in range(0, rows, CHUNK):
                change, _ = lap_rows(old, s, r0, CHUNK, first, last)
                after = lam[s, :, r0 : r0 + CHUNK, :] + change
                if j < ITERS - 1:
                    at = slice(off + r0, off + r0 + CHUNK)
                    coef = c_ref[s - half, :, at, :] if own else cw[s, :, at, :]
                    new[s, :, HALO + r0 : HALO + r0 + CHUNK, :] = coef * after
                lam[s, :, r0 : r0 + CHUNK, :] = after
            return carry

        def gain(s, carry, k=k):
            for r0 in range(HALO, rows - HALO, CHUNK):
                at = slice(r0 - HALO, r0 - HALO + CHUNK)
                g = lam[s, :, r0 : r0 + CHUNK, :] * slopes[k, s - half, :, off + r0 : off + r0 + CHUNK, :]
                grad[s - half, :, at, :] = grad[s - half, :, at, :] + g
            return carry

        spans(half, half + j, gain)
        spans(half - ITERS + 1 + j, half, lambda s, c: plane(s, c, False))
        spans(half, half + j + 1, lambda s, c: plane(s, c, True))
    me = me_ref[0]
    planes = half // 2
    for r, out in zip(ROUNDS, (o0, o1, o2, o3)):
        block, _ = slot(me, r, planes, 0)

        @pl.when(block == 0)
        def _(r=r, out=out):
            for i in range(planes):
                _, at = slot(me, r, planes, i)
                out[0, i] = grad[at]
                out[1, i] = lam[half + at, :, HALO : HALO + inner, :]

        @pl.when(block == 1)
        def _(r=r, out=out):
            for i in range(planes):
                _, at = slot(me, r, planes, i)
                out[0, i] = grad_in[half + at, :, off : off + inner, :]
                out[1, i] = lam_in[half + at, :, off + HALO : off + HALO + inner, :]


def home_kernel(off, rounds, me_ref, scale_ref, *refs):
    count = len(rounds)
    msgs, (g_out, a_out, near, ready, sems, done) = refs[:count], refs[-6:]
    _, x, c = bits(me_ref[0])
    _, planes, blocks, inner = near.shape[1:5]
    rows = g_out.shape[1] // PARTS
    come = [pltpu.make_async_copy(m, near.at[n], sems.at[n]) for n, m in enumerate(msgs)]
    for copy in come:
        copy.start()
    go = []
    for n, (r1, r0) in enumerate(rounds):
        start = pl.multiple_of(part(c ^ r1, x ^ r0) * rows + off, 8)
        come[n].wait()
        for k, out in enumerate((g_out, a_out)):
            scale = scale_ref[0, k]
            for i in range(planes):
                for b in range(blocks):
                    ready[n, k, i, :, b * LANES : (b + 1) * LANES] = near[n, k, i, b] * scale
            go.append(pltpu.make_async_copy(ready.at[n, k], out.at[:, pl.ds(start, inner), :], done.at[n, k]))
            go[-1].start()
    for copy in go:
        copy.wait()


def shape(*dims):
    return pltpu.VMEM(dims, F32)


def exchange_sum(value, axis, count, steps):
    for step in steps:
        value = value + lax.ppermute(value, axis, [(i, i ^ step) for i in range(count)])
    return value


def on_device(coefficient, initial_field, observed, misfit_weight):
    axis = "gz"
    count = lax.axis_size(axis)
    planes, height, width = coefficient.shape
    if count % GROUP or width % LANES or height % (32 * PARTS) or 2 * planes < ITERS or ITERS * 2 > HALO:
        raise ValueError("unsupported sizes")
    rows = height // PARTS
    tall = rows + 2 * HALO
    half = 2 * planes
    blocks = width // LANES
    me = lax.axis_index(axis).astype(jnp.int32).reshape(1)

    partner = [(i, i ^ 1) for i in range(count)]
    beyond = []
    for i in range(count - GROUP + 1):
        if i % 2:
            if i + GROUP - 1 < count:
                beyond += [(i, i + GROUP - 1), (i + GROUP - 1, i)]

    def regroup(a, b, rim, name):
        message = shape(2, planes, blocks, rows + 2 * rim, LANES)
        msgs = call(partial(pack_kernel, rim), name, [message] * 4, [me], [a, b])
        got = []
        for m, r in zip(msgs, ROUNDS):
            got.append(lax.ppermute(m, axis, send_pairs(count, *r)))
        return outside(*got)

    first = regroup(*outside(initial_field, coefficient), HALO, "pack_state")
    second = regroup(*outside(observed, misfit_weight), HALO - ITERS, "pack_data")

    plane_set = (blocks, tall, LANES)
    padded = (blocks, tall + 2 * HALO, LANES)
    inner = (blocks, rows, LANES)
    saved_shape = shape(ITERS - 1, 2, *plane_set)
    quarter = shape(2, planes, *plane_set)
    (early,) = call(early_kernel, "early", [quarter], [me], first[:2])
    early = lax.ppermute(early, axis, beyond)
    late, blk_a, blk_b = call(place_kernel, "place", [quarter] + [shape(2, half, *plane_set)] * 2, [me], first)
    late = lax.ppermute(late, axis, beyond)
    far_a = lax.ppermute(blk_a, axis, partner)
    far_a, early, late = outside(far_a, early, late)
    final, coef, slopes, saved = call(
        forward_main,
        "forward_main",
        [shape(2 * half, *plane_set), shape(3 * half, *plane_set), shape(ITERS, 2 * half, *plane_set), saved_shape],
        [me],
        inside(blk_a, blk_b) + [far_a],
        [pltpu.VMEM((3 * half, *padded), F32)] * 2,
    )
    final, slopes, far_coef = call(
        forward_wedge,
        "forward_wedge",
        [shape(2 * half, *plane_set), shape(ITERS, 2 * half, *plane_set), shape(half, *plane_set)],
        [me],
        [early, late] + inside(blk_b, coef, saved, final, slopes),
        [pltpu.VMEM((half + ITERS + 2, *padded), F32)] * 2,
        input_output_aliases={6: 0, 7: 1},
    )

    lam_a, lam_b, part_total = call(
        resid_kernel,
        "resid",
        [shape(half, *plane_set)] * 2 + [jax.ShapeDtypeStruct((1, 1), F32)],
        [me],
        second + inside(final),
        [
            pltpu.VMEM((blocks, HALO, LANES), F32),
            pltpu.VMEM((4,) + second[0].shape, F32),
            pltpu.SemaphoreType.DMA((4,)),
        ],
        total=True,
        far=4,
    )
    far_lb = lax.ppermute(lam_b, axis, beyond)
    far_la = lax.ppermute(lam_a, axis, partner)
    (far_la,), (far_lb,) = outside(far_la), outside(far_lb)
    far = [1] + [1 << k for k in range(3, count.bit_length() - 1)]
    part_total = exchange_sum(part_total, axis, count, [2])
    lam, grad, saved = call(
        backward_main,
        "backward_main",
        [shape(3 * half, *plane_set), shape(2 * half, *inner), saved_shape],
        [me],
        [far_la] + inside(lam_a, lam_b, coef, slopes),
        [pltpu.VMEM((3 * half, *padded), F32)] * 2,
    )
    part_total = exchange_sum(part_total, axis, count, [4])
    strip = rows // 2
    back = []
    for n in range(2):
        outs = call(
            partial(backward_wedge, n * strip),
            f"backward_wedge_{n}",
            [shape(2, planes, blocks, strip, LANES)] * 4,
            [me],
            [far_lb] + inside(lam_b, far_coef, coef, slopes, saved, lam, grad),
            [pltpu.VMEM((2 * half, blocks, strip + 2 * HALO, LANES), F32)]
            + [pltpu.VMEM((half + ITERS + 2, blocks, strip + 4 * HALO, LANES), F32)] * 2
            + [pltpu.VMEM((half, blocks, strip, LANES), F32)],
        )
        for m, r in zip(outs, ROUNDS):
            back.append(lax.ppermute(m, axis, [(j, i) for i, j in send_pairs(count, *r)]))
    back = outside(*back)

    if count & (count - 1):
        total = lax.psum(part_total, axis) / 4
    else:
        total = exchange_sum(part_total, axis, count, far)
    cells = count * planes * height * width
    misfit = jnp.sqrt(total[0, 0] / cells + 1e-06)
    inverse = 1.0 / misfit
    scale = jnp.stack([time_step * inverse, inverse]).reshape(1, 2)
    held = []
    for n, size in ((0, 2), (2, 2), (4, 2), (6, 1), (7, 1)):
        held = pl.pallas_call(
            partial(home_kernel, n // 4 * strip, ROUNDS[n % 4 : n % 4 + size]),
            out_shape=[jax.ShapeDtypeStruct((planes, height, width), F32)] * 2,
            in_specs=[SM, SM] + [ANY] * (size + len(held)),
            out_specs=[ANY] * 2,
            scratch_shapes=[
                pltpu.VMEM((size, 2, planes, blocks, strip, LANES), F32),
                pltpu.VMEM((size, 2, planes, strip, width), F32),
                pltpu.SemaphoreType.DMA((size,)),
                pltpu.SemaphoreType.DMA((size, 2)),
            ],
            input_output_aliases={2 + size: 0, 3 + size: 1} if held else {},
            compiler_params=pltpu.CompilerParams(vmem_limit_bytes=14 << 20),
        )(me, scale, *back[n : n + size], *held)
    gradient, adjoint = held
    return gradient, adjoint, misfit


def solution(mesh):
    placed = P("gz", None, None)
    return jax.shard_map(
        on_device,
        mesh=mesh,
        in_specs=(placed,) * 4,
        out_specs=(placed, placed, P()),
        check_vma=False,
    )
```

```python
from functools import partial

import jax
import jax.numpy as jnp
from jax import lax
from jax.experimental import pallas as pl
from jax.experimental.pallas import tpu as pltpu
from jax.sharding import PartitionSpec as P


ITERS = 4
time_step = 0.125

GROUP = 8
PARTS = 4
HALO = 8
LANES = 128
ROUNDS = ((0, 1), (0, 0), (1, 1), (1, 0))


VM = pl.BlockSpec(memory_space=pltpu.VMEM)
SM = pl.BlockSpec(memory_space=pltpu.SMEM)
ANY = pl.BlockSpec(memory_space=pl.ANY)
SHARE = {"forward_main": 30, "forward_wedge": 30, "backward_main": 11, "backward_wedge_0": 9, "backward_wedge_1": 9, "resid": 8}
F32 = jnp.float32


def call(kernel, name, outs, scalars, arrays, scratch=(), total=False, far=0, **options):
    return pl.pallas_call(
        kernel,
        out_shape=outs,
        in_specs=[SM] * len(scalars) + [ANY] * far + [VM] * (len(arrays) - far),
        out_specs=[VM] * (len(outs) - total) + [SM] * total,
        scratch_shapes=scratch,
        compiler_params=pltpu.CompilerParams(vmem_limit_bytes=SHARE.get(name, 14) << 20),
        **options,
    )(*scalars, *arrays)


def inside(*arrays):
    return [pltpu.with_memory_space_constraint(a, pltpu.VMEM) for a in arrays]


def outside(*arrays):
    return [pltpu.with_memory_space_constraint(a, pltpu.HBM) for a in arrays]


def bits(me):
    return (me >> 2) & 1, (me >> 1) & 1, me & 1


def part(y, x):
    return 2 * y + x


def send_pairs(count, r1, r0):
    pairs = []
    for i in range(count):
        y, x, c = bits(i)
        pairs.append((i, (i & ~7) + 4 * (c ^ r1) + 2 * (x ^ r0) + y))
    return pairs


def pack_kernel(rim, me_ref, a_ref, b_ref, *out_refs):
    _, x, c = bits(me_ref[0])
    planes, height, width = a_ref.shape
    rows = height // PARTS
    for (r1, r0), out in zip(ROUNDS, out_refs):
        q = part(c ^ r1, x ^ r0)
        start = pl.multiple_of(q * rows, 8)
        above = pl.multiple_of(jnp.maximum(start - HALO, 0), 8)
        below = pl.multiple_of(jnp.minimum(start + rows, height - HALO), 8)
        for k, src in enumerate((a_ref, b_ref)):
            for i in range(planes):
                for b in range(width // LANES):
                    cols = slice(b * LANES, (b + 1) * LANES)
                    top = src[i, pl.ds(above, HALO), cols]
                    out[k, i, b, :rim, :] = jnp.where(q > 0, top[HALO - rim :], 0.0)
                    low = src[i, pl.ds(below, HALO), cols]
                    out[k, i, b, rim + rows :, :] = jnp.where(q < PARTS - 1, low[:rim], 0.0)
                    for at in range(0, rows, HALO):
                        here = pl.ds(pl.multiple_of(start + at, 8), HALO)
                        out[k, i, b, rim + at : rim + at + HALO, :] = src[i, here, cols]


def slot(me, r, planes, i):
    y, x, c = bits(me)
    r1, r0 = r
    from_c = y ^ r1
    block = x ^ r0 ^ c
    ahead = planes * from_c + i
    return block, jnp.where(c == 0, ahead, 2 * planes - 1 - ahead)


def early_kernel(me_ref, m0, m1, early_ref):
    me = me_ref[0]
    for r, m in zip(ROUNDS, (m0, m1)):
        block, _ = slot(me, r, m.shape[1], 0)

        @pl.when(block == 0)
        def _(m=m):
            early_ref[...] = m[...]


def place_kernel(me_ref, m0, m1, m2, m3, late_ref, a_ref, b_ref):
    me = me_ref[0]
    planes = m0.shape[1]
    for r, m in zip(ROUNDS, (m0, m1, m2, m3)):
        block, _ = slot(me, r, planes, 0)

        @pl.when(block == 0)
        def _(r=r, m=m):
            if r[0]:
                late_ref[...] = m[...]
            for i in range(planes):
                _, at = slot(me, r, planes, i)
                for k in range(2):
                    b_ref[k, at] = m[k, i]

        @pl.when(block == 1)
        def _(r=r, m=m):
            for i in range(planes):
                _, at = slot(me, r, planes, i)
                for k in range(2):
                    a_ref[k, at] = m[k, i]


def edges(shape):
    col = lax.broadcasted_iota(jnp.int32, shape, 2)
    return col == 0, col == shape[2] - 1


def lap_rows(ref, s, r0, n, first, last):
    lo = HALO + r0
    mid = ref[s, :, lo : lo + n, :]
    none = jnp.zeros((1,) + mid.shape[1:], F32)
    beside = ref[s + 1, :, lo : lo + n, :] + ref[s - 1, :, lo : lo + n, :]
    beside = beside + (ref[s, :, lo + 1 : lo + n + 1, :] + ref[s, :, lo - 1 : lo + n - 1, :])
    right = pltpu.roll(mid, LANES - 1, 2)
    right = jnp.where(last, jnp.concatenate([right[1:], none], axis=0), right)
    left = pltpu.roll(mid, 1, 2)
    left = jnp.where(first, jnp.concatenate([none, left[:-1]], axis=0), left)
    return beside + (right + left) - 6.0 * mid, mid


def clear_rims(ref, rows):
    none = jnp.zeros((ref.shape[1], HALO, LANES), F32)

    def one(s, carry):
        ref[s, :, :HALO, :] = none
        ref[s, :, HALO + rows :, :] = none
        return carry

    lax.fori_loop(0, ref.shape[0], one, 0)


CHUNK = 16


def copy_rows(rows, move):
    def one(t, carry):
        r = pl.multiple_of(t * CHUNK, 8)
        move(pl.ds(r, CHUNK), pl.ds(r + HALO, CHUNK))
        return carry

    lax.fori_loop(0, rows // CHUNK, one, 0)


def spans(lo, hi, body):
    if (hi - lo) % 2:
        body(lo, 0)
        lo += 1

    def two(t, carry):
        body(lo + 2 * t, carry)
        body(lo + 2 * t + 1, carry)
        return carry

    if hi > lo:
        lax.fori_loop(0, (hi - lo) // 2, two, 0)


def forward_main(me_ref, a_ref, b_ref, ra_ref, u_out, c_out, slopes, saved, u0, u1):
    half, blocks, rows = a_ref.shape[1:4]
    clear_rims(u0, rows)
    clear_rims(u1, rows)
    for i in range(half):
        for src, at, t in ((b_ref, i, i), (a_ref, i, half + i), (ra_ref, half - 1 - i, 2 * half + i)):

            def fill(r, rh, src=src, at=at, t=t):
                u0[t, :, rh, :] = src[0, at, :, r, :]
                c_out[t, :, r, :] = time_step * src[1, at, :, r, :]

            copy_rows(rows, fill)
    first, last = edges((blocks, CHUNK, LANES))
    for k in range(ITERS):
        old, new = (u0, u1) if k % 2 == 0 else (u1, u0)

        def plane(t, carry, own, k=k, old=old, new=new):
            for r0 in range(0, rows, CHUNK):
                slope, mid = lap_rows(old, t, r0, CHUNK, first, last)
                moved = mid + c_out[t, :, r0 : r0 + CHUNK, :] * slope
                if own:
                    slopes[k, t, :, r0 : r0 + CHUNK, :] = slope
                if k == ITERS - 1:
                    u_out[t, :, r0 : r0 + CHUNK, :] = moved
                else:
                    new[t, :, HALO + r0 : HALO + r0 + CHUNK, :] = moved
            return carry

        spans(1 + k, 2 * half, lambda t, c: plane(t, c, True))
        spans(2 * half, 2 * half + ITERS - 1 - k, lambda t, c: plane(t, c, False))
        if k < ITERS - 1:
            for i in range(2):

                def keep(r, rh, k=k, i=i, new=new):
                    saved[k, i, :, r, :] = new[k + 1 + i, :, rh, :]

                copy_rows(rows, keep)


def forward_wedge(me_ref, early, late, b_ref, c_ref, saved, u_in, slopes_in, u_out, slopes, cw, w0, w1):
    y, _, c = bits(me_ref[0])
    half, blocks, rows = b_ref.shape[1:4]
    planes = early.shape[1]
    clear_rims(w0, rows)
    clear_rims(w1, rows)
    for r1, far in enumerate((early, late)):
        for i in range(planes):
            ahead = planes * (y ^ r1) + i
            s = half - 1 - jnp.where(c == 1, ahead, half - 1 - ahead)

            def fill(r, rh, far=far, i=i, s=s):
                w0[s, :, rh, :] = far[0, i, :, r, :]
                cw[s, :, r, :] = time_step * far[1, i, :, r, :]

            copy_rows(rows, fill)
    for i in range(2):
        copy_rows(rows, lambda r, rh, i=i: w0.__setitem__((half + i, slice(None), rh), b_ref[0, i, :, r, :]))
    first, last = edges((blocks, CHUNK, LANES))
    for k in range(ITERS):
        old, new = (w0, w1) if k % 2 == 0 else (w1, w0)
        if k:
            for i in range(2):
                copy_rows(rows, lambda r, rh, i=i: old.__setitem__((half + k + i, slice(None), rh), saved[k - 1, i, :, r, :]))

        def plane(s, carry, own, k=k, old=old, new=new):
            for r0 in range(0, rows, CHUNK):
                slope, mid = lap_rows(old, s, r0, CHUNK, first, last)
                at = slice(r0, r0 + CHUNK)
                coef = c_ref[s - half, :, at, :] if own else cw[s, :, at, :]
                moved = mid + coef * slope
                if own:
                    slopes[k, s - half, :, at, :] = slope
                if k == ITERS - 1:
                    u_out[s - half, :, at, :] = moved
                else:
                    new[s, :, HALO + r0 : HALO + r0 + CHUNK, :] = moved
            return carry

        spans(half - ITERS + 1 + k, half, lambda s, c: plane(s, c, False))
        spans(half, half + k + 1, lambda s, c: plane(s, c, True))


def resid_kernel(me_ref, f0, f1, f2, f3, u_ref, a_ref, b_ref, total_ref, acc_ref, near, sems):
    me = me_ref[0]
    copies = [pltpu.make_async_copy(f, near.at[n], sems.at[n]) for n, f in enumerate((f0, f1, f2, f3))]
    for copy in copies:
        copy.start()
    planes, blocks, short = near.shape[2:5]
    rows = u_ref.shape[2]
    rim = (rows - short) // 2
    shape = (blocks, HALO, LANES)
    row = lax.broadcasted_iota(jnp.int32, shape, 1)
    acc_ref[...] = jnp.zeros(shape, F32)
    for n, r in enumerate(ROUNDS):
        copies[n].wait()
        for i in range(planes):
            block, at = slot(me, r, planes, i)
            for flag, dst in ((1, a_ref), (0, b_ref)):

                @pl.when(block == flag)
                def _(n=n, i=i, at=at, dst=dst, flag=flag):
                    dst[at, :, :rim, :] = jnp.zeros((blocks, rim, LANES), F32)
                    dst[at, :, rows - rim :, :] = jnp.zeros((blocks, rim, LANES), F32)
                    acc = jnp.zeros(shape, F32)
                    for lo in range(0, short, HALO):
                        here = slice(lo + rim, lo + rim + HALO)
                        resid = u_ref[2 * planes * flag + at, :, here, :] - near[n, 0, i, :, lo : lo + HALO, :]
                        weighted = near[n, 1, i, :, lo : lo + HALO, :] * resid
                        dst[at, :, here, :] = weighted
                        share = weighted * resid
                        if lo + rim < HALO:
                            share = jnp.where(row >= HALO - rim, share, 0.0)
                        if lo + rim + HALO > rows - HALO:
                            share = jnp.where(row < HALO - rim, share, 0.0)
                        acc = acc + share
                    acc_ref[...] = acc_ref[...] + acc

    total_ref[0, 0] = jnp.sum(acc_ref[...])


def backward_main(me_ref, ra_ref, a_ref, b_ref, c_ref, slopes, lam, grad, saved, mv0, mv1):
    half, blocks, rows = a_ref.shape[:3]
    clear_rims(mv0, rows)
    clear_rims(mv1, rows)
    for i in range(half):
        for src, at, t in ((b_ref, i, i), (a_ref, i, half + i), (ra_ref, half - 1 - i, 2 * half + i)):

            def fill(r, rh, src=src, at=at, t=t):
                v = src[at, :, r, :]
                lam[t, :, r, :] = v
                mv0[t, :, rh, :] = c_ref[t, :, r, :] * v

            copy_rows(rows, fill)
    first, last = edges((blocks, CHUNK, LANES))
    first8, last8 = edges((blocks, HALO, LANES))

    for j in range(ITERS):
        k = ITERS - 1 - j
        old, new = (mv0, mv1) if j % 2 == 0 else (mv1, mv0)

        def gain(t, r0, j=j, k=k):
            g = lam[t, :, r0 : r0 + CHUNK, :] * slopes[k, t, :, r0 : r0 + CHUNK, :]
            at = slice(r0 - HALO, r0 - HALO + CHUNK)
            grad[t, :, at, :] = grad[t, :, at, :] + g if j else g

        def gain_plane(t, carry, gain=gain):
            for r0 in range(HALO, rows - HALO, CHUNK):
                gain(t, r0)
            return carry

        def step(t, r0, n, f, l, j=j, old=old, new=new):
            change, _ = lap_rows(old, t, r0, n, f, l)
            after = lam[t, :, r0 : r0 + n, :] + change
            lam[t, :, r0 : r0 + n, :] = after
            if j < ITERS - 1:
                new[t, :, HALO + r0 : HALO + r0 + n, :] = c_ref[t, :, r0 : r0 + n, :] * after

        def own_plane(t, carry, gain=gain, step=step, j=j):
            for r0 in range(HALO, rows - HALO, CHUNK):
                gain(t, r0)
                step(t, r0, CHUNK, first, last)
            if j < ITERS - 1:
                step(t, 0, HALO, first8, last8)
                step(t, rows - HALO, HALO, first8, last8)
            return carry

        def halo_plane(t, carry, step=step):
            for r0 in range(0, rows, CHUNK):
                step(t, r0, CHUNK, first, last)
            return carry

        gain_plane(j, 0)
        spans(1 + j, 2 * half, own_plane)
        spans(2 * half, 2 * half + ITERS - 1 - j, halo_plane)
        if j < ITERS - 1:
            for i in range(2):

                def keep(r, rh, j=j, i=i, new=new):
                    saved[j, i, :, r, :] = new[j + 1 + i, :, rh, :]

                copy_rows(rows, keep)


def backward_wedge(off, me_ref, rb_ref, b_ref, cw, c_ref, slopes, saved, lam_in, grad_in, o0, o1, o2, o3, lam, mv0, mv1, grad):
    inner = o0.shape[3]
    rows = inner + 2 * HALO
    half, blocks = b_ref.shape[:2]
    clear_rims(mv0, rows)
    clear_rims(mv1, rows)

    def there(r):
        return pl.ds(pl.multiple_of(r.start + off, 8), r.size)

    for i in range(half):

        def fill(r, rh, i=i):
            v = rb_ref[half - 1 - i, :, there(r), :]
            lam[i, :, r, :] = v
            mv0[i, :, rh, :] = cw[i, :, there(r), :] * v
            lam[half + i, :, r, :] = lam_in[i, :, there(r), :]
            if i < 2:
                mv0[half + i, :, rh, :] = c_ref[i, :, there(r), :] * b_ref[i, :, there(r), :]

        copy_rows(rows, fill)
        copy_rows(inner, lambda r, rh, i=i: grad.__setitem__((i, slice(None), r), grad_in[i, :, there(r), :]))
    first, last = edges((blocks, CHUNK, LANES))
    for j in range(ITERS):
        k = ITERS - 1 - j
        old, new = (mv0, mv1) if j % 2 == 0 else (mv1, mv0)
        if j:
            for i in range(2):

                def recall(r, rh, j=j, i=i, old=old):
                    old[half + j + i, :, rh, :] = saved[j - 1, i, :, there(r), :]

                copy_rows(rows, recall)

        def plane(s, carry, own, j=j, old=old, new=new):
            for r0 in range(0, rows, CHUNK):
                change, _ = lap_rows(old, s, r0, CHUNK, first, last)
                after = lam[s, :, r0 : r0 + CHUNK, :] + change
                if j < ITERS - 1:
                    at = slice(off + r0, off + r0 + CHUNK)
                    coef = c_ref[s - half, :, at, :] if own else cw[s, :, at, :]
                    new[s, :, HALO + r0 : HALO + r0 + CHUNK, :] = coef * after
                lam[s, :, r0 : r0 + CHUNK, :] = after
            return carry

        def gain(s, carry, k=k):
            for r0 in range(HALO, rows - HALO, CHUNK):
                at = slice(r0 - HALO, r0 - HALO + CHUNK)
                g = lam[s, :, r0 : r0 + CHUNK, :] * slopes[k, s - half, :, off + r0 : off + r0 + CHUNK, :]
                grad[s - half, :, at, :] = grad[s - half, :, at, :] + g
            return carry

        spans(half, half + j, gain)
        spans(half - ITERS + 1 + j, half, lambda s, c: plane(s, c, False))
        spans(half, half + j + 1, lambda s, c: plane(s, c, True))
    me = me_ref[0]
    planes = half // 2
    for r, out in zip(ROUNDS, (o0, o1, o2, o3)):
        block, _ = slot(me, r, planes, 0)

        @pl.when(block == 0)
        def _(r=r, out=out):
            for i in range(planes):
                _, at = slot(me, r, planes, i)
                out[0, i] = grad[at]
                out[1, i] = lam[half + at, :, HALO : HALO + inner, :]

        @pl.when(block == 1)
        def _(r=r, out=out):
            for i in range(planes):
                _, at = slot(me, r, planes, i)
                out[0, i] = grad_in[half + at, :, off : off + inner, :]
                out[1, i] = lam_in[half + at, :, off + HALO : off + HALO + inner, :]


def home_kernel(off, rounds, me_ref, scale_ref, *refs):
    count = len(rounds)
    msgs, (g_out, a_out, near, ready, sems, done) = refs[:count], refs[-6:]
    _, x, c = bits(me_ref[0])
    _, planes, blocks, inner = near.shape[1:5]
    rows = g_out.shape[1] // PARTS
    come = [pltpu.make_async_copy(m, near.at[n], sems.at[n]) for n, m in enumerate(msgs)]
    for copy in come:
        copy.start()
    go = []
    for n, (r1, r0) in enumerate(rounds):
        start = pl.multiple_of(part(c ^ r1, x ^ r0) * rows + off, 8)
        come[n].wait()
        for k, out in enumerate((g_out, a_out)):
            scale = scale_ref[0, k]
            for i in range(planes):
                for b in range(blocks):
                    ready[n, k, i, :, b * LANES : (b + 1) * LANES] = near[n, k, i, b] * scale
            go.append(pltpu.make_async_copy(ready.at[n, k], out.at[:, pl.ds(start, inner), :], done.at[n, k]))
            go[-1].start()
    for copy in go:
        copy.wait()


def shape(*dims):
    return pltpu.VMEM(dims, F32)


def exchange_sum(value, axis, count, steps):
    for step in steps:
        value = value + lax.ppermute(value, axis, [(i, i ^ step) for i in range(count)])
    return value


def on_device(coefficient, initial_field, observed, misfit_weight):
    axis = "gz"
    count = lax.axis_size(axis)
    planes, height, width = coefficient.shape
    if count % GROUP or width % LANES or height % (32 * PARTS) or 2 * planes < ITERS or ITERS * 2 > HALO:
        raise ValueError("unsupported sizes")
    rows = height // PARTS
    tall = rows + 2 * HALO
    half = 2 * planes
    blocks = width // LANES
    me = lax.axis_index(axis).astype(jnp.int32).reshape(1)

    partner = [(i, i ^ 1) for i in range(count)]
    beyond = []
    for i in range(count - GROUP + 1):
        if i % 2:
            if i + GROUP - 1 < count:
                beyond += [(i, i + GROUP - 1), (i + GROUP - 1, i)]

    def regroup(a, b, rim, name):
        message = shape(2, planes, blocks, rows + 2 * rim, LANES)
        msgs = call(partial(pack_kernel, rim), name, [message] * 4, [me], [a, b])
        got = []
        for m, r in zip(msgs, ROUNDS):
            got.append(lax.ppermute(m, axis, send_pairs(count, *r)))
        return outside(*got)

    first = regroup(*outside(initial_field, coefficient), HALO, "pack_state")
    second = regroup(*outside(observed, misfit_weight), HALO - ITERS, "pack_data")

    plane_set = (blocks, tall, LANES)
    padded = (blocks, tall + 2 * HALO, LANES)
    inner = (blocks, rows, LANES)
    saved_shape = shape(ITERS - 1, 2, *plane_set)
    quarter = shape(2, planes, *plane_set)
    (early,) = call(early_kernel, "early", [quarter], [me], first[:2])
    early = lax.ppermute(early, axis, beyond)
    late, blk_a, blk_b = call(place_kernel, "place", [quarter] + [shape(2, half, *plane_set)] * 2, [me], first)
    late = lax.ppermute(late, axis, beyond)
    far_a = lax.ppermute(blk_a, axis, partner)
    far_a, early, late = outside(far_a, early, late)
    final, coef, slopes, saved = call(
        forward_main,
        "forward_main",
        [shape(2 * half, *plane_set), shape(3 * half, *plane_set), shape(ITERS, 2 * half, *plane_set), saved_shape],
        [me],
        inside(blk_a, blk_b) + [far_a],
        [pltpu.VMEM((3 * half, *padded), F32)] * 2,
    )
    final, slopes, far_coef = call(
        forward_wedge,
        "forward_wedge",
        [shape(2 * half, *plane_set), shape(ITERS, 2 * half, *plane_set), shape(half, *plane_set)],
        [me],
        [early, late] + inside(blk_b, coef, saved, final, slopes),
        [pltpu.VMEM((half + ITERS + 2, *padded), F32)] * 2,
        input_output_aliases={6: 0, 7: 1},
    )

    lam_a, lam_b, part_total = call(
        resid_kernel,
        "resid",
        [shape(half, *plane_set)] * 2 + [jax.ShapeDtypeStruct((1, 1), F32)],
        [me],
        second + inside(final),
        [
            pltpu.VMEM((blocks, HALO, LANES), F32),
            pltpu.VMEM((4,) + second[0].shape, F32),
            pltpu.SemaphoreType.DMA((4,)),
        ],
        total=True,
        far=4,
    )
    far_lb = lax.ppermute(lam_b, axis, beyond)
    far_la = lax.ppermute(lam_a, axis, partner)
    (far_la,), (far_lb,) = outside(far_la), outside(far_lb)
    far = [1] + [1 << k for k in range(3, count.bit_length() - 1)]
    part_total = exchange_sum(part_total, axis, count, [2])
    lam, grad, saved = call(
        backward_main,
        "backward_main",
        [shape(3 * half, *plane_set), shape(2 * half, *inner), saved_shape],
        [me],
        [far_la] + inside(lam_a, lam_b, coef, slopes),
        [pltpu.VMEM((3 * half, *padded), F32)] * 2,
    )
    part_total = exchange_sum(part_total, axis, count, [4])
    cut = max(CHUNK, rows * 3 // 8 // CHUNK * CHUNK)
    strips = ((0, cut), (cut, rows - cut))
    back = []
    for n, (off, strip) in enumerate(strips):
        outs = call(
            partial(backward_wedge, off),
            f"backward_wedge_{n}",
            [shape(2, planes, blocks, strip, LANES)] * 4,
            [me],
            [far_lb] + inside(lam_b, far_coef, coef, slopes, saved, lam, grad),
            [pltpu.VMEM((2 * half, blocks, strip + 2 * HALO, LANES), F32)]
            + [pltpu.VMEM((half + ITERS + 2, blocks, strip + 4 * HALO, LANES), F32)] * 2
            + [pltpu.VMEM((half, blocks, strip, LANES), F32)],
        )
        for m, r in zip(outs, ROUNDS):
            back.append(lax.ppermute(m, axis, [(j, i) for i, j in send_pairs(count, *r)]))
    back = outside(*back)

    if count & (count - 1):
        total = lax.psum(part_total, axis) / 4
    else:
        total = exchange_sum(part_total, axis, count, far)
    cells = count * planes * height * width
    misfit = jnp.sqrt(total[0, 0] / cells + 1e-06)
    inverse = 1.0 / misfit
    scale = jnp.stack([time_step * inverse, inverse]).reshape(1, 2)
    held = []
    for n in range(0, 8, 2):
        off, strip = strips[n // 4]
        held = pl.pallas_call(
            partial(home_kernel, off, ROUNDS[n % 4 : n % 4 + 2]),
            out_shape=[jax.ShapeDtypeStruct((planes, height, width), F32)] * 2,
            in_specs=[SM, SM, ANY, ANY] + [ANY] * len(held),
            out_specs=[ANY] * 2,
            scratch_shapes=[
                pltpu.VMEM((2, 2, planes, blocks, strip, LANES), F32),
                pltpu.VMEM((2, 2, planes, strip, width), F32),
                pltpu.SemaphoreType.DMA((2,)),
                pltpu.SemaphoreType.DMA((2, 2)),
            ],
            input_output_aliases={4: 0, 5: 1} if held else {},
            compiler_params=pltpu.CompilerParams(vmem_limit_bytes=14 << 20),
        )(me, scale, *back[n : n + 2], *held)
    gradient, adjoint = held
    return gradient, adjoint, misfit


def solution(mesh):
    placed = P("gz", None, None)
    return jax.shard_map(
        on_device,
        mesh=mesh,
        in_specs=(placed,) * 4,
        out_specs=(placed, placed, P()),
        check_vma=False,
    )
```
